32 devices in a mesh: seq: 8 (over y, x, core), batch: 4 (over z).
Axes of the slice: x: 2, y: 2, z: 4, core: 2. Of those that a mesh axis runs over, the one named last changes fastest.
Arguments:
- inputs: bfloat16 [4, 1024, 1024], P('batch', 'seq'), may hold values from -6 to 6
- lengths: int32 [4], P('batch'), may hold values from 256 to 1024, as said below
- w_qkv: bfloat16 [1024, 3072], P(('seq', 'batch')), may hold values from -0.1875 to 0.1875
- w_out: bfloat16 [1024, 1024], P(('seq', 'batch')), may hold values from -0.1875 to 0.1875
- w_up: bfloat16 [1024, 4096], P(('seq', 'batch')), may hold values from -0.1875 to 0.1875
- w_down: bfloat16 [4096, 1024], P(('seq', 'batch')), may hold values from -0.09375 to 0.09375
- norm_gains: bfloat16 [3, 1024], P(None, ('seq', 'batch')), may hold values from 0.5 to 1.5
- model_biases: bfloat16 [5, 1024], P(None, ('seq', 'batch')), may hold values from -4 to 4
- attn_biases: bfloat16 [2, 1024], P(None, ('seq', 'batch')), may hold values from -0.3125 to 0.3125
- ff_gain: bfloat16 [4096], P(('seq', 'batch')), may hold values from 0.5 to 1.5
- ff_biases: bfloat16 [2, 4096], P(None, ('seq', 'batch')), may hold values from -4 to 4
- head_scale: bfloat16 [16], replicated, may hold values from 0.5 to 2
- cotangent: bfloat16 [4, 1024, 1024], P('batch', 'seq'), may hold values from -6 to 6
Outputs:
- output: bfloat16 [4, 1024, 1024], P('batch', 'seq')
- grad_input: bfloat16 [4, 1024, 1024], P('batch', 'seq')
- grad_qkv: float32 [1024, 3072], P(('seq', 'batch'))
- grad_out: float32 [1024, 1024], P(('seq', 'batch'))
- grad_up: float32 [1024, 4096], P(('seq', 'batch'))
- grad_down: float32 [4096, 1024], P(('seq', 'batch'))
- grad_norm_gains: float32 [3, 1024], P(None, ('seq', 'batch'))
- grad_model_biases: float32 [5, 1024], P(None, ('seq', 'batch'))
- grad_attn_biases: float32 [2, 1024], P(None, ('seq', 'batch'))
- grad_ff_gain: float32 [4096], P(('seq', 'batch'))
- grad_ff_biases: float32 [2, 4096], P(None, ('seq', 'batch'))
- grad_head_scale: float32 [16], replicated
The draws below stay inside these ranges and needn't reach their ends.
Inputs may be any that keep to these rules, and one draw needn't show every extreme that they name: `lengths`: the number of leading valid rows of each sequence; every draw has one sequence with 1024 valid rows and one with 256.
All inputs are finite; a program needn't handle non-finite values.
Results may differ from the reference program's by a relative error of at most 0.01.
Values may be sent and summed in bfloat16 or wider, within the bound.
A program may use at most 192 MiB of HBM per device.

```python
import math
import jax
import jax.numpy as jnp
from jax import lax

D = 1024
H = 16
HD = 64
FF = 4096
SEQS = 4
LENGTH = 1024
KEY_BLOCK = 512


def draw_lengths(key, part):
    drawn = jax.random.randint(key, (SEQS,), LENGTH // 4, LENGTH + 1)
    shuffled = jax.random.permutation(jax.random.fold_in(key, 7), SEQS)
    drawn = drawn.at[shuffled[0]].set(LENGTH)
    drawn = drawn.at[shuffled[1]].set(LENGTH // 4)
    return drawn.astype(jnp.int32)


def level_of(own_key, dims, cuts, low, top_value):
    def one(axis_at, shards_of):
        draws = jax.random.uniform(jax.random.fold_in(jax.random.fold_in(own_key, 6), axis_at), (shards_of,), jnp.float32, low / len(cuts), top_value / len(cuts))
        return jnp.repeat(jnp.exp(draws), dims[axis_at] // shards_of).reshape((-1,) + (1,) * (len(dims) - axis_at - 1))

    level = one(*cuts[0])
    for cut in cuts[1:]:
        level = level * one(*cut)
    return level


def scatter_about(own_key, shape, scale, reach, pieces=(), held_as=jnp.bfloat16):
    factor_of = level_of(own_key, shape, pieces, -0.22, 0.18) if pieces else 1.0
    values = jax.random.normal(own_key, shape, jnp.float32) * scale * factor_of
    return jnp.minimum(jnp.maximum(values, -reach), reach).astype(held_as)


def setup_inputs(seed: int = 0) -> dict:
    splits = jax.random.split(jax.random.key(seed), 14)
    return {
        "inputs": scatter_about(splits[0], (SEQS, LENGTH, D), 1.0, 6.0, ((0, 4), (1, 8))),
        "lengths": draw_lengths(jax.random.fold_in(splits[13], 71), 0),
        "w_qkv": scatter_about(splits[2], (D, 3 * D), D ** -0.5, 0.1875, ((0, 32),)),
        "w_out": scatter_about(splits[3], (D, D), D ** -0.5, 0.1875, ((0, 32),)),
        "w_up": scatter_about(splits[4], (D, FF), D ** -0.5, 0.1875, ((0, 32),)),
        "w_down": scatter_about(splits[5], (FF, D), FF ** -0.5, 0.09375, ((0, 32),)),
        "norm_gains": jnp.clip(1.0 + 0.1 * jax.random.normal(splits[6], (3, D), jnp.float32), 0.5, 1.5).astype(jnp.bfloat16),
        "model_biases": scatter_about(splits[7], (5, D), 0.3, 4.0, ((1, 32),)),
        "attn_biases": scatter_about(splits[8], (2, D), 0.02, 0.3125, ((1, 32),)),
        "ff_gain": jnp.clip(1.0 + 0.1 * jax.random.normal(splits[9], (FF,), jnp.float32), 0.5, 1.5).astype(jnp.bfloat16),
        "ff_biases": scatter_about(splits[10], (2, FF), 0.3, 4.0, ((1, 32),)),
        "head_scale": jnp.clip(jnp.exp(jax.random.uniform(splits[11], (H,), jnp.float32, math.log(0.5), math.log(2.0))), 0.5, 2.0).astype(jnp.bfloat16),
        "cotangent": scatter_about(splits[12], (SEQS, LENGTH, D), 1.0, 6.0, ((0, 4), (1, 8))),
    }


NORM_EPSILON = 1e-05
HIGHEST = lax.Precision.HIGHEST

@jax.custom_vjp
def low(v):
    return lax.optimization_barrier(v.astype(jnp.bfloat16)).astype(jnp.float32)

@jax.custom_vjp
def low_back(v):
    return v

def low_keep(v):
    return (low(v), None)

def low_pass(kept, grad):
    return (grad,)

def back_keep(v):
    return (v, None)

def back_low(kept, grad):
    return (low(grad),)
low.defvjp(low_keep, low_pass)
low_back.defvjp(back_keep, back_low)

def layer_norm(vector, norm_gain, norm_bias):
    centered = vector - lax.optimization_barrier(jnp.mean(vector, axis=-1, keepdims=True))
    spread = lax.optimization_barrier(jnp.mean(centered * centered, axis=-1, keepdims=True))
    return centered * lax.rsqrt(spread + NORM_EPSILON) * norm_gain + norm_bias

def product(left, right):
    return jnp.dot(left, right, precision=HIGHEST)

def one_sequence(inputs, length, params):
    w_qkv, w_out, w_up, w_down, norm_gains, model_biases, attn_biases, ff_gain, ff_biases, head_scale = params
    model_width = H * HD
    positions = jnp.arange(LENGTH, dtype=jnp.int32)
    valid_mask = (positions < length)[:, None]
    normed = low(layer_norm(inputs, norm_gains[0], model_biases[0]))
    offsets = jnp.concatenate([model_biases[3], jnp.zeros_like(model_biases[3]), attn_biases[0]])
    projected = low(low_back(product(normed, w_qkv) + offsets))
    queries = projected[:, :model_width].reshape(LENGTH, H, HD)
    key_rows = projected[:, model_width:2 * model_width].reshape(LENGTH, H, HD)
    values = projected[:, 2 * model_width:].reshape(LENGTH, H, HD)
    score_scale = HD ** (-0.5)

    def attend(start):
        query_tile = lax.dynamic_slice_in_dim(queries, start, KEY_BLOCK, 0)
        scores = low_back(score_scale * jnp.einsum('qhd,khd->hqk', query_tile, key_rows, precision=HIGHEST))
        query_index = start + jnp.arange(KEY_BLOCK, dtype=jnp.int32)
        allowed = (positions[None, :] <= query_index[:, None]) & (positions[None, :] < length)
        masked = jnp.where(allowed[None], scores, -1e+30)
        log_total = jax.nn.logsumexp(masked, axis=-1, keepdims=True)
        weights = low(jnp.exp(masked - log_total))
        return low_back(jnp.einsum('hqk,khd->qhd', weights, values, precision=HIGHEST))
    starts = jnp.arange(LENGTH // KEY_BLOCK, dtype=jnp.int32) * KEY_BLOCK
    attended = lax.map(jax.checkpoint(attend), starts).reshape(LENGTH, H, HD)
    scaled = low(attended * head_scale[None, :, None]).reshape(LENGTH, model_width)
    attn_proj = low_back(product(scaled, w_out) + attn_biases[1])
    residual = inputs + layer_norm(attn_proj, norm_gains[1], model_biases[1])
    ffn_in = low(layer_norm(residual, norm_gains[2], model_biases[2]))
    hidden = low_back(product(ffn_in, w_up) + ff_biases[0])
    ffn_normed = low(layer_norm(jax.nn.gelu(hidden, approximate=False), ff_gain, ff_biases[1]))
    return jnp.where(valid_mask, residual + product(ffn_normed, w_down) + model_biases[4], 0.0)

def reference(inputs, lengths, w_qkv, w_out, w_up, w_down, norm_gains, model_biases, attn_biases, ff_gain, ff_biases, head_scale, cotangent):
    params = tuple((weight.astype(jnp.float32) for weight in (w_qkv, w_out, w_up, w_down, norm_gains, model_biases, attn_biases, ff_gain, ff_biases, head_scale)))

    def forward(sequence_inputs, weight_set):

        def single(sequence_pair):
            return jax.checkpoint(one_sequence)(sequence_pair[0], sequence_pair[1], weight_set)
        return lax.map(single, (sequence_inputs, lengths))
    output, pullback = jax.vjp(forward, inputs.astype(jnp.float32), params)
    grad_inputs, weight_grads = pullback(cotangent.astype(jnp.float32))
    return (output.astype(jnp.bfloat16), grad_inputs.astype(jnp.bfloat16), weight_grads[0], weight_grads[1], weight_grads[2], weight_grads[3], weight_grads[4], weight_grads[5], weight_grads[6], weight_grads[7], weight_grads[8], weight_grads[9])
```

```python
import jax
import jax.numpy as jnp
from jax import lax
from jax.experimental import pallas as pl
from jax.experimental.pallas import tpu as pltpu
from jax.sharding import PartitionSpec as P

H = 16
HD = 64


NORM_EPSILON = 1e-05


def layer_norm(vector, norm_gain, norm_bias):
    centered = vector - jnp.mean(vector, axis=-1, keepdims=True)
    spread = jnp.mean(centered * centered, axis=-1, keepdims=True)
    return centered * lax.rsqrt(spread + NORM_EPSILON) * norm_gain + norm_bias


def gelu_norm(hidden, norm_gain, norm_bias):
    return layer_norm(jax.nn.gelu(hidden, approximate=False), norm_gain, norm_bias)


def contract_rows(left, right):
    return lax.dot_general(
        left, right, (((0,), (0,)), ((), ())), preferred_element_type=jnp.float32
    )


def times_transposed(left, right):
    return lax.dot_general(
        left, right, (((1,), (1,)), ((), ())), preferred_element_type=jnp.float32
    )


def shards(
    inputs,
    lengths,
    w_qkv,
    w_out,
    w_up,
    w_down,
    norm_gains,
    model_biases,
    attn_biases,
    ff_gain,
    ff_biases,
    head_scale,
    cotangent,
):
    gathered = (
        lax.all_gather(w_qkv, ("seq", "batch"), axis=0, tiled=True),
        lax.all_gather(w_out, ("seq", "batch"), axis=0, tiled=True),
        lax.all_gather(w_up, ("seq", "batch"), axis=0, tiled=True),
        lax.all_gather(w_down, ("seq", "batch"), axis=0, tiled=True),
        lax.all_gather(norm_gains, ("seq", "batch"), axis=1, tiled=True),
        lax.all_gather(model_biases, ("seq", "batch"), axis=1, tiled=True),
        lax.all_gather(attn_biases, ("seq", "batch"), axis=1, tiled=True),
        lax.all_gather(ff_gain, ("seq", "batch"), axis=0, tiled=True),
        lax.all_gather(ff_biases, ("seq", "batch"), axis=1, tiled=True),
    )
    qkv_full, out_full, up_full, down_full = (gathered[0], gathered[1], gathered[2], gathered[3])
    gain_rows = gathered[4].astype(jnp.float32)
    bias_rows = gathered[5].astype(jnp.float32)
    attn_rows = gathered[6].astype(jnp.float32)
    ffn_gain = gathered[7].astype(jnp.float32)
    ffn_rows = gathered[8].astype(jnp.float32)
    scales = head_scale.astype(jnp.float32)
    local_rows = inputs.shape[1]
    model_width = inputs.shape[2]
    seq_length = local_rows * lax.axis_size("seq")
    tile_rows = min(512, seq_length)
    first_row = lax.axis_index("seq") * local_rows
    valid_rows = lengths[0]
    positions = first_row + jnp.arange(local_rows, dtype=jnp.int32)
    valid_mask = (positions < valid_rows)[:, None]
    score_scale = HD ** (-0.5)
    residual_in = inputs[0].astype(jnp.float32)
    normed, norm_a_pull = jax.vjp(layer_norm, residual_in, gain_rows[0], bias_rows[0])
    normed_low = normed.astype(jnp.bfloat16)
    offsets = jnp.concatenate([bias_rows[3], jnp.zeros_like(bias_rows[3]), attn_rows[0]])
    projected = (
        jnp.dot(normed_low, qkv_full, preferred_element_type=jnp.float32) + offsets
    ).astype(jnp.bfloat16)
    queries = projected[:, :model_width]
    key_local = projected[:, model_width : 2 * model_width]
    value_local = projected[:, 2 * model_width :]
    key_rows, value_rows = (
        lax.all_gather(key_local, "seq", axis=0, tiled=True),
        lax.all_gather(value_local, "seq", axis=0, tiled=True),
    )
    query_heads = queries.reshape(local_rows, H, HD)
    last_needed = jnp.minimum(first_row + local_rows - 1, valid_rows - 1)
    tile_count = last_needed // tile_rows + 1

    def tile_scores(j):
        start = j * tile_rows
        key_tile = lax.dynamic_slice_in_dim(key_rows, start, tile_rows, 0).reshape(tile_rows, H, HD)
        scores = (
            jnp.einsum("qhd,khd->hqk", query_heads, key_tile, preferred_element_type=jnp.float32)
            * score_scale
        )
        key_index = start + jnp.arange(tile_rows, dtype=jnp.int32)
        allowed = (key_index[None, :] <= positions[:, None]) & (key_index[None, :] < valid_rows)
        return (scores, allowed[None], key_tile)

    def max_and_sum(j, carry):
        running_max, running_sum = carry
        scores, allowed, unused_tile = tile_scores(j)
        masked = jnp.where(allowed, scores, -1e30)
        new_max = jnp.maximum(running_max, jnp.max(masked, axis=-1))
        kept_terms = jnp.where(allowed, jnp.exp(masked - new_max[..., None]), 0.0)
        return (
            new_max,
            running_sum * jnp.exp(running_max - new_max) + jnp.sum(kept_terms, axis=-1),
        )

    start_stats = (
        jnp.full((H, local_rows), -1e30, jnp.float32),
        jnp.zeros((H, local_rows), jnp.float32),
    )
    running_max, running_sum = lax.fori_loop(0, tile_count, max_and_sum, start_stats)
    log_total = running_max + jnp.log(running_sum)

    def tile_probs(j):
        scores, allowed, key_tile = tile_scores(j)
        attn_probs = jnp.where(allowed, jnp.exp(scores - log_total[..., None]), 0.0)
        value_tile = lax.dynamic_slice_in_dim(value_rows, j * tile_rows, tile_rows, 0).reshape(
            tile_rows, H, HD
        )
        return (attn_probs, key_tile, value_tile)

    def accumulate(j, summed):
        attn_probs, unused_tile, value_tile = tile_probs(j)
        return summed + jnp.einsum(
            "hqk,khd->qhd",
            attn_probs.astype(jnp.bfloat16),
            value_tile,
            preferred_element_type=jnp.float32,
        )

    attended = lax.fori_loop(0, tile_count, accumulate, jnp.zeros((local_rows, H, HD), jnp.float32))
    scaled_low = (
        (attended * scales[None, :, None]).reshape(local_rows, model_width).astype(jnp.bfloat16)
    )
    attn_proj = jnp.dot(scaled_low, out_full, preferred_element_type=jnp.float32) + attn_rows[1]
    attn_normed, norm_b_pull = jax.vjp(layer_norm, attn_proj, gain_rows[1], bias_rows[1])
    residual = residual_in + attn_normed
    ffn_in, norm_c_pull = jax.vjp(layer_norm, residual, gain_rows[2], bias_rows[2])
    ffn_low = ffn_in.astype(jnp.bfloat16)
    hidden = jnp.dot(ffn_low, up_full, preferred_element_type=jnp.float32) + ffn_rows[0]
    ffn_normed, ffn_pull = jax.vjp(gelu_norm, hidden, ffn_gain, ffn_rows[1])
    ffn_out_low = ffn_normed.astype(jnp.bfloat16)
    combined = jnp.where(
        valid_mask,
        residual
        + jnp.dot(ffn_out_low, down_full, preferred_element_type=jnp.float32)
        + bias_rows[4],
        0.0,
    )
    output = combined.astype(jnp.bfloat16)[None]
    barrier_out = lax.optimization_barrier(((w_qkv, w_out, w_up, w_down), combined))
    regathered = (
        lax.all_gather(barrier_out[0][0], ("seq", "batch"), axis=0, tiled=True),
        lax.all_gather(barrier_out[0][1], ("seq", "batch"), axis=0, tiled=True),
        lax.all_gather(barrier_out[0][2], ("seq", "batch"), axis=0, tiled=True),
        lax.all_gather(barrier_out[0][3], ("seq", "batch"), axis=0, tiled=True),
    )
    qkv_full, out_full, up_full, down_full = (
        regathered[0],
        regathered[1],
        regathered[2],
        regathered[3],
    )
    cotan_rows = jnp.where(valid_mask, cotangent[0], jnp.zeros_like(cotangent[0]))
    cotan_float = cotan_rows.astype(jnp.float32)
    grad_down = contract_rows(ffn_out_low, cotan_rows)
    grad_bias_out = jnp.sum(cotan_float, axis=0)
    grad_ffn_normed = times_transposed(cotan_rows, down_full)
    grad_hidden, grad_ffn_gain, grad_ffn_shift = ffn_pull(grad_ffn_normed)
    grad_hidden_low = grad_hidden.astype(jnp.bfloat16)
    grad_up = contract_rows(ffn_low, grad_hidden_low)
    grad_ffn_bias = jnp.sum(grad_hidden_low.astype(jnp.float32), axis=0)
    grad_ffn_in = times_transposed(grad_hidden_low, up_full)
    grad_from_ffn, grad_gain_c, grad_shift_c = norm_c_pull(grad_ffn_in)
    grad_residual = cotan_float + grad_from_ffn
    grad_proj, grad_gain_b, grad_shift_b = norm_b_pull(grad_residual)
    grad_proj_low = grad_proj.astype(jnp.bfloat16)
    grad_out_bias = jnp.sum(grad_proj_low.astype(jnp.float32), axis=0)
    grad_out = contract_rows(scaled_low, grad_proj_low)
    grad_scaled = times_transposed(grad_proj_low, out_full).reshape(local_rows, H, HD)
    grad_scales = jnp.sum(grad_scaled * attended, axis=(0, 2))
    grad_heads_low = (grad_scaled * scales[None, :, None]).astype(jnp.bfloat16)
    row_delta = jnp.einsum("qhd,qhd->hq", grad_heads_low.astype(jnp.float32), attended)

    def score_grads(j):
        attn_probs, key_tile, value_tile = tile_probs(j)
        grad_probs = jnp.einsum(
            "qhd,khd->hqk", grad_heads_low, value_tile, preferred_element_type=jnp.float32
        )
        grad_scores = (attn_probs * (grad_probs - row_delta[..., None])).astype(jnp.bfloat16)
        return (attn_probs, grad_scores, key_tile)

    def backward_tile(j, carry):
        grad_query, terms = carry
        attn_probs, grad_scores, key_tile = score_grads(j)
        grad_query = grad_query + jnp.einsum(
            "hqk,khd->qhd", grad_scores, key_tile, preferred_element_type=jnp.float32
        )
        grad_key = (
            jnp.einsum("hqk,qhd->khd", grad_scores, query_heads, preferred_element_type=jnp.float32)
            * score_scale
        )
        grad_value = jnp.einsum(
            "hqk,qhd->khd",
            attn_probs.astype(jnp.bfloat16),
            grad_heads_low,
            preferred_element_type=jnp.float32,
        )
        piece = jnp.concatenate(
            [grad_key.reshape(tile_rows, model_width), grad_value.reshape(tile_rows, model_width)],
            axis=1,
        )
        return (grad_query, lax.dynamic_update_slice_in_dim(terms, piece, j * tile_rows, 0))

    start_carry = (
        jnp.zeros((local_rows, H, HD), jnp.float32),
        jnp.zeros((seq_length, 2 * model_width), jnp.float32),
    )
    grad_query, terms = lax.fori_loop(0, tile_count, backward_tile, start_carry)
    grad_kv = lax.psum_scatter(terms, "seq", scatter_dimension=0, tiled=True)
    grad_query_low = (
        (grad_query * score_scale).reshape(local_rows, model_width).astype(jnp.bfloat16)
    )
    grad_kv_low = grad_kv.astype(jnp.bfloat16)
    grad_projected = jnp.concatenate([grad_query_low, grad_kv_low], axis=1)
    grad_qkv = contract_rows(normed_low, grad_projected)
    grad_query_bias = jnp.sum(grad_query_low.astype(jnp.float32), axis=0)
    grad_value_bias = jnp.sum(grad_kv_low[:, model_width:].astype(jnp.float32), axis=0)
    grad_normed = times_transposed(grad_projected, qkv_full)
    grad_from_attn, grad_gain_a, grad_shift_a = norm_a_pull(grad_normed)
    grad_input = (grad_residual + grad_from_attn).astype(jnp.bfloat16)[None]
    reduced = (
        lax.psum_scatter(grad_qkv, ("seq", "batch"), scatter_dimension=0, tiled=True),
        lax.psum_scatter(grad_out, ("seq", "batch"), scatter_dimension=0, tiled=True),
        lax.psum_scatter(grad_up, ("seq", "batch"), scatter_dimension=0, tiled=True),
        lax.psum_scatter(grad_down, ("seq", "batch"), scatter_dimension=0, tiled=True),
        lax.psum_scatter(
            jnp.stack([grad_gain_a, grad_gain_b, grad_gain_c]),
            ("seq", "batch"),
            scatter_dimension=1,
            tiled=True,
        ),
        lax.psum_scatter(
            jnp.stack([grad_shift_a, grad_shift_b, grad_shift_c, grad_query_bias, grad_bias_out]),
            ("seq", "batch"),
            scatter_dimension=1,
            tiled=True,
        ),
        lax.psum_scatter(
            jnp.stack([grad_value_bias, grad_out_bias]),
            ("seq", "batch"),
            scatter_dimension=1,
            tiled=True,
        ),
        lax.psum_scatter(grad_ffn_gain, ("seq", "batch"), scatter_dimension=0, tiled=True),
        lax.psum_scatter(
            jnp.stack([grad_ffn_bias, grad_ffn_shift]),
            ("seq", "batch"),
            scatter_dimension=1,
            tiled=True,
        ),
    )
    scale_total = lax.psum(grad_scales, ("seq", "batch"))
    return (
        output,
        grad_input,
        reduced[0],
        reduced[1],
        reduced[2],
        reduced[3],
        reduced[4],
        reduced[5],
        reduced[6],
        reduced[7],
        reduced[8],
        scale_total,
    )


class Exchange:
    def __init__(self, send_sems, recv_sems, local_sems, scratches):
        self.send_sems = send_sems
        self.recv_sems = recv_sems
        self.local_sems = local_sems
        self.scratches = scratches
        self.count = 0
        self.locals = 0
        self.sent = []
        self.open_recv = []
        self.s = lax.axis_index("seq")
        self.b = lax.axis_index("batch")
        self.chip = self.s // 2
        self.core = self.s % 2
        self.sibling = self.chip * 2 + 1 - self.core

    def send(self, src, dst, seq, batch):
        at = self.count
        self.count += 1
        copy = pltpu.make_async_remote_copy(
            src_ref=src,
            dst_ref=dst,
            send_sem=self.send_sems.at[at],
            recv_sem=self.recv_sems.at[at],
            device_id=(seq, batch),
            device_id_type=pl.DeviceIdType.MESH,
        )
        copy.start()
        self.sent.append(copy)
        self.open_recv.append(copy)
        return copy

    def arrived(self, copy):
        copy.wait_recv()
        self.open_recv = [one for one in self.open_recv if one is not copy]

    def local(self, src, dst):
        at = self.locals
        self.locals += 1
        inward = pltpu.make_async_copy(src, self.scratches[at], self.local_sems.at[2 * at])
        inward.start()
        return (inward, at, dst)

    def local_out(self, held):
        inward, at, dst = held
        inward.wait()
        outward = pltpu.make_async_copy(self.scratches[at], dst, self.local_sems.at[2 * at + 1])
        outward.start()
        return outward

    def finish(self):
        for copy in self.open_recv:
            copy.wait_recv()
        for copy in self.sent:
            copy.wait_send()

    def peer(self, k):
        return ((self.chip + k) % 4) * 2 + self.core

    def source(self, k):
        return ((self.chip + 4 - k) % 4) * 2 + self.core

    def gather_start(self, src, slot):
        copies = [self.send(src, slot(self.s), self.peer(k), self.b) for k in (1, 2, 3)]
        self.send(src, slot(self.s), self.sibling, self.b)
        return copies

    def gather_forward(self, copies, slot):
        for k in (1, 2, 3):
            self.arrived(copies[k - 1])
            came = slot(self.source(k))
            self.send(came, came, self.sibling, self.b)


def run_exchange(name, collective_id, plan, operands, out_shapes, scratch, copies, everyone=False):
    ins = len(operands)
    outs = len(out_shapes)

    def kernel(*refs):
        in_refs = refs[:ins]
        out_refs = refs[ins : ins + outs]
        scratches = refs[ins + outs : ins + outs + len(scratch)]
        send_sems, recv_sems, local_sems = refs[ins + outs + len(scratch) :]
        s = lax.axis_index("seq")
        b = lax.axis_index("batch")
        barrier = pltpu.get_barrier_semaphore()
        if everyone:
            partners = [((s + j // 4) % 8, (b + j % 4) % 4) for j in range(1, 32)]
        else:
            partners = [((s + j) % 8, b) for j in range(1, 8)] + [
                (s, (b + k) % 4) for k in range(1, 4)
            ]
        for seq, batch in partners:
            pl.semaphore_signal(
                barrier, inc=1, device_id=(seq, batch), device_id_type=pl.DeviceIdType.MESH
            )
        pl.semaphore_wait(barrier, len(partners))
        exchange = Exchange(send_sems, recv_sems, local_sems, scratches)
        plan(exchange, in_refs, out_refs)
        exchange.finish()

    return pl.pallas_call(
        kernel,
        name=name,
        out_shape=[jax.ShapeDtypeStruct(shape, dtype) for shape, dtype in out_shapes],
        in_specs=[pl.BlockSpec(memory_space=pl.ANY)] * ins,
        out_specs=[pl.BlockSpec(memory_space=pl.ANY)] * outs,
        scratch_shapes=[pltpu.VMEM(shape, dtype) for shape, dtype in scratch]
        + [
            pltpu.SemaphoreType.DMA((copies,)),
            pltpu.SemaphoreType.DMA((copies,)),
            pltpu.SemaphoreType.DMA((max(2 * len(scratch), 1),)),
        ],
        compiler_params=pltpu.CompilerParams(
            collective_id=collective_id, has_side_effects=True, vmem_limit_bytes=16 * 2**20
        ),
    )(*operands)


def columns(start, size):
    return pl.ds(pl.multiple_of(start, 128), size)


BF = jnp.bfloat16
F32 = jnp.float32


def opening_plan(ex, ins, outs):
    x_in, g_in, qkv_in, out_in, up_in, down_in, vec_in = ins
    x_out, g_out, qkv_out, w_out, up_out, down_out, vec_out = outs
    s, b = ex.s, ex.b
    for j in range(1, 32):
        ex.send(vec_in, vec_out.at[s * 4 + b], (s + j // 4) % 8, (b + j % 4) % 4)
    qkv_copies, up_copies = [], []
    for j in range(1, 8):
        p = (s + j) % 8
        for t in range(3):
            qkv_copies.append(
                ex.send(
                    qkv_in.at[:, columns(t * 1024 + p * 128, 128)],
                    qkv_out.at[s, b, :, pl.ds(t * 128, 128)],
                    p,
                    b,
                )
            )
    for j in range(1, 8):
        p = (s + j) % 8
        up_copies.append(ex.send(up_in.at[:, columns(p * 512, 512)], up_out.at[s, b], p, b))
    out_copies = [ex.send(out_in, w_out.at[s, b], s, (b + k) % 4) for k in (1, 2, 3)]
    x_slot = lambda i: x_out.at[i]
    g_slot = lambda i: g_out.at[i]
    out_slot = lambda i: w_out.at[i]
    x_copies = ex.gather_start(x_in, x_slot)
    held = [ex.local(qkv_in.at[:, columns(t * 1024 + s * 128, 128)], qkv_out.at[s, b, :, pl.ds(t * 128, 128)]) for t in range(3)]
    held.append(ex.local(up_in.at[:, columns(s * 512, 512)], up_out.at[s, b]))
    held.append(ex.local(out_in, w_out.at[s, b]))
    held.append(ex.local(x_in, x_out.at[s]))
    held.append(ex.local(g_in, g_out.at[s]))
    held.append(ex.local(down_in, down_out.at[b]))
    held.append(ex.local(vec_in, vec_out.at[s * 4 + b]))
    done = [ex.local_out(one) for one in held]
    for copy in qkv_copies:
        ex.arrived(copy)
    for one in done:
        one.wait()
    for k in (1, 2, 3):
        ex.send(qkv_out.at[:, b], qkv_out.at[:, b], s, (b + k) % 4)
    for copy in up_copies:
        ex.arrived(copy)
    for k in (1, 2, 3):
        ex.send(up_out.at[:, b], up_out.at[:, b], s, (b + k) % 4)
    for k in (1, 2, 3):
        ex.send(down_in, down_out.at[b], s, (b + k) % 4)
    g_copies = ex.gather_start(g_in, g_slot)
    ex.gather_forward(x_copies, x_slot)
    for copy in out_copies:
        ex.arrived(copy)
    out_copies = ex.gather_start(w_out.at[s], out_slot)
    ex.gather_forward(g_copies, g_slot)
    ex.gather_forward(out_copies, out_slot)


def heads_to_rows_plan(ex, ins, outs):
    (src,), (dst,) = ins, outs
    for j in range(1, 8):
        p = (ex.s + j) % 8
        ex.send(src.at[p], dst.at[:, columns(ex.s * 128, 128)], p, ex.b)
    ex.local_out(ex.local(src.at[ex.s], dst.at[:, columns(ex.s * 128, 128)])).wait()


def gather_plan(ex, ins, outs):
    (src,), (dst,) = ins, outs
    slot = lambda i: dst.at[i]
    copies = ex.gather_start(src, slot)
    out = ex.local_out(ex.local(src, dst.at[ex.s]))
    ex.gather_forward(copies, slot)
    out.wait()


def stats_plan(ex, ins, outs):
    (src,), (dst,) = ins, outs
    for j in range(1, 8):
        ex.send(src, dst.at[ex.s], (ex.s + j) % 8, ex.b)
    ex.local_out(ex.local(src, dst.at[ex.s])).wait()


def blocks_plan(ex, ins, outs):
    done = []
    for src, dst in zip(ins, outs):
        for j in range(1, 8):
            p = (ex.s + j) % 8
            ex.send(src.at[p], dst.at[ex.s], p, ex.b)
        done.append(ex.local(src.at[ex.s], dst.at[ex.s]))
    done = [ex.local_out(one) for one in done]
    for one in done:
        one.wait()


def rows_to_heads_plan(ex, ins, outs):
    (do_in, da_in), (do_out, da_out) = ins, outs
    for j in range(1, 8):
        p = (ex.s + j) % 8
        ex.send(do_in.at[:, columns(p * 128, 128)], do_out.at[ex.s], p, ex.b)
    slot = lambda i: da_out.at[i]
    copies = ex.gather_start(da_in, slot)
    held = [
        ex.local(do_in.at[:, columns(ex.s * 128, 128)], do_out.at[ex.s]),
        ex.local(da_in, da_out.at[ex.s]),
    ]
    done = [ex.local_out(one) for one in held]
    ex.gather_forward(copies, slot)
    for one in done:
        one.wait()


def grads_plan(ex, ins, outs):
    dh_in, qkv_in, out_in, up_in, down_in = ins
    dh_out, qkv_out, out_out, up_out, down_out = outs
    s, b = ex.s, ex.b
    for j in range(1, 8):
        p = (s + j) % 8
        ex.send(dh_in.at[p], dh_out.at[s], p, b)
    views = [
        (lambda q: qkv_in.at[:, q], qkv_out),
        (lambda q: out_in.at[q], out_out),
        (lambda q: up_in.at[:, q], up_out),
        (lambda q: down_in.at[q], down_out),
    ]
    for view, dst in views:
        for k in (1, 2, 3):
            q = (b + k) % 4
            ex.send(view(q), dst.at[b], s, q)
    held = [ex.local(dh_in.at[s], dh_out.at[s])] + [ex.local(view(b), dst.at[b]) for view, dst in views]
    done = [ex.local_out(one) for one in held]
    for one in done:
        one.wait()


def closing_plan(ex, ins, outs):
    vec_in, qkv_in, up_in = ins
    vec_out, qkv_out, up_out = outs
    s, b = ex.s, ex.b
    for j in range(1, 32):
        p, q = (s + j // 4) % 8, (b + j % 4) % 4
        ex.send(vec_in.at[p * 4 + q], vec_out.at[s * 4 + b], p, q)
    for j in range(1, 8):
        p = (s + j) % 8
        for t in range(3):
            ex.send(
                qkv_in.at[p, :, pl.ds(t * 128, 128)],
                qkv_out.at[:, columns(t * 1024 + s * 128, 128)],
                p,
                b,
            )
        ex.send(up_in.at[p], up_out.at[:, columns(s * 512, 512)], p, b)
    held = [ex.local(vec_in.at[s * 4 + b], vec_out.at[s * 4 + b])]
    held += [
        ex.local(qkv_in.at[s, :, pl.ds(t * 128, 128)], qkv_out.at[:, columns(t * 1024 + s * 128, 128)])
        for t in range(3)
    ]
    held.append(ex.local(up_in.at[s], up_out.at[:, columns(s * 512, 512)]))
    done = [ex.local_out(one) for one in held]
    for one in done:
        one.wait()


def centred(rows):
    middle = rows - jnp.mean(rows, axis=-1, keepdims=True)
    inverse = lax.rsqrt(jnp.mean(middle * middle, axis=-1, keepdims=True) + NORM_EPSILON)
    return middle * inverse, inverse


def norm_back(upstream, gain, normal, inverse):
    scaled = upstream * gain
    average = jnp.mean(scaled, axis=-1, keepdims=True)
    along = jnp.mean(scaled * normal, axis=-1, keepdims=True)
    return inverse * (scaled - average - normal * along)


def gelu_parts(z):
    phi = 0.5 * (1.0 + lax.erf(z * 0.7071067811865476))
    density = 0.3989422804014327 * jnp.exp(-0.5 * z * z)
    return z * phi, phi + z * density


def plane_shards(
    inputs,
    lengths,
    w_qkv,
    w_out,
    w_up,
    w_down,
    norm_gains,
    model_biases,
    attn_biases,
    ff_gain,
    ff_biases,
    head_scale,
    cotangent,
):
    s = lax.axis_index("seq")
    valid_rows = lengths[0]
    positions = s * 128 + jnp.arange(128, dtype=jnp.int32)
    valid_mask = (positions < valid_rows)[:, None]
    all_rows = jnp.arange(1024, dtype=jnp.int32)
    packed = jnp.concatenate(
        [
            norm_gains.reshape(-1),
            model_biases.reshape(-1),
            attn_biases.reshape(-1),
            ff_gain,
            ff_biases.reshape(-1),
            jnp.zeros((2048 - 704,), BF),
        ]
    ).reshape(16, 128)
    x_all, g_all, qkv_w, out_w, up_w, down_w, vectors = run_exchange(
        "opening",
        1,
        opening_plan,
        [inputs[0], cotangent[0], w_qkv, w_out, w_up, w_down, packed],
        [
            ((8, 128, 1024), BF),
            ((8, 128, 1024), BF),
            ((8, 4, 32, 384), BF),
            ((8, 4, 32, 1024), BF),
            ((8, 4, 32, 512), BF),
            ((4, 128, 1024), BF),
            ((32, 16, 128), BF),
        ],
        [((32, 128), BF)] * 3
        + [((32, 512), BF), ((32, 1024), BF), ((128, 1024), BF), ((128, 1024), BF), ((128, 1024), BF), ((16, 128), BF)],
        100,
        everyone=True,
    )
    x_all = x_all.reshape(1024, 1024)
    g_all = jnp.where((all_rows < valid_rows)[:, None], g_all.reshape(1024, 1024), jnp.zeros((), BF))
    qkv_w = qkv_w.reshape(1024, 384)
    out_w = out_w.reshape(1024, 1024)
    up_w = up_w.reshape(1024, 512)
    down_w = down_w.reshape(512, 1024)
    flat = vectors.reshape(32, 2048).astype(F32)
    take = lambda at, n, w: flat[:, at : at + n * w].reshape(32, n, w).transpose(1, 0, 2).reshape(n, 32 * w)
    gains = take(0, 3, 32)
    biases = take(96, 5, 32)
    attn_b = take(256, 2, 32)
    own = lax.dynamic_slice_in_dim(flat, s * 4, 4, 0)
    take_own = lambda at, n, w: own[:, at : at + n * w].reshape(4, n, w).transpose(1, 0, 2).reshape(n, 4 * w)
    ffn_gain = take_own(320, 1, 128)[0]
    ffn_b = take_own(448, 2, 128)
    scales = head_scale.astype(F32)
    own_scales = lax.dynamic_slice_in_dim(scales, s * 2, 2, 0)
    own_scale_row = jnp.repeat(own_scales, HD)
    scale_row = jnp.repeat(scales, HD)

    normal_a_all, _ = centred(x_all.astype(F32))
    h1 = (normal_a_all * gains[0] + biases[0]).astype(BF)
    query_bias = lax.dynamic_slice_in_dim(biases[3], s * 128, 128, 0)
    value_bias = lax.dynamic_slice_in_dim(attn_b[0], s * 128, 128, 0)
    offsets = jnp.concatenate([query_bias, jnp.zeros((128,), F32), value_bias])
    qkv = (jnp.dot(h1, qkv_w, preferred_element_type=F32) + offsets).astype(BF)
    heads = qkv.reshape(1024, 3, 2, HD).transpose(1, 2, 0, 3)
    q, k, v = heads[0], heads[1], heads[2]
    score_scale = HD ** (-0.5)
    allowed = (all_rows[None, :] <= all_rows[:, None]) & (all_rows[None, :] < valid_rows)
    scores = jnp.einsum("hqd,hkd->hqk", q, k, preferred_element_type=F32) * score_scale
    masked = jnp.where(allowed[None], scores, -1e30)
    top = jnp.max(masked, axis=-1, keepdims=True)
    raised = jnp.exp(masked - top)
    total = jnp.sum(raised, axis=-1, keepdims=True)
    log_total = top + jnp.log(total)
    probs = jnp.exp(masked - log_total)
    probs_low = probs.astype(BF)
    attended = jnp.einsum("hqk,hkd->hqd", probs_low, v, preferred_element_type=F32)
    scaled = (attended * own_scales[:, None, None]).astype(BF)
    scaled_rows = scaled.transpose(1, 0, 2).reshape(1024, 128)
    (scaled_local,) = run_exchange(
        "heads_to_rows", 2, heads_to_rows_plan, [scaled_rows.reshape(8, 128, 128)], [((128, 1024), BF)], [((128, 128), BF)], 8
    )

    residual_in = inputs[0].astype(F32)
    attn_proj = jnp.dot(scaled_local, out_w, preferred_element_type=F32) + attn_b[1]
    normal_b, inverse_b = centred(attn_proj)
    residual = residual_in + normal_b * gains[1] + biases[1]
    normal_c, inverse_c = centred(residual)
    h2_local = (normal_c * gains[2] + biases[2]).astype(BF)
    (h2,) = run_exchange("gather_h2", 3, gather_plan, [h2_local], [((8, 128, 1024), BF)], [((128, 1024), BF)], 8)
    h2 = h2.reshape(1024, 1024)

    hidden = jnp.dot(h2, up_w, preferred_element_type=F32) + ffn_b[0]
    active, slope = gelu_parts(hidden)
    du2 = times_transposed(g_all, down_w)
    dgain = du2 * ffn_gain
    local_mean = jnp.mean(active, axis=-1)
    off = active - local_mean[:, None]
    stats = jnp.stack(
        [local_mean, jnp.sum(off * off, axis=-1), jnp.sum(dgain, axis=-1), jnp.sum(dgain * off, axis=-1)]
    )
    (stats_all,) = run_exchange(
        "stats", 4, stats_plan, [stats.reshape(32, 128)], [((8, 32, 128), F32)], [((32, 128), F32)], 8
    )
    stats_all = stats_all.reshape(8, 4, 1024)
    means = stats_all[:, 0]
    mean = jnp.mean(means, axis=0)
    shift = means - mean[None]
    spread = (jnp.sum(stats_all[:, 1], axis=0) + 512.0 * jnp.sum(shift * shift, axis=0)) / 4096.0
    inverse = lax.rsqrt(spread + NORM_EPSILON)
    average = jnp.sum(stats_all[:, 2], axis=0) / 4096.0
    along = inverse * jnp.sum(stats_all[:, 3] + shift * stats_all[:, 2], axis=0) / 4096.0
    normal_f = (active - mean[:, None]) * inverse[:, None]
    u2 = (normal_f * ffn_gain + ffn_b[1]).astype(BF)
    dz = (inverse[:, None] * (dgain - average[:, None] - normal_f * along[:, None]) * slope).astype(BF)
    grad_ffn_gain = jnp.sum(du2 * normal_f, axis=0)
    grad_ffn_shift = jnp.sum(du2, axis=0)
    grad_ffn_bias = jnp.sum(dz.astype(F32), axis=0)
    ffo_part = jnp.dot(u2, down_w, preferred_element_type=F32).astype(BF)
    dh2_part = times_transposed(dz, up_w).astype(BF)
    dh2_blocks, ffo_blocks = run_exchange(
        "sum_ff",
        5,
        blocks_plan,
        [dh2_part.reshape(8, 128, 1024), ffo_part.reshape(8, 128, 1024)],
        [((8, 128, 1024), BF)] * 2,
        [((128, 1024), BF)] * 2,
        16,
    )
    grad_up = contract_rows(h2, dz)
    grad_down = contract_rows(u2, g_all)
    ffo = jnp.sum(ffo_blocks.astype(F32), axis=0)
    output = jnp.where(valid_mask, residual + ffo + biases[4], 0.0).astype(BF)[None]

    dh2 = jnp.sum(dh2_blocks.astype(F32), axis=0)
    g_local = jnp.where(valid_mask, cotangent[0], jnp.zeros((), BF)).astype(F32)
    dr = g_local + norm_back(dh2, gains[2], normal_c, inverse_c)
    da = norm_back(dr, gains[1], normal_b, inverse_b).astype(BF)
    dscaled = times_transposed(da, out_w)
    do_local = (dscaled * scale_row).astype(BF)
    do_blocks, da_all = run_exchange(
        "rows_to_heads",
        6,
        rows_to_heads_plan,
        [do_local, da],
        [((8, 128, 128), BF), ((8, 128, 1024), BF)],
        [((128, 128), BF), ((128, 1024), BF)],
        16,
    )
    da_all = da_all.reshape(1024, 1024)
    do_rows = do_blocks.reshape(1024, 128)
    do = do_rows.reshape(1024, 2, HD).transpose(1, 0, 2)
    grad_out = contract_rows(scaled_rows, da_all)

    delta = jnp.sum(do.astype(F32) * attended, axis=-1)
    grad_scales = jnp.sum(delta, axis=-1) / own_scales
    dp = jnp.einsum("hqd,hkd->hqk", do, v, preferred_element_type=F32)
    ds = (probs * (dp - delta[..., None])).astype(BF)
    dq = jnp.einsum("hqk,hkd->hqd", ds, k, preferred_element_type=F32) * score_scale
    dk = jnp.einsum("hqk,hqd->hkd", ds, q, preferred_element_type=F32) * score_scale
    dv = jnp.einsum("hqk,hqd->hkd", probs_low, do, preferred_element_type=F32)
    dqkv = jnp.stack([dq, dk, dv]).astype(BF).transpose(2, 0, 1, 3).reshape(1024, 384)
    column_sums = jnp.sum(dqkv.astype(F32), axis=0)
    grad_qkv = contract_rows(h1, dqkv)
    dh1_part = times_transposed(dqkv, qkv_w).astype(BF)
    dh1_blocks, qkv_terms, out_terms, up_terms, down_terms = run_exchange(
        "sum_grads",
        7,
        grads_plan,
        [
            dh1_part.reshape(8, 128, 1024),
            grad_qkv.astype(BF).reshape(8, 4, 32, 384),
            grad_out.astype(BF).reshape(4, 32, 1024),
            grad_up.astype(BF).reshape(8, 4, 32, 512),
            grad_down.astype(BF).reshape(4, 128, 1024),
        ],
        [
            ((8, 128, 1024), BF),
            ((4, 8, 32, 384), BF),
            ((4, 32, 1024), BF),
            ((4, 8, 32, 512), BF),
            ((4, 128, 1024), BF),
        ],
        [((128, 1024), BF), ((8, 32, 384), BF), ((32, 1024), BF), ((8, 32, 512), BF), ((128, 1024), BF)],
        20,
    )
    add = lambda terms: jnp.sum(terms.astype(F32), axis=0)
    grad_out_own = add(out_terms)
    grad_down_own = add(down_terms)
    dh1 = add(dh1_blocks)
    normal_a, inverse_a = centred(residual_in)
    grad_input = (dr + norm_back(dh1, gains[0], normal_a, inverse_a)).astype(BF)[None]

    place = lambda row: lax.dynamic_update_slice_in_dim(jnp.zeros((1024,), F32), row, s * 128, 0)
    place_ff = lambda rows: lax.dynamic_update_slice_in_dim(jnp.zeros((3, 4096), F32), rows, s * 512, 1)
    wide = jnp.stack(
        [
            jnp.sum(dh1 * normal_a, axis=0),
            jnp.sum(dr * normal_b, axis=0),
            jnp.sum(dh2 * normal_c, axis=0),
            jnp.sum(dh1, axis=0),
            jnp.sum(dr, axis=0),
            jnp.sum(dh2, axis=0),
            place(column_sums[:128]),
            jnp.sum(g_local, axis=0),
            place(column_sums[256:]),
            jnp.sum(da.astype(F32), axis=0),
        ]
    )
    ff_wide = place_ff(jnp.stack([grad_ffn_gain, grad_ffn_bias, grad_ffn_shift]))
    scale_wide = lax.dynamic_update_slice_in_dim(jnp.zeros((H,), F32), grad_scales, s * 2, 0)
    terms = jnp.concatenate(
        [
            wide.reshape(10, 32, 32).transpose(1, 0, 2).reshape(32, 320),
            ff_wide.reshape(3, 32, 128).transpose(1, 0, 2).reshape(32, 384),
            jnp.broadcast_to(scale_wide[None], (32, H)),
            jnp.zeros((32, 1024 - 720), F32),
        ],
        axis=1,
    ).reshape(32, 8, 128)
    vec_terms, qkv_own, up_own = run_exchange(
        "closing",
        8,
        closing_plan,
        [terms, add(qkv_terms).astype(BF), add(up_terms).astype(BF)],
        [((32, 8, 128), F32), ((32, 3072), BF), ((32, 4096), BF)],
        [((8, 128), F32)] + [((32, 128), BF)] * 3 + [((32, 512), BF)],
        64,
        everyone=True,
    )
    sums = jnp.sum(vec_terms, axis=0).reshape(1024)
    wide_sums = sums[:320].reshape(10, 32)
    ff_sums = sums[320:704].reshape(3, 128)
    return (
        output,
        grad_input,
        qkv_own.astype(F32),
        grad_out_own,
        up_own.astype(F32),
        grad_down_own,
        wide_sums[0:3],
        wide_sums[3:8],
        wide_sums[8:10],
        ff_sums[0],
        ff_sums[1:3],
        sums[704:720],
    )


def solution(mesh):
    in_plane = mesh.shape["seq"] == 8 and mesh.shape["batch"] == 4
    return jax.shard_map(
        plane_shards if in_plane else shards,
        mesh=mesh,
        in_specs=(
            P("batch", "seq", None),
            P("batch"),
            P(("seq", "batch"), None),
            P(("seq", "batch"), None),
            P(("seq", "batch"), None),
            P(("seq", "batch"), None),
            P(None, ("seq", "batch")),
            P(None, ("seq", "batch")),
            P(None, ("seq", "batch")),
            P(("seq", "batch")),
            P(None, ("seq", "batch")),
            P(),
            P("batch", "seq", None),
        ),
        out_specs=(
            P("batch", "seq", None),
            P("batch", "seq", None),
            P(("seq", "batch"), None),
            P(("seq", "batch"), None),
            P(("seq", "batch"), None),
            P(("seq", "batch"), None),
            P(None, ("seq", "batch")),
            P(None, ("seq", "batch")),
            P(None, ("seq", "batch")),
            P(("seq", "batch")),
            P(None, ("seq", "batch")),
            P(),
        ),
        check_vma=False,
    )
```

```python
import jax
import jax.numpy as jnp
from jax import lax
from jax.experimental import pallas as pl
from jax.experimental.pallas import tpu as pltpu
from jax.sharding import PartitionSpec as P

H = 16
HD = 64


NORM_EPSILON = 1e-05


def layer_norm(vector, norm_gain, norm_bias):
    centered = vector - jnp.mean(vector, axis=-1, keepdims=True)
    spread = jnp.mean(centered * centered, axis=-1, keepdims=True)
    return centered * lax.rsqrt(spread + NORM_EPSILON) * norm_gain + norm_bias


def gelu_norm(hidden, norm_gain, norm_bias):
    return layer_norm(jax.nn.gelu(hidden, approximate=False), norm_gain, norm_bias)


def contract_rows(left, right):
    return lax.dot_general(
        left, right, (((0,), (0,)), ((), ())), preferred_element_type=jnp.float32
    )


def times_transposed(left, right):
    return lax.dot_general(
        left, right, (((1,), (1,)), ((), ())), preferred_element_type=jnp.float32
    )


def shards(
    inputs,
    lengths,
    w_qkv,
    w_out,
    w_up,
    w_down,
    norm_gains,
    model_biases,
    attn_biases,
    ff_gain,
    ff_biases,
    head_scale,
    cotangent,
):
    gathered = (
        lax.all_gather(w_qkv, ("seq", "batch"), axis=0, tiled=True),
        lax.all_gather(w_out, ("seq", "batch"), axis=0, tiled=True),
        lax.all_gather(w_up, ("seq", "batch"), axis=0, tiled=True),
        lax.all_gather(w_down, ("seq", "batch"), axis=0, tiled=True),
        lax.all_gather(norm_gains, ("seq", "batch"), axis=1, tiled=True),
        lax.all_gather(model_biases, ("seq", "batch"), axis=1, tiled=True),
        lax.all_gather(attn_biases, ("seq", "batch"), axis=1, tiled=True),
        lax.all_gather(ff_gain, ("seq", "batch"), axis=0, tiled=True),
        lax.all_gather(ff_biases, ("seq", "batch"), axis=1, tiled=True),
    )
    qkv_full, out_full, up_full, down_full = (gathered[0], gathered[1], gathered[2], gathered[3])
    gain_rows = gathered[4].astype(jnp.float32)
    bias_rows = gathered[5].astype(jnp.float32)
    attn_rows = gathered[6].astype(jnp.float32)
    ffn_gain = gathered[7].astype(jnp.float32)
    ffn_rows = gathered[8].astype(jnp.float32)
    scales = head_scale.astype(jnp.float32)
    local_rows = inputs.shape[1]
    model_width = inputs.shape[2]
    seq_length = local_rows * lax.axis_size("seq")
    tile_rows = min(512, seq_length)
    first_row = lax.axis_index("seq") * local_rows
    valid_rows = lengths[0]
    positions = first_row + jnp.arange(local_rows, dtype=jnp.int32)
    valid_mask = (positions < valid_rows)[:, None]
    score_scale = HD ** (-0.5)
    residual_in = inputs[0].astype(jnp.float32)
    normed, norm_a_pull = jax.vjp(layer_norm, residual_in, gain_rows[0], bias_rows[0])
    normed_low = normed.astype(jnp.bfloat16)
    offsets = jnp.concatenate([bias_rows[3], jnp.zeros_like(bias_rows[3]), attn_rows[0]])
    projected = (
        jnp.dot(normed_low, qkv_full, preferred_element_type=jnp.float32) + offsets
    ).astype(jnp.bfloat16)
    queries = projected[:, :model_width]
    key_local = projected[:, model_width : 2 * model_width]
    value_local = projected[:, 2 * model_width :]
    key_rows, value_rows = (
        lax.all_gather(key_local, "seq", axis=0, tiled=True),
        lax.all_gather(value_local, "seq", axis=0, tiled=True),
    )
    query_heads = queries.reshape(local_rows, H, HD)
    last_needed = jnp.minimum(first_row + local_rows - 1, valid_rows - 1)
    tile_count = last_needed // tile_rows + 1

    def tile_scores(j):
        start = j * tile_rows
        key_tile = lax.dynamic_slice_in_dim(key_rows, start, tile_rows, 0).reshape(tile_rows, H, HD)
        scores = (
            jnp.einsum("qhd,khd->hqk", query_heads, key_tile, preferred_element_type=jnp.float32)
            * score_scale
        )
        key_index = start + jnp.arange(tile_rows, dtype=jnp.int32)
        allowed = (key_index[None, :] <= positions[:, None]) & (key_index[None, :] < valid_rows)
        return (scores, allowed[None], key_tile)

    def max_and_sum(j, carry):
        running_max, running_sum = carry
        scores, allowed, unused_tile = tile_scores(j)
        masked = jnp.where(allowed, scores, -1e30)
        new_max = jnp.maximum(running_max, jnp.max(masked, axis=-1))
        kept_terms = jnp.where(allowed, jnp.exp(masked - new_max[..., None]), 0.0)
        return (
            new_max,
            running_sum * jnp.exp(running_max - new_max) + jnp.sum(kept_terms, axis=-1),
        )

    start_stats = (
        jnp.full((H, local_rows), -1e30, jnp.float32),
        jnp.zeros((H, local_rows), jnp.float32),
    )
    running_max, running_sum = lax.fori_loop(0, tile_count, max_and_sum, start_stats)
    log_total = running_max + jnp.log(running_sum)

    def tile_probs(j):
        scores, allowed, key_tile = tile_scores(j)
        attn_probs = jnp.where(allowed, jnp.exp(scores - log_total[..., None]), 0.0)
        value_tile = lax.dynamic_slice_in_dim(value_rows, j * tile_rows, tile_rows, 0).reshape(
            tile_rows, H, HD
        )
        return (attn_probs, key_tile, value_tile)

    def accumulate(j, summed):
        attn_probs, unused_tile, value_tile = tile_probs(j)
        return summed + jnp.einsum(
            "hqk,khd->qhd",
            attn_probs.astype(jnp.bfloat16),
            value_tile,
            preferred_element_type=jnp.float32,
        )

    attended = lax.fori_loop(0, tile_count, accumulate, jnp.zeros((local_rows, H, HD), jnp.float32))
    scaled_low = (
        (attended * scales[None, :, None]).reshape(local_rows, model_width).astype(jnp.bfloat16)
    )
    attn_proj = jnp.dot(scaled_low, out_full, preferred_element_type=jnp.float32) + attn_rows[1]
    attn_normed, norm_b_pull = jax.vjp(layer_norm, attn_proj, gain_rows[1], bias_rows[1])
    residual = residual_in + attn_normed
    ffn_in, norm_c_pull = jax.vjp(layer_norm, residual, gain_rows[2], bias_rows[2])
    ffn_low = ffn_in.astype(jnp.bfloat16)
    hidden = jnp.dot(ffn_low, up_full, preferred_element_type=jnp.float32) + ffn_rows[0]
    ffn_normed, ffn_pull = jax.vjp(gelu_norm, hidden, ffn_gain, ffn_rows[1])
    ffn_out_low = ffn_normed.astype(jnp.bfloat16)
    combined = jnp.where(
        valid_mask,
        residual
        + jnp.dot(ffn_out_low, down_full, preferred_element_type=jnp.float32)
        + bias_rows[4],
        0.0,
    )
    output = combined.astype(jnp.bfloat16)[None]
    barrier_out = lax.optimization_barrier(((w_qkv, w_out, w_up, w_down), combined))
    regathered = (
        lax.all_gather(barrier_out[0][0], ("seq", "batch"), axis=0, tiled=True),
        lax.all_gather(barrier_out[0][1], ("seq", "batch"), axis=0, tiled=True),
        lax.all_gather(barrier_out[0][2], ("seq", "batch"), axis=0, tiled=True),
        lax.all_gather(barrier_out[0][3], ("seq", "batch"), axis=0, tiled=True),
    )
    qkv_full, out_full, up_full, down_full = (
        regathered[0],
        regathered[1],
        regathered[2],
        regathered[3],
    )
    cotan_rows = jnp.where(valid_mask, cotangent[0], jnp.zeros_like(cotangent[0]))
    cotan_float = cotan_rows.astype(jnp.float32)
    grad_down = contract_rows(ffn_out_low, cotan_rows)
    grad_bias_out = jnp.sum(cotan_float, axis=0)
    grad_ffn_normed = times_transposed(cotan_rows, down_full)
    grad_hidden, grad_ffn_gain, grad_ffn_shift = ffn_pull(grad_ffn_normed)
    grad_hidden_low = grad_hidden.astype(jnp.bfloat16)
    grad_up = contract_rows(ffn_low, grad_hidden_low)
    grad_ffn_bias = jnp.sum(grad_hidden_low.astype(jnp.float32), axis=0)
    grad_ffn_in = times_transposed(grad_hidden_low, up_full)
    grad_from_ffn, grad_gain_c, grad_shift_c = norm_c_pull(grad_ffn_in)
    grad_residual = cotan_float + grad_from_ffn
    grad_proj, grad_gain_b, grad_shift_b = norm_b_pull(grad_residual)
    grad_proj_low = grad_proj.astype(jnp.bfloat16)
    grad_out_bias = jnp.sum(grad_proj_low.astype(jnp.float32), axis=0)
    grad_out = contract_rows(scaled_low, grad_proj_low)
    grad_scaled = times_transposed(grad_proj_low, out_full).reshape(local_rows, H, HD)
    grad_scales = jnp.sum(grad_scaled * attended, axis=(0, 2))
    grad_heads_low = (grad_scaled * scales[None, :, None]).astype(jnp.bfloat16)
    row_delta = jnp.einsum("qhd,qhd->hq", grad_heads_low.astype(jnp.float32), attended)

    def score_grads(j):
        attn_probs, key_tile, value_tile = tile_probs(j)
        grad_probs = jnp.einsum(
            "qhd,khd->hqk", grad_heads_low, value_tile, preferred_element_type=jnp.float32
        )
        grad_scores = (attn_probs * (grad_probs - row_delta[..., None])).astype(jnp.bfloat16)
        return (attn_probs, grad_scores, key_tile)

    def backward_tile(j, carry):
        grad_query, terms = carry
        attn_probs, grad_scores, key_tile = score_grads(j)
        grad_query = grad_query + jnp.einsum(
            "hqk,khd->qhd", grad_scores, key_tile, preferred_element_type=jnp.float32
        )
        grad_key = (
            jnp.einsum("hqk,qhd->khd", grad_scores, query_heads, preferred_element_type=jnp.float32)
            * score_scale
        )
        grad_value = jnp.einsum(
            "hqk,qhd->khd",
            attn_probs.astype(jnp.bfloat16),
            grad_heads_low,
            preferred_element_type=jnp.float32,
        )
        piece = jnp.concatenate(
            [grad_key.reshape(tile_rows, model_width), grad_value.reshape(tile_rows, model_width)],
            axis=1,
        )
        return (grad_query, lax.dynamic_update_slice_in_dim(terms, piece, j * tile_rows, 0))

    start_carry = (
        jnp.zeros((local_rows, H, HD), jnp.float32),
        jnp.zeros((seq_length, 2 * model_width), jnp.float32),
    )
    grad_query, terms = lax.fori_loop(0, tile_count, backward_tile, start_carry)
    grad_kv = lax.psum_scatter(terms, "seq", scatter_dimension=0, tiled=True)
    grad_query_low = (
        (grad_query * score_scale).reshape(local_rows, model_width).astype(jnp.bfloat16)
    )
    grad_kv_low = grad_kv.astype(jnp.bfloat16)
    grad_projected = jnp.concatenate([grad_query_low, grad_kv_low], axis=1)
    grad_qkv = contract_rows(normed_low, grad_projected)
    grad_query_bias = jnp.sum(grad_query_low.astype(jnp.float32), axis=0)
    grad_value_bias = jnp.sum(grad_kv_low[:, model_width:].astype(jnp.float32), axis=0)
    grad_normed = times_transposed(grad_projected, qkv_full)
    grad_from_attn, grad_gain_a, grad_shift_a = norm_a_pull(grad_normed)
    grad_input = (grad_residual + grad_from_attn).astype(jnp.bfloat16)[None]
    reduced = (
        lax.psum_scatter(grad_qkv, ("seq", "batch"), scatter_dimension=0, tiled=True),
        lax.psum_scatter(grad_out, ("seq", "batch"), scatter_dimension=0, tiled=True),
        lax.psum_scatter(grad_up, ("seq", "batch"), scatter_dimension=0, tiled=True),
        lax.psum_scatter(grad_down, ("seq", "batch"), scatter_dimension=0, tiled=True),
        lax.psum_scatter(
            jnp.stack([grad_gain_a, grad_gain_b, grad_gain_c]),
            ("seq", "batch"),
            scatter_dimension=1,
            tiled=True,
        ),
        lax.psum_scatter(
            jnp.stack([grad_shift_a, grad_shift_b, grad_shift_c, grad_query_bias, grad_bias_out]),
            ("seq", "batch"),
            scatter_dimension=1,
            tiled=True,
        ),
        lax.psum_scatter(
            jnp.stack([grad_value_bias, grad_out_bias]),
            ("seq", "batch"),
            scatter_dimension=1,
            tiled=True,
        ),
        lax.psum_scatter(grad_ffn_gain, ("seq", "batch"), scatter_dimension=0, tiled=True),
        lax.psum_scatter(
            jnp.stack([grad_ffn_bias, grad_ffn_shift]),
            ("seq", "batch"),
            scatter_dimension=1,
            tiled=True,
        ),
    )
    scale_total = lax.psum(grad_scales, ("seq", "batch"))
    return (
        output,
        grad_input,
        reduced[0],
        reduced[1],
        reduced[2],
        reduced[3],
        reduced[4],
        reduced[5],
        reduced[6],
        reduced[7],
        reduced[8],
        scale_total,
    )


class Exchange:
    def __init__(self, send_sems, recv_sems, local_sems, scratches):
        self.send_sems = send_sems
        self.recv_sems = recv_sems
        self.local_sems = local_sems
        self.scratches = scratches
        self.count = 0
        self.locals = 0
        self.sent = []
        self.open_recv = []
        self.s = lax.axis_index("seq")
        self.b = lax.axis_index("batch")
        self.chip = self.s // 2
        self.core = self.s % 2
        self.sibling = self.chip * 2 + 1 - self.core

    def send(self, src, dst, seq, batch):
        at = self.count
        self.count += 1
        copy = pltpu.make_async_remote_copy(
            src_ref=src,
            dst_ref=dst,
            send_sem=self.send_sems.at[at],
            recv_sem=self.recv_sems.at[at],
            device_id=(seq, batch),
            device_id_type=pl.DeviceIdType.MESH,
        )
        copy.start()
        self.sent.append(copy)
        self.open_recv.append(copy)
        return copy

    def arrived(self, copy):
        copy.wait_recv()
        self.open_recv = [one for one in self.open_recv if one is not copy]

    def local(self, src, dst):
        at = self.locals
        self.locals += 1
        inward = pltpu.make_async_copy(src, self.scratches[at], self.local_sems.at[2 * at])
        inward.start()
        return (inward, at, dst)

    def local_out(self, held):
        inward, at, dst = held
        inward.wait()
        outward = pltpu.make_async_copy(self.scratches[at], dst, self.local_sems.at[2 * at + 1])
        outward.start()
        return outward

    def finish(self):
        for copy in self.open_recv:
            copy.wait_recv()
        for copy in self.sent:
            copy.wait_send()

    def peer(self, k):
        return ((self.chip + k) % 4) * 2 + self.core

    def source(self, k):
        return ((self.chip + 4 - k) % 4) * 2 + self.core

    def gather_start(self, src, slot):
        copies = [self.send(src, slot(self.s), self.peer(k), self.b) for k in (1, 2, 3)]
        self.send(src, slot(self.s), self.sibling, self.b)
        return copies

    def gather_forward(self, copies, slot):
        for k in (1, 2, 3):
            self.arrived(copies[k - 1])
            came = slot(self.source(k))
            self.send(came, came, self.sibling, self.b)


def run_exchange(
    name, collective_id, plan, operands, out_shapes, scratch, copies, everyone=False, near_in=(), near_out=()
):
    ins = len(operands)
    outs = len(out_shapes)

    def kernel(*refs):
        in_refs = refs[:ins]
        out_refs = refs[ins : ins + outs]
        scratches = refs[ins + outs : ins + outs + len(scratch)]
        send_sems, recv_sems, local_sems = refs[ins + outs + len(scratch) :]
        s = lax.axis_index("seq")
        b = lax.axis_index("batch")
        barrier = pltpu.get_barrier_semaphore()
        if everyone:
            partners = [((s + j // 4) % 8, (b + j % 4) % 4) for j in range(1, 32)]
        else:
            partners = [((s + j) % 8, b) for j in range(1, 8)] + [
                (s, (b + k) % 4) for k in range(1, 4)
            ]
        for seq, batch in partners:
            pl.semaphore_signal(
                barrier, inc=1, device_id=(seq, batch), device_id_type=pl.DeviceIdType.MESH
            )
        pl.semaphore_wait(barrier, len(partners))
        exchange = Exchange(send_sems, recv_sems, local_sems, scratches)
        plan(exchange, in_refs, out_refs)
        exchange.finish()

    return pl.pallas_call(
        kernel,
        name=name,
        out_shape=[jax.ShapeDtypeStruct(shape, dtype) for shape, dtype in out_shapes],
        in_specs=[
            pl.BlockSpec(memory_space=pltpu.VMEM if at in near_in else pl.ANY) for at in range(ins)
        ],
        out_specs=[
            pl.BlockSpec(memory_space=pltpu.VMEM if at in near_out else pl.ANY) for at in range(outs)
        ],
        scratch_shapes=[pltpu.VMEM(shape, dtype) for shape, dtype in scratch]
        + [
            pltpu.SemaphoreType.DMA((copies,)),
            pltpu.SemaphoreType.DMA((copies,)),
            pltpu.SemaphoreType.DMA((max(2 * len(scratch), 1),)),
        ],
        compiler_params=pltpu.CompilerParams(
            collective_id=collective_id, has_side_effects=True, vmem_limit_bytes=16 * 2**20
        ),
    )(*operands)


def columns(start, size):
    return pl.ds(pl.multiple_of(start, 128), size)


BF = jnp.bfloat16
F32 = jnp.float32


def opening_plan(ex, ins, outs):
    x_in, qkv_in, out_in, up_in, vec_in = ins
    x_out, qkv_out, w_out, up_out, vec_out = outs
    s, b = ex.s, ex.b
    for j in range(1, 32):
        ex.send(vec_in, vec_out.at[s * 4 + b], (s + j // 4) % 8, (b + j % 4) % 4)
    qkv_copies = []
    for j in range(1, 8):
        p = (s + j) % 8
        for t in range(3):
            qkv_copies.append(
                ex.send(
                    qkv_in.at[:, columns(t * 1024 + p * 128, 128)],
                    qkv_out.at[s, b, :, pl.ds(t * 128, 128)],
                    p,
                    b,
                )
            )
    out_copies = [ex.send(out_in, w_out.at[s, b], s, (b + k) % 4) for k in (1, 2, 3)]
    x_slot = lambda i: x_out.at[i]
    out_slot = lambda i: w_out.at[i]
    x_copies = ex.gather_start(x_in, x_slot)
    held = [
        ex.local(qkv_in.at[:, columns(t * 1024 + s * 128, 128)], qkv_out.at[s, b, :, pl.ds(t * 128, 128)])
        for t in range(3)
    ]
    held.append(ex.local(up_in.at[:, columns(s * 512, 512)], up_out.at[s]))
    held.append(ex.local(out_in, w_out.at[s, b]))
    held.append(ex.local(x_in, x_out.at[s]))
    held.append(ex.local(vec_in, vec_out.at[s * 4 + b]))
    done = [ex.local_out(one) for one in held]
    for copy in qkv_copies:
        ex.arrived(copy)
    for one in done:
        one.wait()
    for k in (1, 2, 3):
        ex.send(qkv_out.at[:, b], qkv_out.at[:, b], s, (b + k) % 4)
    for j in range(1, 8):
        p = (s + j) % 8
        ex.send(up_in.at[:, columns(p * 512, 512)], up_out.at[s], p, b)
    for copy in out_copies:
        ex.arrived(copy)
    out_copies = ex.gather_start(w_out.at[s], out_slot)
    ex.gather_forward(x_copies, x_slot)
    ex.gather_forward(out_copies, out_slot)


def heads_to_rows_plan(ex, ins, outs):
    (src,), (dst,) = ins, outs
    for j in range(1, 8):
        p = (ex.s + j) % 8
        ex.send(src.at[p], dst.at[:, columns(ex.s * 128, 128)], p, ex.b)
    ex.local_out(ex.local(src.at[ex.s], dst.at[:, columns(ex.s * 128, 128)])).wait()


def gather_plan(ex, ins, outs):
    (src,), (dst,) = ins, outs
    slot = lambda i: dst.at[i]
    copies = ex.gather_start(src, slot)
    out = ex.local_out(ex.local(src, dst.at[ex.s]))
    ex.gather_forward(copies, slot)
    out.wait()


def stats_plan(ex, ins, outs):
    (src,), (dst,) = ins, outs
    for j in range(1, 8):
        ex.send(src, dst.at[ex.s], (ex.s + j) % 8, ex.b)
    ex.local_out(ex.local(src, dst.at[ex.s])).wait()


def blocks_sum(ex, src, from_pair, paired, from_chips, total):
    chip, core = ex.chip, ex.core
    to_pair = []
    for k in (1, 2, 3, 0):
        other = (chip + k) % 4
        to_pair.append(ex.send(src.at[other * 2 + 1 - core], from_pair.at[k], ex.sibling, ex.b))
    over = []
    for k in (1, 2, 3, 0):
        ex.arrived(to_pair[(k + 3) % 4])
        mine = src[((chip + k) % 4) * 2 + core].astype(F32)
        both = mine + from_pair[k].astype(F32)
        if k:
            paired[k - 1] = both.astype(BF)
            over.append(ex.send(paired.at[k - 1], from_chips.at[k - 1], ex.peer(k), ex.b))
        else:
            total[...] = both
    for k in (1, 2, 3):
        ex.arrived(over[k - 1])
        total[...] += from_chips[k - 1].astype(F32)


def sum_ff_plan(ex, ins, outs):
    (src,), (total,) = ins, outs
    blocks_sum(ex, src, *ex.scratches, total)


def rows_to_heads_plan(ex, ins, outs):
    (do_in,), (do_out,) = ins, outs
    for j in range(1, 8):
        p = (ex.s + j) % 8
        ex.send(do_in.at[:, columns(p * 128, 128)], do_out.at[ex.s], p, ex.b)
    ex.local_out(ex.local(do_in.at[:, columns(ex.s * 128, 128)], do_out.at[ex.s])).wait()


def grads_plan(ex, ins, outs):
    dh_in, da_in, qkv_in = ins
    dh_total, da_out, qkv_out = outs
    s, b = ex.s, ex.b
    for k in (1, 2, 3):
        q = (b + k) % 4
        ex.send(qkv_in.at[:, q], qkv_out.at[b], s, q)
    slot = lambda i: da_out.at[i]
    held = [ex.local(da_in, da_out.at[s]), ex.local(qkv_in.at[:, b], qkv_out.at[b])]
    blocks_sum(ex, dh_in, *ex.scratches[2:], dh_total)
    copies = ex.gather_start(da_in, slot)
    done = [ex.local_out(one) for one in held]
    ex.gather_forward(copies, slot)
    for one in done:
        one.wait()


def closing_plan(ex, ins, outs):
    vec_in, qkv_in, up_in, out_in = ins
    vec_out, qkv_out, up_out, out_terms = outs
    s, b = ex.s, ex.b
    for j in range(1, 32):
        p, q = (s + j // 4) % 8, (b + j % 4) % 4
        ex.send(vec_in.at[p * 4 + q], vec_out.at[s * 4 + b], p, q)
    for j in range(1, 8):
        p = (s + j) % 8
        for t in range(3):
            ex.send(
                qkv_in.at[p, :, pl.ds(t * 128, 128)],
                qkv_out.at[:, columns(t * 1024 + s * 128, 128)],
                p,
                b,
            )
        ex.send(up_in.at[p], up_out.at[:, columns(s * 512, 512)], p, b)
    for k in (1, 2, 3):
        q = (b + k) % 4
        ex.send(out_in.at[q], out_terms.at[b], s, q)
    held = [ex.local(vec_in.at[s * 4 + b], vec_out.at[s * 4 + b])]
    held += [
        ex.local(qkv_in.at[s, :, pl.ds(t * 128, 128)], qkv_out.at[:, columns(t * 1024 + s * 128, 128)])
        for t in range(3)
    ]
    held.append(ex.local(up_in.at[s], up_out.at[:, columns(s * 512, 512)]))
    held.append(ex.local(out_in.at[b], out_terms.at[b]))
    done = [ex.local_out(one) for one in held]
    for one in done:
        one.wait()


SUM_SCRATCH = [((4, 128, 1024), BF), ((3, 128, 1024), BF), ((3, 128, 1024), BF)]


def shift_batch(rows, k):
    return lax.ppermute(rows, "batch", [(i, (i + k) % 4) for i in range(4)])


def shift_chip(rows, k):
    return lax.ppermute(
        rows, "seq", [(i, (i // 2 + k) % 4 * 2 + i % 2) for i in range(8)]
    )


def swap_cores(rows):
    return lax.ppermute(rows, "seq", [(i, i // 2 * 2 + 1 - i % 2) for i in range(8)])


def gather_batch(rows, b):
    came = [rows] + [shift_batch(rows, k) for k in (1, 2, 3)]
    whole = jnp.zeros((4,) + rows.shape, rows.dtype)
    for k in range(4):
        whole = lax.dynamic_update_index_in_dim(whole, came[k], (b + 4 - k) % 4, 0)
    return whole


def sum_batch(blocks, b):
    at = lambda k: lax.dynamic_index_in_dim(blocks, (b + k) % 4, 0, keepdims=False)
    came = [shift_batch(at(k), k) for k in (1, 2, 3)]
    return at(0).astype(F32) + came[0].astype(F32) + came[1].astype(F32) + came[2].astype(F32)


def gather_plane(rows, s):
    came = jnp.stack([rows] + [shift_chip(rows, k) for k in (1, 2, 3)])
    other = swap_cores(came)
    chip, core = s // 2, s % 2
    whole = jnp.zeros((4, 2) + rows.shape, rows.dtype)
    for k in range(4):
        whole = lax.dynamic_update_slice(whole, came[k][None, None], ((chip + 4 - k) % 4, core, 0, 0))
        whole = lax.dynamic_update_slice(whole, other[k][None, None], ((chip + 4 - k) % 4, 1 - core, 0, 0))
    return whole.reshape((8,) + rows.shape)


def sum_plane(blocks, s):
    chip, core = s // 2, s % 2
    shaped = blocks.reshape((4, 2) + blocks.shape[1:])
    mine = lax.dynamic_index_in_dim(shaped, core, 1, keepdims=False)
    other = lax.dynamic_index_in_dim(shaped, 1 - core, 1, keepdims=False)
    both = mine.astype(F32) + swap_cores(other).astype(F32)
    at = lambda k: lax.dynamic_index_in_dim(both, (chip + k) % 4, 0, keepdims=False)
    total = at(0)
    for k in (1, 2, 3):
        total = total + shift_chip(at(k).astype(BF), k).astype(F32)
    return total


def centred(rows):
    middle = rows - jnp.mean(rows, axis=-1, keepdims=True)
    inverse = lax.rsqrt(jnp.mean(middle * middle, axis=-1, keepdims=True) + NORM_EPSILON)
    return middle * inverse, inverse


def norm_back(upstream, gain, normal, inverse):
    scaled = upstream * gain
    average = jnp.mean(scaled, axis=-1, keepdims=True)
    along = jnp.mean(scaled * normal, axis=-1, keepdims=True)
    return inverse * (scaled - average - normal * along)


def gelu_parts(z):
    phi = 0.5 * (1.0 + lax.erf(z * 0.7071067811865476))
    density = 0.3989422804014327 * jnp.exp(-0.5 * z * z)
    return z * phi, phi + z * density


def plane_shards(
    inputs,
    lengths,
    w_qkv,
    w_out,
    w_up,
    w_down,
    norm_gains,
    model_biases,
    attn_biases,
    ff_gain,
    ff_biases,
    head_scale,
    cotangent,
):
    s = lax.axis_index("seq")
    b = lax.axis_index("batch")
    valid_rows = lengths[0]
    positions = s * 128 + jnp.arange(128, dtype=jnp.int32)
    valid_mask = (positions < valid_rows)[:, None]
    all_rows = jnp.arange(1024, dtype=jnp.int32)
    packed = jnp.concatenate(
        [
            norm_gains.reshape(-1),
            model_biases.reshape(-1),
            attn_biases.reshape(-1),
            ff_gain,
            ff_biases.reshape(-1),
            jnp.zeros((2048 - 704,), BF),
        ]
    ).reshape(16, 128)
    x_all, qkv_w, out_w, up_columns, vectors = run_exchange(
        "opening",
        1,
        opening_plan,
        [inputs[0], w_qkv, w_out, w_up, packed],
        [
            ((8, 128, 1024), BF),
            ((8, 4, 32, 384), BF),
            ((8, 4, 32, 1024), BF),
            ((8, 32, 512), BF),
            ((32, 16, 128), BF),
        ],
        [((32, 128), BF)] * 3
        + [((32, 512), BF), ((32, 1024), BF), ((128, 1024), BF), ((16, 128), BF)],
        80,
        everyone=True,
    )
    x_all = x_all.reshape(1024, 1024)
    qkv_w = qkv_w.reshape(1024, 384)
    out_w = out_w.reshape(1024, 1024)
    up_columns, down_rows, g_rows = lax.optimization_barrier((up_columns, w_down, cotangent[0]))
    up_w = gather_batch(up_columns, b).transpose(1, 0, 2, 3).reshape(1024, 512)
    down_w = gather_batch(down_rows, b).reshape(512, 1024)
    g_all = gather_plane(g_rows, s).reshape(1024, 1024)
    g_all = jnp.where((all_rows < valid_rows)[:, None], g_all, jnp.zeros((), BF))
    flat = vectors.reshape(32, 2048).astype(F32)
    take = lambda at, n, w: flat[:, at : at + n * w].reshape(32, n, w).transpose(1, 0, 2).reshape(n, 32 * w)
    gains = take(0, 3, 32)
    biases = take(96, 5, 32)
    attn_b = take(256, 2, 32)
    own = lax.dynamic_slice_in_dim(flat, s * 4, 4, 0)
    take_own = lambda at, n, w: own[:, at : at + n * w].reshape(4, n, w).transpose(1, 0, 2).reshape(n, 4 * w)
    ffn_gain = take_own(320, 1, 128)[0]
    ffn_b = take_own(448, 2, 128)
    scales = head_scale.astype(F32)
    own_scales = lax.dynamic_slice_in_dim(scales, s * 2, 2, 0)
    own_scale_row = jnp.repeat(own_scales, HD)
    scale_row = jnp.repeat(scales, HD)

    normal_a_all, _ = centred(x_all.astype(F32))
    h1 = (normal_a_all * gains[0] + biases[0]).astype(BF)
    query_bias = lax.dynamic_slice_in_dim(biases[3], s * 128, 128, 0)
    value_bias = lax.dynamic_slice_in_dim(attn_b[0], s * 128, 128, 0)
    offsets = jnp.concatenate([query_bias, jnp.zeros((128,), F32), value_bias])
    qkv = (jnp.dot(h1, qkv_w, preferred_element_type=F32) + offsets).astype(BF)
    heads = qkv.reshape(1024, 3, 2, HD).transpose(1, 2, 0, 3)
    q, k, v = heads[0], heads[1], heads[2]
    score_scale = HD ** (-0.5)
    allowed = (all_rows[None, :] <= all_rows[:, None]) & (all_rows[None, :] < valid_rows)
    scores = jnp.einsum("hqd,hkd->hqk", q, k, preferred_element_type=F32) * score_scale
    masked = jnp.where(allowed[None], scores, -1e30)
    top = jnp.max(masked, axis=-1, keepdims=True)
    raised = jnp.exp(masked - top)
    total = jnp.sum(raised, axis=-1, keepdims=True)
    log_total = top + jnp.log(total)
    probs = jnp.exp(masked - log_total)
    probs_low = probs.astype(BF)
    attended = jnp.einsum("hqk,hkd->hqd", probs_low, v, preferred_element_type=F32)
    scaled = (attended * own_scales[:, None, None]).astype(BF)
    scaled_rows = scaled.transpose(1, 0, 2).reshape(1024, 128)
    (scaled_local,) = run_exchange(
        "heads_to_rows", 2, heads_to_rows_plan, [scaled_rows.reshape(8, 128, 128)], [((128, 1024), BF)], [((128, 128), BF)], 8
    )

    residual_in = inputs[0].astype(F32)
    attn_proj = jnp.dot(scaled_local, out_w, preferred_element_type=F32) + attn_b[1]
    normal_b, inverse_b = centred(attn_proj)
    residual = residual_in + normal_b * gains[1] + biases[1]
    normal_c, inverse_c = centred(residual)
    h2_local = (normal_c * gains[2] + biases[2]).astype(BF)
    (h2,) = run_exchange("gather_h2", 3, gather_plan, [h2_local], [((8, 128, 1024), BF)], [((128, 1024), BF)], 8)
    h2 = h2.reshape(1024, 1024)

    hidden = jnp.dot(h2, up_w, preferred_element_type=F32) + ffn_b[0]
    active, slope = gelu_parts(hidden)
    du2 = times_transposed(g_all, down_w)
    dgain = du2 * ffn_gain
    local_mean = jnp.mean(active, axis=-1)
    off = active - local_mean[:, None]
    stats = jnp.stack(
        [local_mean, jnp.sum(off * off, axis=-1), jnp.sum(dgain, axis=-1), jnp.sum(dgain * off, axis=-1)]
    )
    (stats_all,) = run_exchange(
        "stats", 4, stats_plan, [stats.reshape(32, 128)], [((8, 32, 128), F32)], [((32, 128), F32)], 8
    )
    stats_all = stats_all.reshape(8, 4, 1024)
    means = stats_all[:, 0]
    mean = jnp.mean(means, axis=0)
    shift = means - mean[None]
    spread = (jnp.sum(stats_all[:, 1], axis=0) + 512.0 * jnp.sum(shift * shift, axis=0)) / 4096.0
    inverse = lax.rsqrt(spread + NORM_EPSILON)
    average = jnp.sum(stats_all[:, 2], axis=0) / 4096.0
    along = inverse * jnp.sum(stats_all[:, 3] + shift * stats_all[:, 2], axis=0) / 4096.0
    normal_f = (active - mean[:, None]) * inverse[:, None]
    u2 = (normal_f * ffn_gain + ffn_b[1]).astype(BF)
    dz = (inverse[:, None] * (dgain - average[:, None] - normal_f * along[:, None]) * slope).astype(BF)
    grad_ffn_gain = jnp.sum(du2 * normal_f, axis=0)
    grad_ffn_shift = jnp.sum(du2, axis=0)
    grad_ffn_bias = jnp.sum(dz.astype(F32), axis=0)
    ffo_part = jnp.dot(u2, down_w, preferred_element_type=F32).astype(BF)
    dh2_part = times_transposed(dz, up_w).astype(BF)
    (dh2,) = run_exchange(
        "sum_ff",
        5,
        sum_ff_plan,
        [dh2_part.reshape(8, 128, 1024)],
        [((128, 1024), F32)],
        SUM_SCRATCH,
        12,
        near_in=(0,),
        near_out=(0,),
    )
    grad_up = contract_rows(h2, dz)
    grad_down = contract_rows(u2, g_all)
    up_terms = sum_batch(grad_up.astype(BF).reshape(8, 4, 32, 512).transpose(1, 0, 2, 3), b)
    grad_down_own = sum_batch(grad_down.astype(BF).reshape(4, 128, 1024), b)
    ffo = sum_plane(ffo_part.reshape(8, 128, 1024), s)
    output = jnp.where(valid_mask, residual + ffo + biases[4], 0.0).astype(BF)[None]

    g_local = jnp.where(valid_mask, cotangent[0], jnp.zeros((), BF)).astype(F32)
    dr = g_local + norm_back(dh2, gains[2], normal_c, inverse_c)
    da = norm_back(dr, gains[1], normal_b, inverse_b).astype(BF)
    dscaled = times_transposed(da, out_w)
    do_local = (dscaled * scale_row).astype(BF)
    (do_blocks,) = run_exchange(
        "rows_to_heads", 6, rows_to_heads_plan, [do_local], [((8, 128, 128), BF)], [((128, 128), BF)], 8
    )
    do_rows = do_blocks.reshape(1024, 128)
    do = do_rows.reshape(1024, 2, HD).transpose(1, 0, 2)

    delta = jnp.sum(do.astype(F32) * attended, axis=-1)
    grad_scales = jnp.sum(delta, axis=-1) / own_scales
    dp = jnp.einsum("hqd,hkd->hqk", do, v, preferred_element_type=F32)
    ds = (probs * (dp - delta[..., None])).astype(BF)
    dq = jnp.einsum("hqk,hkd->hqd", ds, k, preferred_element_type=F32) * score_scale
    dk = jnp.einsum("hqk,hqd->hkd", ds, q, preferred_element_type=F32) * score_scale
    dv = jnp.einsum("hqk,hqd->hkd", probs_low, do, preferred_element_type=F32)
    dqkv = jnp.stack([dq, dk, dv]).astype(BF).transpose(2, 0, 1, 3).reshape(1024, 384)
    column_sums = jnp.sum(dqkv.astype(F32), axis=0)
    grad_qkv = contract_rows(h1, dqkv)
    dh1_part = times_transposed(dqkv, qkv_w).astype(BF)
    dh1, da_all, qkv_terms = run_exchange(
        "sum_grads",
        7,
        grads_plan,
        [dh1_part.reshape(8, 128, 1024), da, grad_qkv.astype(BF).reshape(8, 4, 32, 384)],
        [((128, 1024), F32), ((8, 128, 1024), BF), ((4, 8, 32, 384), BF)],
        [((128, 1024), BF), ((8, 32, 384), BF)] + SUM_SCRATCH,
        24,
        near_in=(0,),
        near_out=(0,),
    )
    add = lambda terms: jnp.sum(terms.astype(F32), axis=0)
    grad_out = contract_rows(scaled_rows, da_all.reshape(1024, 1024)).astype(BF)
    normal_a, inverse_a = centred(residual_in)
    grad_input = (dr + norm_back(dh1, gains[0], normal_a, inverse_a)).astype(BF)[None]

    place = lambda row: lax.dynamic_update_slice_in_dim(jnp.zeros((1024,), F32), row, s * 128, 0)
    place_ff = lambda rows: lax.dynamic_update_slice_in_dim(jnp.zeros((3, 4096), F32), rows, s * 512, 1)
    wide = jnp.stack(
        [
            jnp.sum(dh1 * normal_a, axis=0),
            jnp.sum(dr * normal_b, axis=0),
            jnp.sum(dh2 * normal_c, axis=0),
            jnp.sum(dh1, axis=0),
            jnp.sum(dr, axis=0),
            jnp.sum(dh2, axis=0),
            place(column_sums[:128]),
            jnp.sum(g_local, axis=0),
            place(column_sums[256:]),
            jnp.sum(da.astype(F32), axis=0),
        ]
    )
    ff_wide = place_ff(jnp.stack([grad_ffn_gain, grad_ffn_bias, grad_ffn_shift]))
    scale_wide = lax.dynamic_update_slice_in_dim(jnp.zeros((H,), F32), grad_scales, s * 2, 0)
    terms = jnp.concatenate(
        [
            wide.reshape(10, 32, 32).transpose(1, 0, 2).reshape(32, 320),
            ff_wide.reshape(3, 32, 128).transpose(1, 0, 2).reshape(32, 384),
            jnp.broadcast_to(scale_wide[None], (32, H)),
            jnp.zeros((32, 1024 - 720), F32),
        ],
        axis=1,
    ).reshape(32, 8, 128)
    vec_terms, qkv_own, up_own, out_terms = run_exchange(
        "closing",
        8,
        closing_plan,
        [terms, add(qkv_terms).astype(BF), up_terms.astype(BF), grad_out.reshape(4, 32, 1024)],
        [((32, 8, 128), F32), ((32, 3072), BF), ((32, 4096), BF), ((4, 32, 1024), BF)],
        [((8, 128), F32)] + [((32, 128), BF)] * 3 + [((32, 512), BF), ((32, 1024), BF)],
        72,
        everyone=True,
    )
    sums = jnp.sum(vec_terms, axis=0).reshape(1024)
    wide_sums = sums[:320].reshape(10, 32)
    ff_sums = sums[320:704].reshape(3, 128)
    return (
        output,
        grad_input,
        qkv_own.astype(F32),
        add(out_terms),
        up_own.astype(F32),
        grad_down_own,
        wide_sums[0:3],
        wide_sums[3:8],
        wide_sums[8:10],
        ff_sums[0],
        ff_sums[1:3],
        sums[704:720],
    )


def solution(mesh):
    in_plane = mesh.shape["seq"] == 8 and mesh.shape["batch"] == 4
    return jax.shard_map(
        plane_shards if in_plane else shards,
        mesh=mesh,
        in_specs=(
            P("batch", "seq", None),
            P("batch"),
            P(("seq", "batch"), None),
            P(("seq", "batch"), None),
            P(("seq", "batch"), None),
            P(("seq", "batch"), None),
            P(None, ("seq", "batch")),
            P(None, ("seq", "batch")),
            P(None, ("seq", "batch")),
            P(("seq", "batch")),
            P(None, ("seq", "batch")),
            P(),
            P("batch", "seq", None),
        ),
        out_specs=(
            P("batch", "seq", None),
            P("batch", "seq", None),
            P(("seq", "batch"), None),
            P(("seq", "batch"), None),
            P(("seq", "batch"), None),
            P(("seq", "batch"), None),
            P(None, ("seq", "batch")),
            P(None, ("seq", "batch")),
            P(None, ("seq", "batch")),
            P(("seq", "batch")),
            P(None, ("seq", "batch")),
            P(),
        ),
        check_vma=False,
    )
```

```python
import jax
import jax.numpy as jnp
from jax import lax
from jax.experimental import pallas as pl
from jax.experimental.pallas import tpu as pltpu
from jax.sharding import PartitionSpec as P

H = 16
HD = 64


NORM_EPSILON = 1e-05


def layer_norm(vector, norm_gain, norm_bias):
    centered = vector - jnp.mean(vector, axis=-1, keepdims=True)
    spread = jnp.mean(centered * centered, axis=-1, keepdims=True)
    return centered * lax.rsqrt(spread + NORM_EPSILON) * norm_gain + norm_bias


def gelu_norm(hidden, norm_gain, norm_bias):
    return layer_norm(jax.nn.gelu(hidden, approximate=False), norm_gain, norm_bias)


def contract_rows(left, right):
    return lax.dot_general(
        left, right, (((0,), (0,)), ((), ())), preferred_element_type=jnp.float32
    )


def times_transposed(left, right):
    return lax.dot_general(
        left, right, (((1,), (1,)), ((), ())), preferred_element_type=jnp.float32
    )


def shards(
    inputs,
    lengths,
    w_qkv,
    w_out,
    w_up,
    w_down,
    norm_gains,
    model_biases,
    attn_biases,
    ff_gain,
    ff_biases,
    head_scale,
    cotangent,
):
    gathered = (
        lax.all_gather(w_qkv, ("seq", "batch"), axis=0, tiled=True),
        lax.all_gather(w_out, ("seq", "batch"), axis=0, tiled=True),
        lax.all_gather(w_up, ("seq", "batch"), axis=0, tiled=True),
        lax.all_gather(w_down, ("seq", "batch"), axis=0, tiled=True),
        lax.all_gather(norm_gains, ("seq", "batch"), axis=1, tiled=True),
        lax.all_gather(model_biases, ("seq", "batch"), axis=1, tiled=True),
        lax.all_gather(attn_biases, ("seq", "batch"), axis=1, tiled=True),
        lax.all_gather(ff_gain, ("seq", "batch"), axis=0, tiled=True),
        lax.all_gather(ff_biases, ("seq", "batch"), axis=1, tiled=True),
    )
    qkv_full, out_full, up_full, down_full = (gathered[0], gathered[1], gathered[2], gathered[3])
    gain_rows = gathered[4].astype(jnp.float32)
    bias_rows = gathered[5].astype(jnp.float32)
    attn_rows = gathered[6].astype(jnp.float32)
    ffn_gain = gathered[7].astype(jnp.float32)
    ffn_rows = gathered[8].astype(jnp.float32)
    scales = head_scale.astype(jnp.float32)
    local_rows = inputs.shape[1]
    model_width = inputs.shape[2]
    seq_length = local_rows * lax.axis_size("seq")
    tile_rows = min(512, seq_length)
    first_row = lax.axis_index("seq") * local_rows
    valid_rows = lengths[0]
    positions = first_row + jnp.arange(local_rows, dtype=jnp.int32)
    valid_mask = (positions < valid_rows)[:, None]
    score_scale = HD ** (-0.5)
    residual_in = inputs[0].astype(jnp.float32)
    normed, norm_a_pull = jax.vjp(layer_norm, residual_in, gain_rows[0], bias_rows[0])
    normed_low = normed.astype(jnp.bfloat16)
    offsets = jnp.concatenate([bias_rows[3], jnp.zeros_like(bias_rows[3]), attn_rows[0]])
    projected = (
        jnp.dot(normed_low, qkv_full, preferred_element_type=jnp.float32) + offsets
    ).astype(jnp.bfloat16)
    queries = projected[:, :model_width]
    key_local = projected[:, model_width : 2 * model_width]
    value_local = projected[:, 2 * model_width :]
    key_rows, value_rows = (
        lax.all_gather(key_local, "seq", axis=0, tiled=True),
        lax.all_gather(value_local, "seq", axis=0, tiled=True),
    )
    query_heads = queries.reshape(local_rows, H, HD)
    last_needed = jnp.minimum(first_row + local_rows - 1, valid_rows - 1)
    tile_count = last_needed // tile_rows + 1

    def tile_scores(j):
        start = j * tile_rows
        key_tile = lax.dynamic_slice_in_dim(key_rows, start, tile_rows, 0).reshape(tile_rows, H, HD)
        scores = (
            jnp.einsum("qhd,khd->hqk", query_heads, key_tile, preferred_element_type=jnp.float32)
            * score_scale
        )
        key_index = start + jnp.arange(tile_rows, dtype=jnp.int32)
        allowed = (key_index[None, :] <= positions[:, None]) & (key_index[None, :] < valid_rows)
        return (scores, allowed[None], key_tile)

    def max_and_sum(j, carry):
        running_max, running_sum = carry
        scores, allowed, unused_tile = tile_scores(j)
        masked = jnp.where(allowed, scores, -1e30)
        new_max = jnp.maximum(running_max, jnp.max(masked, axis=-1))
        kept_terms = jnp.where(allowed, jnp.exp(masked - new_max[..., None]), 0.0)
        return (
            new_max,
            running_sum * jnp.exp(running_max - new_max) + jnp.sum(kept_terms, axis=-1),
        )

    start_stats = (
        jnp.full((H, local_rows), -1e30, jnp.float32),
        jnp.zeros((H, local_rows), jnp.float32),
    )
    running_max, running_sum = lax.fori_loop(0, tile_count, max_and_sum, start_stats)
    log_total = running_max + jnp.log(running_sum)

    def tile_probs(j):
        scores, allowed, key_tile = tile_scores(j)
        attn_probs = jnp.where(allowed, jnp.exp(scores - log_total[..., None]), 0.0)
        value_tile = lax.dynamic_slice_in_dim(value_rows, j * tile_rows, tile_rows, 0).reshape(
            tile_rows, H, HD
        )
        return (attn_probs, key_tile, value_tile)

    def accumulate(j, summed):
        attn_probs, unused_tile, value_tile = tile_probs(j)
        return summed + jnp.einsum(
            "hqk,khd->qhd",
            attn_probs.astype(jnp.bfloat16),
            value_tile,
            preferred_element_type=jnp.float32,
        )

    attended = lax.fori_loop(0, tile_count, accumulate, jnp.zeros((local_rows, H, HD), jnp.float32))
    scaled_low = (
        (attended * scales[None, :, None]).reshape(local_rows, model_width).astype(jnp.bfloat16)
    )
    attn_proj = jnp.dot(scaled_low, out_full, preferred_element_type=jnp.float32) + attn_rows[1]
    attn_normed, norm_b_pull = jax.vjp(layer_norm, attn_proj, gain_rows[1], bias_rows[1])
    residual = residual_in + attn_normed
    ffn_in, norm_c_pull = jax.vjp(layer_norm, residual, gain_rows[2], bias_rows[2])
    ffn_low = ffn_in.astype(jnp.bfloat16)
    hidden = jnp.dot(ffn_low, up_full, preferred_element_type=jnp.float32) + ffn_rows[0]
    ffn_normed, ffn_pull = jax.vjp(gelu_norm, hidden, ffn_gain, ffn_rows[1])
    ffn_out_low = ffn_normed.astype(jnp.bfloat16)
    combined = jnp.where(
        valid_mask,
        residual
        + jnp.dot(ffn_out_low, down_full, preferred_element_type=jnp.float32)
        + bias_rows[4],
        0.0,
    )
    output = combined.astype(jnp.bfloat16)[None]
    barrier_out = lax.optimization_barrier(((w_qkv, w_out, w_up, w_down), combined))
    regathered = (
        lax.all_gather(barrier_out[0][0], ("seq", "batch"), axis=0, tiled=True),
        lax.all_gather(barrier_out[0][1], ("seq", "batch"), axis=0, tiled=True),
        lax.all_gather(barrier_out[0][2], ("seq", "batch"), axis=0, tiled=True),
        lax.all_gather(barrier_out[0][3], ("seq", "batch"), axis=0, tiled=True),
    )
    qkv_full, out_full, up_full, down_full = (
        regathered[0],
        regathered[1],
        regathered[2],
        regathered[3],
    )
    cotan_rows = jnp.where(valid_mask, cotangent[0], jnp.zeros_like(cotangent[0]))
    cotan_float = cotan_rows.astype(jnp.float32)
    grad_down = contract_rows(ffn_out_low, cotan_rows)
    grad_bias_out = jnp.sum(cotan_float, axis=0)
    grad_ffn_normed = times_transposed(cotan_rows, down_full)
    grad_hidden, grad_ffn_gain, grad_ffn_shift = ffn_pull(grad_ffn_normed)
    grad_hidden_low = grad_hidden.astype(jnp.bfloat16)
    grad_up = contract_rows(ffn_low, grad_hidden_low)
    grad_ffn_bias = jnp.sum(grad_hidden_low.astype(jnp.float32), axis=0)
    grad_ffn_in = times_transposed(grad_hidden_low, up_full)
    grad_from_ffn, grad_gain_c, grad_shift_c = norm_c_pull(grad_ffn_in)
    grad_residual = cotan_float + grad_from_ffn
    grad_proj, grad_gain_b, grad_shift_b = norm_b_pull(grad_residual)
    grad_proj_low = grad_proj.astype(jnp.bfloat16)
    grad_out_bias = jnp.sum(grad_proj_low.astype(jnp.float32), axis=0)
    grad_out = contract_rows(scaled_low, grad_proj_low)
    grad_scaled = times_transposed(grad_proj_low, out_full).reshape(local_rows, H, HD)
    grad_scales = jnp.sum(grad_scaled * attended, axis=(0, 2))
    grad_heads_low = (grad_scaled * scales[None, :, None]).astype(jnp.bfloat16)
    row_delta = jnp.einsum("qhd,qhd->hq", grad_heads_low.astype(jnp.float32), attended)

    def score_grads(j):
        attn_probs, key_tile, value_tile = tile_probs(j)
        grad_probs = jnp.einsum(
            "qhd,khd->hqk", grad_heads_low, value_tile, preferred_element_type=jnp.float32
        )
        grad_scores = (attn_probs * (grad_probs - row_delta[..., None])).astype(jnp.bfloat16)
        return (attn_probs, grad_scores, key_tile)

    def backward_tile(j, carry):
        grad_query, terms = carry
        attn_probs, grad_scores, key_tile = score_grads(j)
        grad_query = grad_query + jnp.einsum(
            "hqk,khd->qhd", grad_scores, key_tile, preferred_element_type=jnp.float32
        )
        grad_key = (
            jnp.einsum("hqk,qhd->khd", grad_scores, query_heads, preferred_element_type=jnp.float32)
            * score_scale
        )
        grad_value = jnp.einsum(
            "hqk,qhd->khd",
            attn_probs.astype(jnp.bfloat16),
            grad_heads_low,
            preferred_element_type=jnp.float32,
        )
        piece = jnp.concatenate(
            [grad_key.reshape(tile_rows, model_width), grad_value.reshape(tile_rows, model_width)],
            axis=1,
        )
        return (grad_query, lax.dynamic_update_slice_in_dim(terms, piece, j * tile_rows, 0))

    start_carry = (
        jnp.zeros((local_rows, H, HD), jnp.float32),
        jnp.zeros((seq_length, 2 * model_width), jnp.float32),
    )
    grad_query, terms = lax.fori_loop(0, tile_count, backward_tile, start_carry)
    grad_kv = lax.psum_scatter(terms, "seq", scatter_dimension=0, tiled=True)
    grad_query_low = (
        (grad_query * score_scale).reshape(local_rows, model_width).astype(jnp.bfloat16)
    )
    grad_kv_low = grad_kv.astype(jnp.bfloat16)
    grad_projected = jnp.concatenate([grad_query_low, grad_kv_low], axis=1)
    grad_qkv = contract_rows(normed_low, grad_projected)
    grad_query_bias = jnp.sum(grad_query_low.astype(jnp.float32), axis=0)
    grad_value_bias = jnp.sum(grad_kv_low[:, model_width:].astype(jnp.float32), axis=0)
    grad_normed = times_transposed(grad_projected, qkv_full)
    grad_from_attn, grad_gain_a, grad_shift_a = norm_a_pull(grad_normed)
    grad_input = (grad_residual + grad_from_attn).astype(jnp.bfloat16)[None]
    reduced = (
        lax.psum_scatter(grad_qkv, ("seq", "batch"), scatter_dimension=0, tiled=True),
        lax.psum_scatter(grad_out, ("seq", "batch"), scatter_dimension=0, tiled=True),
        lax.psum_scatter(grad_up, ("seq", "batch"), scatter_dimension=0, tiled=True),
        lax.psum_scatter(grad_down, ("seq", "batch"), scatter_dimension=0, tiled=True),
        lax.psum_scatter(
            jnp.stack([grad_gain_a, grad_gain_b, grad_gain_c]),
            ("seq", "batch"),
            scatter_dimension=1,
            tiled=True,
        ),
        lax.psum_scatter(
            jnp.stack([grad_shift_a, grad_shift_b, grad_shift_c, grad_query_bias, grad_bias_out]),
            ("seq", "batch"),
            scatter_dimension=1,
            tiled=True,
        ),
        lax.psum_scatter(
            jnp.stack([grad_value_bias, grad_out_bias]),
            ("seq", "batch"),
            scatter_dimension=1,
            tiled=True,
        ),
        lax.psum_scatter(grad_ffn_gain, ("seq", "batch"), scatter_dimension=0, tiled=True),
        lax.psum_scatter(
            jnp.stack([grad_ffn_bias, grad_ffn_shift]),
            ("seq", "batch"),
            scatter_dimension=1,
            tiled=True,
        ),
    )
    scale_total = lax.psum(grad_scales, ("seq", "batch"))
    return (
        output,
        grad_input,
        reduced[0],
        reduced[1],
        reduced[2],
        reduced[3],
        reduced[4],
        reduced[5],
        reduced[6],
        reduced[7],
        reduced[8],
        scale_total,
    )


BF = jnp.bfloat16
F32 = jnp.float32


class Exchange:
    def __init__(self, send_sems, recv_sems, local_sems):
        self.send_sems = send_sems
        self.recv_sems = recv_sems
        self.local_sems = local_sems
        self.count = 0
        self.locals = 0
        self.sent = []
        self.s = lax.axis_index("seq")
        self.b = lax.axis_index("batch")
        self.chip = self.s // 2
        self.core = self.s % 2
        self.sibling = self.chip * 2 + 1 - self.core

    def send(self, src, dst, seq, batch):
        at = self.count
        self.count += 1
        copy = pltpu.make_async_remote_copy(
            src_ref=src,
            dst_ref=dst,
            send_sem=self.send_sems.at[at],
            recv_sem=self.recv_sems.at[at],
            device_id=(seq, batch),
            device_id_type=pl.DeviceIdType.MESH,
        )
        copy.start()
        self.sent.append(copy)
        return copy

    def local(self, src, dst):
        at = self.locals
        self.locals += 1
        copy = pltpu.make_async_copy(src, dst, self.local_sems.at[at])
        copy.start()
        return copy

    def arrived(self, copies):
        for copy in copies:
            copy.wait_recv()

    def finish(self):
        for copy in self.sent:
            copy.wait_send()

    def peer(self, k):
        return ((self.chip + k) % 4) * 2 + self.core

    def source(self, k):
        return ((self.chip + 4 - k) % 4) * 2 + self.core

    def plane(self):
        return [(self.s + j) % 8 for j in range(1, 8)]

    def line(self):
        return [(self.b + k) % 4 for k in range(1, 4)]

    def gather_start(self, src, slot):
        copies = [self.send(src, slot(self.s), self.peer(k), self.b) for k in (1, 2, 3)]
        copies.append(self.send(src, slot(self.s), self.sibling, self.b))
        return copies

    def gather_forward(self, copies, slot):
        passed = []
        for k in (1, 2, 3):
            copies[k - 1].wait_recv()
            came = slot(self.source(k))
            passed.append(self.send(came, came, self.sibling, self.b))
        return [copies[3]] + passed

    def sum_pair(self, src, from_pair):
        return [
            self.send(src.at[((self.chip + k) % 4) * 2 + 1 - self.core], from_pair.at[k], self.sibling, self.b)
            for k in (1, 2, 3, 0)
        ]

    def sum_chips(self, copies, src, from_pair, paired, from_chips, total):
        over = []
        for at, k in enumerate((1, 2, 3, 0)):
            copies[at].wait_recv()
            mine = src[((self.chip + k) % 4) * 2 + self.core].astype(F32)
            both = mine + from_pair[k].astype(F32)
            if k:
                paired[k - 1] = both.astype(BF)
                over.append(self.send(paired.at[k - 1], from_chips.at[k - 1], self.peer(k), self.b))
            else:
                total[...] = both
        return over

    def sum_end(self, over, from_chips, total):
        self.arrived(over)
        return total[...] + from_chips[0].astype(F32) + from_chips[1].astype(F32) + from_chips[2].astype(F32)


def columns(start, size):
    return pl.ds(pl.multiple_of(start, 128), size)


def centred(rows):
    middle = rows - jnp.mean(rows, axis=-1, keepdims=True)
    inverse = lax.rsqrt(jnp.mean(middle * middle, axis=-1, keepdims=True) + NORM_EPSILON)
    return middle * inverse, inverse


def norm_back(upstream, gain, normal, inverse):
    scaled = upstream * gain
    average = jnp.mean(scaled, axis=-1, keepdims=True)
    along = jnp.mean(scaled * normal, axis=-1, keepdims=True)
    return inverse * (scaled - average - normal * along)


def gelu_parts(z):
    phi = 0.5 * (1.0 + lax.erf(z * 0.7071067811865476))
    density = 0.3989422804014327 * jnp.exp(-0.5 * z * z)
    return z * phi, phi + z * density


def matmul(left, right):
    return jnp.dot(left, right, preferred_element_type=F32)


def column_sum(rows):
    return jnp.sum(rows, axis=0, keepdims=True)


def pack_columns(parts):
    lane = lax.broadcasted_iota(jnp.int32, (128, 128), 1)
    wide = jnp.zeros((128, 128), F32)
    for at, part in enumerate(parts):
        wide = jnp.where(lane == at, part, wide)
    return wide.T[:8]


BUFFERS = dict(
    x_all=((8, 128, 1024), BF),
    g_all=((8, 128, 1024), BF),
    qkv_w=((8, 4, 32, 384), BF),
    out_w=((8, 4, 32, 1024), BF),
    up_w=((8, 4, 32, 512), BF),
    down_w=((4, 128, 1024), BF),
    vec_all=((32, 16, 128), F32),
    rows=((16, 1024), F32),
    ff_rows=((8, 512), F32),
    h1=((1024, 1024), BF),
    qkv=((1024, 384), BF),
    probs_low=((2, 512, 512), F32),
    probs_high=((2, 512, 1024), F32),
    attended=((1024, 128), F32),
    scaled=((8, 128, 128), BF),
    scaled_local=((128, 1024), BF),
    normal_b=((128, 1024), F32),
    normal_c=((128, 1024), F32),
    residual=((128, 1024), F32),
    h2_all=((8, 128, 1024), BF),
    active=((1024, 512), F32),
    slope=((1024, 512), F32),
    du2=((1024, 512), F32),
    stats=((8, 8, 128), F32),
    stats_all=((8, 8, 8, 128), F32),
    u2=((1024, 512), BF),
    dz=((1024, 512), BF),
    dh2_src=((8, 128, 1024), BF),
    dh2_pair=((4, 128, 1024), BF),
    dh2_paired=((3, 128, 1024), BF),
    dh2_chips=((3, 128, 1024), BF),
    ffo_src=((8, 128, 1024), BF),
    ffo_pair=((4, 128, 1024), BF),
    ffo_paired=((3, 128, 1024), BF),
    ffo_chips=((3, 128, 1024), BF),
    dh1_src=((8, 128, 1024), BF),
    dh1_pair=((4, 128, 1024), BF),
    dh1_paired=((3, 128, 1024), BF),
    dh1_chips=((3, 128, 1024), BF),
    total=((128, 1024), F32),
    ffo_total=((128, 1024), F32),
    dr=((128, 1024), F32),
    da_all=((8, 128, 1024), BF),
    do_local=((128, 1024), BF),
    do_all=((8, 128, 128), BF),
    dq=((1024, 128), F32),
    dk=((1024, 128), F32),
    dv=((1024, 128), F32),
    dqkv=((1024, 384), BF),
    up_src=((8, 4, 32, 512), BF),
    up_terms=((4, 8, 32, 512), BF),
    down_src=((4, 128, 1024), BF),
    down_terms=((4, 128, 1024), BF),
    qkv_src=((8, 4, 32, 384), BF),
    qkv_terms=((4, 8, 32, 384), BF),
    out_src=((4, 32, 1024), BF),
    out_terms=((4, 32, 1024), BF),
    up_own=((8, 32, 512), BF),
    up_fin=((32, 4096), BF),
    qkv_own=((8, 32, 384), BF),
    qkv_fin=((32, 3072), BF),
    close_src=((8, 16, 128), F32),
    close_all=((32, 16, 128), F32),
    ff_src=((4, 8, 128), F32),
    ff_all=((4, 8, 128), F32),
)
COPIES = 240
INPUTS = 9
OUTPUTS = 8


def block_kernel(length_in, x_in, g_in, qkv_in, out_in, up_in, down_in, vec_in, scale_in, *refs):
    output, grad_input, grad_qkv, grad_out, grad_up, grad_down, vec_out, ff_out = refs[:OUTPUTS]
    B = type("Buffers", (), dict(zip(BUFFERS, refs[OUTPUTS : OUTPUTS + len(BUFFERS)])))
    ex = Exchange(*refs[OUTPUTS + len(BUFFERS) :])
    s, b = ex.s, ex.b
    me = s * 4 + b
    valid_rows = length_in[0, 0]

    barrier = pltpu.get_barrier_semaphore()
    partners = [((s + j // 4) % 8, (b + j % 4) % 4) for j in range(1, 32)]
    for seq, batch in partners:
        pl.semaphore_signal(barrier, inc=1, device_id=(seq, batch), device_id_type=pl.DeviceIdType.MESH)
    pl.semaphore_wait(barrier, len(partners))

    qkv_part = lambda p, t: qkv_in.at[:, columns(t * 1024 + p * 128, 128)]
    qkv_slot = lambda t: B.qkv_w.at[s, b, :, pl.ds(t * 128, 128)]
    qkv_copies = [ex.send(qkv_part(p, t), qkv_slot(t), p, b) for p in ex.plane() for t in range(3)]
    own = [ex.local(qkv_part(s, t), qkv_slot(t)) for t in range(3)]
    own_up = ex.local(up_in.at[:, columns(s * 512, 512)], B.up_w.at[s, b])
    own_rest = [
        ex.local(out_in, B.out_w.at[s, b]),
        ex.local(x_in, B.x_all.at[s]),
        ex.local(g_in, B.g_all.at[s]),
        ex.local(down_in, B.down_w.at[b]),
        ex.local(vec_in, B.vec_all.at[me]),
    ]
    x_slot = lambda i: B.x_all.at[i]
    g_slot = lambda i: B.g_all.at[i]
    x_copies = ex.gather_start(x_in, x_slot)
    vec_copies = [ex.send(vec_in, B.vec_all.at[me], p, q) for p, q in partners]
    up_copies = [ex.send(up_in.at[:, columns(p * 512, 512)], B.up_w.at[s, b], p, b) for p in ex.plane()]
    ex.arrived(qkv_copies)
    for one in own:
        one.wait()
    qkv_line = [ex.send(B.qkv_w.at[:, b], B.qkv_w.at[:, b], s, q) for q in ex.line()]
    out_line = [ex.send(out_in, B.out_w.at[s, b], s, q) for q in ex.line()]
    down_line = [ex.send(down_in, B.down_w.at[b], s, q) for q in ex.line()]
    x_passed = ex.gather_forward(x_copies, x_slot)
    g_copies = ex.gather_start(g_in, g_slot)
    ex.arrived(up_copies)
    own_up.wait()
    up_line = [ex.send(B.up_w.at[:, b], B.up_w.at[:, b], s, q) for q in ex.line()]
    ex.arrived(vec_copies)
    for one in own_rest:
        one.wait()

    for p in range(8):
        group = B.vec_all[4 * p] + B.vec_all[4 * p + 1] + B.vec_all[4 * p + 2] + B.vec_all[4 * p + 3]
        B.rows[:, p * 128 : (p + 1) * 128] = group
    for q in range(4):
        B.ff_rows[:, q * 128 : (q + 1) * 128] = B.vec_all[s * 4 + q][8:16]
    row = lambda at: B.rows[at : at + 1, :]
    gain_a, gain_b, gain_c = row(0), row(1), row(2)
    bias_a, bias_b, bias_c, bias_out, bias_attn = row(3), row(4), row(5), row(7), row(9)
    ffn_gain, ffn_bias, ffn_shift = B.ff_rows[2:3, :], B.ff_rows[3:4, :], B.ff_rows[4:5, :]
    own_columns = columns(s * 128, 128)
    query_bias = B.rows[6:7, own_columns]
    value_bias = B.rows[8:9, own_columns]
    own_scale = scale_in[0:1, own_columns]

    ex.arrived(x_passed)

    @pl.loop(0, 8)
    def _(t):
        normal, _unused = centred(B.x_all[t].astype(F32))
        B.h1[pl.ds(t * 128, 128), :] = (normal * gain_a + bias_a).astype(BF)

    ex.arrived(qkv_line)
    offsets = jnp.concatenate([query_bias, jnp.zeros_like(query_bias), value_bias], axis=1)

    @pl.loop(0, 4)
    def _(t):
        at = pl.ds(t * 256, 256)
        B.qkv[at, :] = (matmul(B.h1[at, :], B.qkv_w[...].reshape(1024, 384)) + offsets).astype(BF)

    ex.arrived(out_line)
    out_slot = lambda i: B.out_w.at[i]
    out_copies = ex.gather_start(B.out_w.at[s], out_slot)
    g_passed = ex.gather_forward(g_copies, g_slot)

    score_scale = HD ** (-0.5)
    half_of = lax.broadcasted_iota(jnp.int32, (1, 128), 1) // HD

    def of_head(rows, h):
        return jnp.where(half_of == h, rows, jnp.zeros_like(rows))

    for size in (512, 1024):
        for h in range(2):

            @pl.loop(size // 128 - 4, size // 128)
            def _(t):
                at = pl.ds(t * 128, 128)
                scores = times_transposed(of_head(B.qkv[at, 0:128], h), B.qkv[0:size, 128:256]) * score_scale
                key_index = lax.broadcasted_iota(jnp.int32, (128, size), 1)
                query_index = t * 128 + lax.broadcasted_iota(jnp.int32, (128, size), 0)
                allowed = (key_index <= query_index) & (key_index < valid_rows)
                masked = jnp.where(allowed, scores, -1e30)
                raised = jnp.exp(masked - jnp.max(masked, axis=-1, keepdims=True))
                probs = raised * (1.0 / jnp.sum(raised, axis=-1, keepdims=True))
                kept = B.probs_low if size == 512 else B.probs_high
                kept[h, pl.ds(t * 128 - size + 512, 128), :] = probs
                found = matmul(probs.astype(BF), of_head(B.qkv[0:size, 256:384], h))
                if h == 0:
                    B.attended[at, :] = found
                else:
                    both = B.attended[at, :] + found
                    B.attended[at, :] = both
                    B.scaled[t] = (both * own_scale).astype(BF)

    local_lanes = B.scaled_local.at[:, own_columns]
    heads = [ex.send(B.scaled.at[p], local_lanes, p, b) for p in ex.plane()]
    own_heads = ex.local(B.scaled.at[s], local_lanes)
    out_passed = ex.gather_forward(out_copies, out_slot)
    ex.arrived(out_passed)
    ex.arrived(heads)
    own_heads.wait()

    attn_proj = matmul(B.scaled_local[...], B.out_w[...].reshape(1024, 1024)) + bias_attn
    normal_b, inverse_b = centred(attn_proj)
    B.normal_b[...] = normal_b
    residual = x_in[...].astype(F32) + normal_b * gain_b + bias_b
    B.residual[...] = residual
    normal_c, inverse_c = centred(residual)
    B.normal_c[...] = normal_c
    B.h2_all[s] = (normal_c * gain_c + bias_c).astype(BF)
    h2_slot = lambda i: B.h2_all.at[i]
    h2_copies = ex.gather_start(B.h2_all.at[s], h2_slot)

    ex.arrived(g_passed)
    ex.arrived(down_line)

    @pl.loop(0, 8)
    def _(t):
        B.du2[pl.ds(t * 128, 128), :] = times_transposed(B.g_all[t], B.down_w[...].reshape(512, 1024))

    h2_passed = ex.gather_forward(h2_copies, h2_slot)
    ex.arrived(up_line)
    ex.arrived(h2_passed)

    @pl.loop(0, 8)
    def _(t):
        at = pl.ds(t * 128, 128)
        hidden = matmul(B.h2_all[t], B.up_w[...].reshape(1024, 512)) + ffn_bias
        active, slope = gelu_parts(hidden)
        B.active[at, :] = active
        B.slope[at, :] = slope
        dgain = B.du2[at, :] * ffn_gain
        mean = jnp.mean(active, axis=-1, keepdims=True)
        off = active - mean
        add = lambda rows: jnp.sum(rows, axis=-1, keepdims=True)
        B.stats[t] = pack_columns([mean, add(off * off), add(dgain), add(dgain * off)])

    stats_copies = [ex.send(B.stats, B.stats_all.at[s], p, b) for p in ex.plane()]
    own_stats = ex.local(B.stats, B.stats_all.at[s])
    ex.arrived(stats_copies)
    own_stats.wait()

    def finish_hidden(t, sums):
        at = pl.ds(t * 128, 128)
        means = [B.stats_all[i, t, 0:1, :] for i in range(8)]
        squares = [B.stats_all[i, t, 1:2, :] for i in range(8)]
        firsts = [B.stats_all[i, t, 2:3, :] for i in range(8)]
        seconds = [B.stats_all[i, t, 3:4, :] for i in range(8)]
        mean = sum(means) * 0.125
        shifts = [one - mean for one in means]
        spread = (sum(squares) + 512.0 * sum(one * one for one in shifts)) * (1.0 / 4096.0)
        inverse = lax.rsqrt(spread + NORM_EPSILON)
        average = sum(firsts) * (1.0 / 4096.0)
        along = inverse * sum(two + one * first for two, one, first in zip(seconds, shifts, firsts)) * (1.0 / 4096.0)
        packed = jnp.concatenate([mean, inverse, average, along, jnp.zeros((124, 128), F32)], axis=0).T
        mean, inverse, average, along = (packed[:, i : i + 1] for i in range(4))
        normal = (B.active[at, :] - mean) * inverse
        B.u2[at, :] = (normal * ffn_gain + ffn_shift).astype(BF)
        du2 = B.du2[at, :]
        dz = (inverse * (du2 * ffn_gain - average - normal * along) * B.slope[at, :]).astype(BF)
        B.dz[at, :] = dz
        B.dh2_src[t] = times_transposed(dz, B.up_w[...].reshape(1024, 512)).astype(BF)
        return (
            sums[0] + column_sum(du2 * normal),
            sums[1] + column_sum(dz.astype(F32)),
            sums[2] + column_sum(du2),
        )

    nothing = jnp.zeros((1, 512), F32)
    ff_sums = lax.fori_loop(0, 8, finish_hidden, (nothing, nothing, nothing))
    dh2_pairs = ex.sum_pair(B.dh2_src, B.dh2_pair)

    @pl.loop(0, 8)
    def _(t):
        B.ffo_src[t] = matmul(B.u2[pl.ds(t * 128, 128), :], B.down_w[...].reshape(512, 1024)).astype(BF)

    dh2_over = ex.sum_chips(dh2_pairs, B.dh2_src, B.dh2_pair, B.dh2_paired, B.dh2_chips, B.total)
    ffo_pairs = ex.sum_pair(B.ffo_src, B.ffo_pair)

    @pl.loop(0, 4)
    def _(q):
        terms = contract_rows(B.u2[:, columns(q * 128, 128)], B.g_all[...].reshape(1024, 1024))
        B.down_src[q] = terms.astype(BF)

    down_copies = [ex.send(B.down_src.at[q], B.down_terms.at[b], s, q) for q in ex.line()]

    @pl.loop(0, 8)
    def _(c):
        rows = B.h2_all[:, :, columns(c * 128, 128)].reshape(1024, 128)
        B.up_src[c] = contract_rows(rows, B.dz[...]).astype(BF).reshape(4, 32, 512)

    up_grads = [ex.send(B.up_src.at[:, q], B.up_terms.at[b], s, q) for q in ex.line()]

    dh2 = ex.sum_end(dh2_over, B.dh2_chips, B.total)
    sum_gain_c = column_sum(dh2 * B.normal_c[...])
    sum_shift_c = column_sum(dh2)
    held = s * 128 + lax.broadcasted_iota(jnp.int32, (128, 1), 0) < valid_rows
    g_local = g_in[...].astype(F32)
    dr = g_local + norm_back(dh2, gain_c, B.normal_c[...], inverse_c)
    B.dr[...] = dr
    da = norm_back(dr, gain_b, B.normal_b[...], inverse_b).astype(BF)
    B.da_all[s] = da
    B.do_local[...] = (times_transposed(da, B.out_w[...].reshape(1024, 1024)) * scale_in[0:1, :]).astype(BF)
    do_copies = [ex.send(B.do_local.at[:, columns(p * 128, 128)], B.do_all.at[s], p, b) for p in ex.plane()]
    own_do = ex.local(B.do_local.at[:, own_columns], B.do_all.at[s])
    da_slot = lambda i: B.da_all.at[i]
    da_copies = ex.gather_start(B.da_all.at[s], da_slot)
    ffo_over = ex.sum_chips(ffo_pairs, B.ffo_src, B.ffo_pair, B.ffo_paired, B.ffo_chips, B.ffo_total)
    sum_gain_b = column_sum(dr * B.normal_b[...])
    sum_shift_b = column_sum(dr)
    sum_g = column_sum(g_local)
    sum_da = column_sum(da.astype(F32))
    B.dk[...] = jnp.zeros((1024, 128), F32)
    B.dv[...] = jnp.zeros((1024, 128), F32)
    ex.arrived(do_copies)
    own_do.wait()

    scale_sums = jnp.zeros((1, 128), F32)
    for size in (512, 1024):
        for h in range(2):

            def back(t, sums, size=size, h=h):
                at = pl.ds(t * 128, 128)
                do = of_head(B.do_all[t], h)
                along = do.astype(F32) * B.attended[at, :]
                delta = jnp.sum(along, axis=-1, keepdims=True)
                kept = B.probs_low if size == 512 else B.probs_high
                probs = kept[h, pl.ds(t * 128 - size + 512, 128), :]
                dp = times_transposed(do, B.qkv[0:size, 256:384])
                ds = (probs * (dp - delta)).astype(BF)
                found = matmul(ds, of_head(B.qkv[0:size, 128:256], h))
                if h == 0:
                    B.dq[at, :] = found
                else:
                    B.dq[at, :] += found
                B.dk[0:size, :] += contract_rows(ds, of_head(B.qkv[at, 0:128], h))
                B.dv[0:size, :] += contract_rows(probs.astype(BF), do)
                return sums + column_sum(along)

            scale_sums = lax.fori_loop(size // 128 - 4, size // 128, back, scale_sums)

    def join(t, sums):
        at = pl.ds(t * 128, 128)
        dq = (B.dq[at, :] * score_scale).astype(BF)
        dk = (B.dk[at, :] * score_scale).astype(BF)
        dv = B.dv[at, :].astype(BF)
        B.dqkv[at, 0:128] = dq
        B.dqkv[at, 128:256] = dk
        B.dqkv[at, 256:384] = dv
        B.dh1_src[t] = times_transposed(B.dqkv[at, :], B.qkv_w[...].reshape(1024, 384)).astype(BF)
        return (sums[0] + column_sum(dq.astype(F32)), sums[1] + column_sum(dv.astype(F32)))

    blank = jnp.zeros((1, 128), F32)
    sum_dq, sum_dv = lax.fori_loop(0, 8, join, (blank, blank))
    dh1_pairs = ex.sum_pair(B.dh1_src, B.dh1_pair)

    @pl.loop(0, 8)
    def _(c):
        terms = contract_rows(B.h1[:, columns(c * 128, 128)], B.dqkv[...])
        B.qkv_src[c] = terms.astype(BF).reshape(4, 32, 384)

    qkv_grads = [ex.send(B.qkv_src.at[:, q], B.qkv_terms.at[b], s, q) for q in ex.line()]
    dh1_over = ex.sum_chips(dh1_pairs, B.dh1_src, B.dh1_pair, B.dh1_paired, B.dh1_chips, B.total)
    da_passed = ex.gather_forward(da_copies, da_slot)
    ffo = ex.sum_end(ffo_over, B.ffo_chips, B.ffo_total)
    output[...] = jnp.where(held, B.residual[...] + ffo + bias_out, 0.0).astype(BF)
    ex.arrived(da_passed)
    terms = contract_rows(B.scaled[...].reshape(1024, 128), B.da_all[...].reshape(1024, 1024))
    B.out_src[...] = terms.astype(BF).reshape(4, 32, 1024)
    out_grads = [ex.send(B.out_src.at[q], B.out_terms.at[b], s, q) for q in ex.line()]

    def line_sum(copies, mine, landed):
        ex.arrived(copies)
        total = mine
        for k in (1, 2, 3):
            total = total + landed[(b + k) % 4].astype(F32)
        return total

    grad_down[...] = line_sum(down_copies, B.down_src[b].astype(F32), B.down_terms)
    B.up_own[...] = line_sum(up_grads, B.up_src[:, b].astype(F32), B.up_terms).astype(BF)
    up_lanes = B.up_fin.at[:, columns(s * 512, 512)]
    up_copies = [ex.send(B.up_own.at[p], up_lanes, p, b) for p in ex.plane()]
    own_up = ex.local(B.up_own.at[s], up_lanes)

    dh1 = ex.sum_end(dh1_over, B.dh1_chips, B.total)
    normal_a, inverse_a = centred(x_in[...].astype(F32))
    grad_input[...] = (B.dr[...] + norm_back(dh1, gain_a, normal_a, inverse_a)).astype(BF)
    wide = jnp.concatenate(
        [
            column_sum(dh1 * normal_a),
            sum_gain_b,
            sum_gain_c,
            column_sum(dh1),
            sum_shift_b,
            sum_shift_c,
            jnp.zeros((1, 1024), F32),
            sum_g,
            jnp.zeros((1, 1024), F32),
            sum_da,
            jnp.zeros((6, 1024), F32),
        ],
        axis=0,
    )
    lane = lax.broadcasted_iota(jnp.int32, (1, 128), 1)
    by_head = jnp.zeros((1, 128), F32)
    for h in range(2):
        found = jnp.sum(of_head(scale_sums / own_scale, h), axis=-1, keepdims=True)
        by_head = jnp.where(lane == s * 2 + h, found, by_head)
    place = lax.broadcasted_iota(jnp.int32, (16, 128), 0)
    for p in range(8):
        mine = jnp.where(s == p, 1.0, 0.0)
        tile = wide[:, p * 128 : (p + 1) * 128]
        tile = jnp.where(place == 6, sum_dq * mine, tile)
        tile = jnp.where(place == 8, sum_dv * mine, tile)
        B.close_src[p] = jnp.where(place == 10, by_head, tile)
    for q in range(4):
        part = [one[:, q * 128 : (q + 1) * 128] for one in ff_sums]
        B.ff_src[q] = jnp.concatenate(part + [jnp.zeros((5, 128), F32)], axis=0)
    close = [ex.send(B.close_src.at[p], B.close_all.at[me], p, q) for p, q in partners]
    close_ff = [ex.send(B.ff_src.at[q], B.ff_all.at[b], s, q) for q in ex.line()]
    own_close = [ex.local(B.close_src.at[s], B.close_all.at[me]), ex.local(B.ff_src.at[b], B.ff_all.at[b])]

    B.qkv_own[...] = line_sum(qkv_grads, B.qkv_src[:, b].astype(F32), B.qkv_terms).astype(BF)
    qkv_lanes = lambda t: B.qkv_fin.at[:, columns(t * 1024 + s * 128, 128)]
    qkv_piece = lambda p, t: B.qkv_own.at[p, :, pl.ds(t * 128, 128)]
    qkv_copies = [ex.send(qkv_piece(p, t), qkv_lanes(t), p, b) for p in ex.plane() for t in range(3)]
    own_qkv = [ex.local(qkv_piece(s, t), qkv_lanes(t)) for t in range(3)]
    grad_out[...] = line_sum(out_grads, B.out_src[b].astype(F32), B.out_terms)
    ex.arrived(up_copies)
    own_up.wait()
    grad_up[...] = B.up_fin[...].astype(F32)
    ex.arrived(close)
    ex.arrived(close_ff)
    for one in own_close:
        one.wait()
    total = B.close_all[0]
    for i in range(1, 32):
        total = total + B.close_all[i]
    vec_out[...] = total
    ff_out[...] = B.ff_all[0] + B.ff_all[1] + B.ff_all[2] + B.ff_all[3]
    ex.arrived(qkv_copies)
    for one in own_qkv:
        one.wait()
    grad_qkv[...] = B.qkv_fin[...].astype(F32)
    ex.finish()


def plane_shards(
    inputs,
    lengths,
    w_qkv,
    w_out,
    w_up,
    w_down,
    norm_gains,
    model_biases,
    attn_biases,
    ff_gain,
    ff_biases,
    head_scale,
    cotangent,
):
    b = lax.axis_index("batch")
    narrow = jnp.concatenate([norm_gains, model_biases, attn_biases]).astype(F32)
    lanes = jnp.arange(128, dtype=jnp.int32) // 32
    spread = jnp.where(lanes[None] == b, jnp.tile(narrow, (1, 4)), 0.0)
    vectors = jnp.concatenate(
        [spread, ff_gain[None].astype(F32), ff_biases.astype(F32), jnp.zeros((3, 128), F32)]
    )
    positions = lax.axis_index("seq") * 128 + jnp.arange(128, dtype=jnp.int32)
    g_rows = jnp.where((positions < lengths[0])[:, None], cotangent[0], jnp.zeros((), BF))
    near = pl.BlockSpec(memory_space=pltpu.VMEM)
    outs = [
        ((128, 1024), BF),
        ((128, 1024), BF),
        ((32, 3072), F32),
        ((32, 1024), F32),
        ((32, 4096), F32),
        ((128, 1024), F32),
        ((16, 128), F32),
        ((8, 128), F32),
    ]
    found = pl.pallas_call(
        block_kernel,
        name="block",
        out_shape=[jax.ShapeDtypeStruct(shape, dtype) for shape, dtype in outs],
        in_specs=[pl.BlockSpec(memory_space=pltpu.SMEM)] + [near] * (INPUTS - 1),
        out_specs=[near] * OUTPUTS,
        scratch_shapes=[pltpu.VMEM(shape, dtype) for shape, dtype in BUFFERS.values()]
        + [
            pltpu.SemaphoreType.DMA((COPIES,)),
            pltpu.SemaphoreType.DMA((COPIES,)),
            pltpu.SemaphoreType.DMA((32,)),
        ],
        compiler_params=pltpu.CompilerParams(
            collective_id=1, has_side_effects=True, vmem_limit_bytes=67043328
        ),
    )(
        lengths.reshape(1, 1),
        inputs[0],
        g_rows,
        w_qkv,
        w_out,
        w_up,
        w_down,
        vectors,
        jnp.repeat(head_scale.astype(F32), HD).reshape(1, 1024),
    )
    output, grad_input, grad_qkv, grad_out, grad_up, grad_down, narrow, wide = found
    narrow_own = lax.dynamic_slice_in_dim(narrow, b * 32, 32, 1)
    return (
        output[None],
        grad_input[None],
        grad_qkv,
        grad_out,
        grad_up,
        grad_down,
        narrow_own[0:3],
        narrow_own[3:8],
        narrow_own[8:10],
        wide[0],
        wide[1:3],
        narrow[10, :H],
    )


def solution(mesh):
    in_plane = mesh.shape["seq"] == 8 and mesh.shape["batch"] == 4
    return jax.shard_map(
        plane_shards if in_plane else shards,
        mesh=mesh,
        in_specs=(
            P("batch", "seq", None),
            P("batch"),
            P(("seq", "batch"), None),
            P(("seq", "batch"), None),
            P(("seq", "batch"), None),
            P(("seq", "batch"), None),
            P(None, ("seq", "batch")),
            P(None, ("seq", "batch")),
            P(None, ("seq", "batch")),
            P(("seq", "batch")),
            P(None, ("seq", "batch")),
            P(),
            P("batch", "seq", None),
        ),
        out_specs=(
            P("batch", "seq", None),
            P("batch", "seq", None),
            P(("seq", "batch"), None),
            P(("seq", "batch"), None),
            P(("seq", "batch"), None),
            P(("seq", "batch"), None),
            P(None, ("seq", "batch")),
            P(None, ("seq", "batch")),
            P(None, ("seq", "batch")),
            P(("seq", "batch")),
            P(None, ("seq", "batch")),
            P(),
        ),
        check_vma=False,
    )
```

```python
import jax
import jax.numpy as jnp
from jax import lax
from jax.experimental import pallas as pl
from jax.experimental.pallas import tpu as pltpu
from jax.sharding import PartitionSpec as P

H = 16
HD = 64


NORM_EPSILON = 1e-05


def layer_norm(vector, norm_gain, norm_bias):
    centered = vector - jnp.mean(vector, axis=-1, keepdims=True)
    spread = jnp.mean(centered * centered, axis=-1, keepdims=True)
    return centered * lax.rsqrt(spread + NORM_EPSILON) * norm_gain + norm_bias


def gelu_norm(hidden, norm_gain, norm_bias):
    return layer_norm(jax.nn.gelu(hidden, approximate=False), norm_gain, norm_bias)


def contract_rows(left, right):
    return lax.dot_general(
        left, right, (((0,), (0,)), ((), ())), preferred_element_type=jnp.float32
    )


def times_transposed(left, right):
    return lax.dot_general(
        left, right, (((1,), (1,)), ((), ())), preferred_element_type=jnp.float32
    )


def shards(
    inputs,
    lengths,
    w_qkv,
    w_out,
    w_up,
    w_down,
    norm_gains,
    model_biases,
    attn_biases,
    ff_gain,
    ff_biases,
    head_scale,
    cotangent,
):
    gathered = (
        lax.all_gather(w_qkv, ("seq", "batch"), axis=0, tiled=True),
        lax.all_gather(w_out, ("seq", "batch"), axis=0, tiled=True),
        lax.all_gather(w_up, ("seq", "batch"), axis=0, tiled=True),
        lax.all_gather(w_down, ("seq", "batch"), axis=0, tiled=True),
        lax.all_gather(norm_gains, ("seq", "batch"), axis=1, tiled=True),
        lax.all_gather(model_biases, ("seq", "batch"), axis=1, tiled=True),
        lax.all_gather(attn_biases, ("seq", "batch"), axis=1, tiled=True),
        lax.all_gather(ff_gain, ("seq", "batch"), axis=0, tiled=True),
        lax.all_gather(ff_biases, ("seq", "batch"), axis=1, tiled=True),
    )
    qkv_full, out_full, up_full, down_full = (gathered[0], gathered[1], gathered[2], gathered[3])
    gain_rows = gathered[4].astype(jnp.float32)
    bias_rows = gathered[5].astype(jnp.float32)
    attn_rows = gathered[6].astype(jnp.float32)
    ffn_gain = gathered[7].astype(jnp.float32)
    ffn_rows = gathered[8].astype(jnp.float32)
    scales = head_scale.astype(jnp.float32)
    local_rows = inputs.shape[1]
    model_width = inputs.shape[2]
    seq_length = local_rows * lax.axis_size("seq")
    tile_rows = min(512, seq_length)
    first_row = lax.axis_index("seq") * local_rows
    valid_rows = lengths[0]
    positions = first_row + jnp.arange(local_rows, dtype=jnp.int32)
    valid_mask = (positions < valid_rows)[:, None]
    score_scale = HD ** (-0.5)
    residual_in = inputs[0].astype(jnp.float32)
    normed, norm_a_pull = jax.vjp(layer_norm, residual_in, gain_rows[0], bias_rows[0])
    normed_low = normed.astype(jnp.bfloat16)
    offsets = jnp.concatenate([bias_rows[3], jnp.zeros_like(bias_rows[3]), attn_rows[0]])
    projected = (
        jnp.dot(normed_low, qkv_full, preferred_element_type=jnp.float32) + offsets
    ).astype(jnp.bfloat16)
    queries = projected[:, :model_width]
    key_local = projected[:, model_width : 2 * model_width]
    value_local = projected[:, 2 * model_width :]
    key_rows, value_rows = (
        lax.all_gather(key_local, "seq", axis=0, tiled=True),
        lax.all_gather(value_local, "seq", axis=0, tiled=True),
    )
    query_heads = queries.reshape(local_rows, H, HD)
    last_needed = jnp.minimum(first_row + local_rows - 1, valid_rows - 1)
    tile_count = last_needed // tile_rows + 1

    def tile_scores(j):
        start = j * tile_rows
        key_tile = lax.dynamic_slice_in_dim(key_rows, start, tile_rows, 0).reshape(tile_rows, H, HD)
        scores = (
            jnp.einsum("qhd,khd->hqk", query_heads, key_tile, preferred_element_type=jnp.float32)
            * score_scale
        )
        key_index = start + jnp.arange(tile_rows, dtype=jnp.int32)
        allowed = (key_index[None, :] <= positions[:, None]) & (key_index[None, :] < valid_rows)
        return (scores, allowed[None], key_tile)

    def max_and_sum(j, carry):
        running_max, running_sum = carry
        scores, allowed, unused_tile = tile_scores(j)
        masked = jnp.where(allowed, scores, -1e30)
        new_max = jnp.maximum(running_max, jnp.max(masked, axis=-1))
        kept_terms = jnp.where(allowed, jnp.exp(masked - new_max[..., None]), 0.0)
        return (
            new_max,
            running_sum * jnp.exp(running_max - new_max) + jnp.sum(kept_terms, axis=-1),
        )

    start_stats = (
        jnp.full((H, local_rows), -1e30, jnp.float32),
        jnp.zeros((H, local_rows), jnp.float32),
    )
    running_max, running_sum = lax.fori_loop(0, tile_count, max_and_sum, start_stats)
    log_total = running_max + jnp.log(running_sum)

    def tile_probs(j):
        scores, allowed, key_tile = tile_scores(j)
        attn_probs = jnp.where(allowed, jnp.exp(scores - log_total[..., None]), 0.0)
        value_tile = lax.dynamic_slice_in_dim(value_rows, j * tile_rows, tile_rows, 0).reshape(
            tile_rows, H, HD
        )
        return (attn_probs, key_tile, value_tile)

    def accumulate(j, summed):
        attn_probs, unused_tile, value_tile = tile_probs(j)
        return summed + jnp.einsum(
            "hqk,khd->qhd",
            attn_probs.astype(jnp.bfloat16),
            value_tile,
            preferred_element_type=jnp.float32,
        )

    attended = lax.fori_loop(0, tile_count, accumulate, jnp.zeros((local_rows, H, HD), jnp.float32))
    scaled_low = (
        (attended * scales[None, :, None]).reshape(local_rows, model_width).astype(jnp.bfloat16)
    )
    attn_proj = jnp.dot(scaled_low, out_full, preferred_element_type=jnp.float32) + attn_rows[1]
    attn_normed, norm_b_pull = jax.vjp(layer_norm, attn_proj, gain_rows[1], bias_rows[1])
    residual = residual_in + attn_normed
    ffn_in, norm_c_pull = jax.vjp(layer_norm, residual, gain_rows[2], bias_rows[2])
    ffn_low = ffn_in.astype(jnp.bfloat16)
    hidden = jnp.dot(ffn_low, up_full, preferred_element_type=jnp.float32) + ffn_rows[0]
    ffn_normed, ffn_pull = jax.vjp(gelu_norm, hidden, ffn_gain, ffn_rows[1])
    ffn_out_low = ffn_normed.astype(jnp.bfloat16)
    combined = jnp.where(
        valid_mask,
        residual
        + jnp.dot(ffn_out_low, down_full, preferred_element_type=jnp.float32)
        + bias_rows[4],
        0.0,
    )
    output = combined.astype(jnp.bfloat16)[None]
    barrier_out = lax.optimization_barrier(((w_qkv, w_out, w_up, w_down), combined))
    regathered = (
        lax.all_gather(barrier_out[0][0], ("seq", "batch"), axis=0, tiled=True),
        lax.all_gather(barrier_out[0][1], ("seq", "batch"), axis=0, tiled=True),
        lax.all_gather(barrier_out[0][2], ("seq", "batch"), axis=0, tiled=True),
        lax.all_gather(barrier_out[0][3], ("seq", "batch"), axis=0, tiled=True),
    )
    qkv_full, out_full, up_full, down_full = (
        regathered[0],
        regathered[1],
        regathered[2],
        regathered[3],
    )
    cotan_rows = jnp.where(valid_mask, cotangent[0], jnp.zeros_like(cotangent[0]))
    cotan_float = cotan_rows.astype(jnp.float32)
    grad_down = contract_rows(ffn_out_low, cotan_rows)
    grad_bias_out = jnp.sum(cotan_float, axis=0)
    grad_ffn_normed = times_transposed(cotan_rows, down_full)
    grad_hidden, grad_ffn_gain, grad_ffn_shift = ffn_pull(grad_ffn_normed)
    grad_hidden_low = grad_hidden.astype(jnp.bfloat16)
    grad_up = contract_rows(ffn_low, grad_hidden_low)
    grad_ffn_bias = jnp.sum(grad_hidden_low.astype(jnp.float32), axis=0)
    grad_ffn_in = times_transposed(grad_hidden_low, up_full)
    grad_from_ffn, grad_gain_c, grad_shift_c = norm_c_pull(grad_ffn_in)
    grad_residual = cotan_float + grad_from_ffn
    grad_proj, grad_gain_b, grad_shift_b = norm_b_pull(grad_residual)
    grad_proj_low = grad_proj.astype(jnp.bfloat16)
    grad_out_bias = jnp.sum(grad_proj_low.astype(jnp.float32), axis=0)
    grad_out = contract_rows(scaled_low, grad_proj_low)
    grad_scaled = times_transposed(grad_proj_low, out_full).reshape(local_rows, H, HD)
    grad_scales = jnp.sum(grad_scaled * attended, axis=(0, 2))
    grad_heads_low = (grad_scaled * scales[None, :, None]).astype(jnp.bfloat16)
    row_delta = jnp.einsum("qhd,qhd->hq", grad_heads_low.astype(jnp.float32), attended)

    def score_grads(j):
        attn_probs, key_tile, value_tile = tile_probs(j)
        grad_probs = jnp.einsum(
            "qhd,khd->hqk", grad_heads_low, value_tile, preferred_element_type=jnp.float32
        )
        grad_scores = (attn_probs * (grad_probs - row_delta[..., None])).astype(jnp.bfloat16)
        return (attn_probs, grad_scores, key_tile)

    def backward_tile(j, carry):
        grad_query, terms = carry
        attn_probs, grad_scores, key_tile = score_grads(j)
        grad_query = grad_query + jnp.einsum(
            "hqk,khd->qhd", grad_scores, key_tile, preferred_element_type=jnp.float32
        )
        grad_key = (
            jnp.einsum("hqk,qhd->khd", grad_scores, query_heads, preferred_element_type=jnp.float32)
            * score_scale
        )
        grad_value = jnp.einsum(
            "hqk,qhd->khd",
            attn_probs.astype(jnp.bfloat16),
            grad_heads_low,
            preferred_element_type=jnp.float32,
        )
        piece = jnp.concatenate(
            [grad_key.reshape(tile_rows, model_width), grad_value.reshape(tile_rows, model_width)],
            axis=1,
        )
        return (grad_query, lax.dynamic_update_slice_in_dim(terms, piece, j * tile_rows, 0))

    start_carry = (
        jnp.zeros((local_rows, H, HD), jnp.float32),
        jnp.zeros((seq_length, 2 * model_width), jnp.float32),
    )
    grad_query, terms = lax.fori_loop(0, tile_count, backward_tile, start_carry)
    grad_kv = lax.psum_scatter(terms, "seq", scatter_dimension=0, tiled=True)
    grad_query_low = (
        (grad_query * score_scale).reshape(local_rows, model_width).astype(jnp.bfloat16)
    )
    grad_kv_low = grad_kv.astype(jnp.bfloat16)
    grad_projected = jnp.concatenate([grad_query_low, grad_kv_low], axis=1)
    grad_qkv = contract_rows(normed_low, grad_projected)
    grad_query_bias = jnp.sum(grad_query_low.astype(jnp.float32), axis=0)
    grad_value_bias = jnp.sum(grad_kv_low[:, model_width:].astype(jnp.float32), axis=0)
    grad_normed = times_transposed(grad_projected, qkv_full)
    grad_from_attn, grad_gain_a, grad_shift_a = norm_a_pull(grad_normed)
    grad_input = (grad_residual + grad_from_attn).astype(jnp.bfloat16)[None]
    reduced = (
        lax.psum_scatter(grad_qkv, ("seq", "batch"), scatter_dimension=0, tiled=True),
        lax.psum_scatter(grad_out, ("seq", "batch"), scatter_dimension=0, tiled=True),
        lax.psum_scatter(grad_up, ("seq", "batch"), scatter_dimension=0, tiled=True),
        lax.psum_scatter(grad_down, ("seq", "batch"), scatter_dimension=0, tiled=True),
        lax.psum_scatter(
            jnp.stack([grad_gain_a, grad_gain_b, grad_gain_c]),
            ("seq", "batch"),
            scatter_dimension=1,
            tiled=True,
        ),
        lax.psum_scatter(
            jnp.stack([grad_shift_a, grad_shift_b, grad_shift_c, grad_query_bias, grad_bias_out]),
            ("seq", "batch"),
            scatter_dimension=1,
            tiled=True,
        ),
        lax.psum_scatter(
            jnp.stack([grad_value_bias, grad_out_bias]),
            ("seq", "batch"),
            scatter_dimension=1,
            tiled=True,
        ),
        lax.psum_scatter(grad_ffn_gain, ("seq", "batch"), scatter_dimension=0, tiled=True),
        lax.psum_scatter(
            jnp.stack([grad_ffn_bias, grad_ffn_shift]),
            ("seq", "batch"),
            scatter_dimension=1,
            tiled=True,
        ),
    )
    scale_total = lax.psum(grad_scales, ("seq", "batch"))
    return (
        output,
        grad_input,
        reduced[0],
        reduced[1],
        reduced[2],
        reduced[3],
        reduced[4],
        reduced[5],
        reduced[6],
        reduced[7],
        reduced[8],
        scale_total,
    )


BF = jnp.bfloat16
F32 = jnp.float32


class Exchange:
    def __init__(self, send_sems, recv_sems, local_sems):
        self.send_sems = send_sems
        self.recv_sems = recv_sems
        self.local_sems = local_sems
        self.count = 0
        self.locals = 0
        self.sent = []
        self.sent_if = []
        self.s = lax.axis_index("seq")
        self.b = lax.axis_index("batch")
        self.chip = self.s // 2
        self.core = self.s % 2
        self.sibling = self.chip * 2 + 1 - self.core

    def send(self, src, dst, seq, batch):
        at = self.count
        self.count += 1
        copy = pltpu.make_async_remote_copy(
            src_ref=src,
            dst_ref=dst,
            send_sem=self.send_sems.at[at],
            recv_sem=self.recv_sems.at[at],
            device_id=(seq, batch),
            device_id_type=pl.DeviceIdType.MESH,
        )
        copy.start()
        self.sent.append(copy)
        return copy

    def describe(self, src, dst, seq, batch, sent_at, recv_at):
        return pltpu.make_async_remote_copy(
            src_ref=src,
            dst_ref=dst,
            send_sem=self.send_sems.at[sent_at],
            recv_sem=self.recv_sems.at[recv_at],
            device_id=(seq, batch),
            device_id_type=pl.DeviceIdType.MESH,
        )

    def send_if(self, held, copy):
        @pl.when(held)
        def _():
            copy.start()

        self.sent_if.append((held, copy))

    def line_start(self, src, slot):
        first = self.count
        self.count += 4
        b = self.b
        copies = [
            self.describe(src, slot(b), self.s, (b + k) % 4, first + k - 1, first + k - 1) for k in (1, 2, 3)
        ]
        self.send_if(b != 3, copies[0])
        self.send_if(b != 0, copies[2])
        copies[1].start()
        self.sent.append(copies[1])
        return copies, slot, first

    def line_relay(self, line):
        copies, slot, first = line
        b = self.b

        @pl.when((b == 1) | (b == 2))
        def _():
            copies[1].wait_recv()

        came = slot((b + 2) % 4)
        self.send_if(b == 1, self.describe(came, came, self.s, 0, first + 3, first))
        self.send_if(b == 2, self.describe(came, came, self.s, 3, first + 3, first + 2))

    def line_arrived(self, line):
        copies, _slot, _first = line
        copies[0].wait_recv()
        copies[2].wait_recv()

        @pl.when((self.b == 0) | (self.b == 3))
        def _():
            copies[1].wait_recv()

    def terms_start(self, view, landed, passing):
        first = self.count
        self.count += 4
        b = self.b
        at = lambda q, k: self.describe(view(q), landed.at[b], self.s, q, first + k - 1, first + k - 1)
        up, over, down = at((b + 1) % 4, 1), at((b + 2) % 4, 2), at((b + 3) % 4, 3)
        to_one = self.describe(view(3), passing, self.s, 1, first + 3, first + 3)
        to_two = self.describe(view(0), passing, self.s, 2, first + 3, first + 3)
        self.send_if(b == 0, to_one)
        self.send_if(b == 3, to_two)
        self.send_if((b == 0) | (b == 3), over)
        self.send_if(b != 3, up)
        self.send_if(b != 0, down)
        return up, over, down, to_one, landed, passing, first

    def terms_relay(self, terms, mine, joined):
        up, over, down, to_one, landed, passing, first = terms
        b = self.b
        held = (b == 1) | (b == 2)

        @pl.when(held)
        def _():
            to_one.wait_recv()
            joined[...] = (mine((b + 2) % 4).astype(F32) + passing[...].astype(F32)).astype(BF)

        self.send_if(
            held, self.describe(joined, landed.at[b], self.s, (b + 2) % 4, first + 1, first + 1)
        )

    def terms_arrived(self, terms):
        up, over, down = terms[:3]
        over.wait_recv()

        @pl.when(self.b != 0)
        def _():
            up.wait_recv()

        @pl.when(self.b != 3)
        def _():
            down.wait_recv()

    def local(self, src, dst):
        at = self.locals
        self.locals += 1
        copy = pltpu.make_async_copy(src, dst, self.local_sems.at[at])
        copy.start()
        return copy

    def arrived(self, copies):
        for copy in copies:
            copy.wait_recv()

    def finish(self):
        for copy in self.sent:
            copy.wait_send()
        for held, copy in self.sent_if:
            pl.when(held)(copy.wait_send)

    def peer(self, k):
        return ((self.chip + k) % 4) * 2 + self.core

    def source(self, k):
        return ((self.chip + 4 - k) % 4) * 2 + self.core

    def plane(self):
        return [(self.s + j) % 8 for j in range(1, 8)]

    def line(self):
        return [(self.b + k) % 4 for k in range(1, 4)]

    def gather_start(self, src, slot):
        copies = [self.send(src, slot(self.s), self.peer(k), self.b) for k in (1, 2, 3)]
        copies.append(self.send(src, slot(self.s), self.sibling, self.b))
        return copies

    def gather_forward(self, copies, slot):
        passed = []
        for k in (1, 2, 3):
            copies[k - 1].wait_recv()
            came = slot(self.source(k))
            passed.append(self.send(came, came, self.sibling, self.b))
        return [copies[3]] + passed

    def sum_pair(self, src, from_pair):
        return [
            self.send(src.at[((self.chip + k) % 4) * 2 + 1 - self.core], from_pair.at[k], self.sibling, self.b)
            for k in (1, 2, 3, 0)
        ]

    def sum_chips(self, copies, src, from_pair, paired, from_chips, total):
        over = []
        for at, k in enumerate((1, 2, 3, 0)):
            copies[at].wait_recv()
            mine = src[((self.chip + k) % 4) * 2 + self.core].astype(F32)
            both = mine + from_pair[k].astype(F32)
            if k:
                paired[k - 1] = both.astype(BF)
                over.append(self.send(paired.at[k - 1], from_chips.at[k - 1], self.peer(k), self.b))
            else:
                total[...] = both
        return over

    def sum_end(self, over, from_chips, total):
        self.arrived(over)
        return total[...] + from_chips[0].astype(F32) + from_chips[1].astype(F32) + from_chips[2].astype(F32)


def columns(start, size):
    return pl.ds(pl.multiple_of(start, 128), size)


def centred(rows):
    middle = rows - jnp.mean(rows, axis=-1, keepdims=True)
    inverse = lax.rsqrt(jnp.mean(middle * middle, axis=-1, keepdims=True) + NORM_EPSILON)
    return middle * inverse, inverse


def norm_back(upstream, gain, normal, inverse):
    scaled = upstream * gain
    average = jnp.mean(scaled, axis=-1, keepdims=True)
    along = jnp.mean(scaled * normal, axis=-1, keepdims=True)
    return inverse * (scaled - average - normal * along)


def gelu_parts(z):
    phi = 0.5 * (1.0 + lax.erf(z * 0.7071067811865476))
    density = 0.3989422804014327 * jnp.exp(-0.5 * z * z)
    return z * phi, phi + z * density


def matmul(left, right):
    return jnp.dot(left, right, preferred_element_type=F32)


def column_sum(rows):
    return jnp.sum(rows, axis=0, keepdims=True)


def pack_columns(parts):
    lane = lax.broadcasted_iota(jnp.int32, (128, 128), 1)
    wide = jnp.zeros((128, 128), F32)
    for at, part in enumerate(parts):
        wide = jnp.where(lane == at, part, wide)
    return wide.T[:8]


BUFFERS = dict(
    x_all=((8, 128, 1024), BF),
    g_all=((8, 128, 1024), BF),
    qkv_w=((8, 4, 32, 384), BF),
    out_w=((8, 4, 32, 1024), BF),
    up_w=((8, 4, 32, 512), BF),
    down_w=((4, 128, 1024), BF),
    vec_src=((16, 128), F32),
    vec_all=((32, 16, 128), F32),
    scale_row=((8, 1024), F32),
    rows=((16, 1024), F32),
    ff_rows=((8, 512), F32),
    h1=((1024, 1024), BF),
    qkv=((1024, 384), BF),
    probs_low=((2, 512, 512), F32),
    probs_high=((2, 512, 1024), F32),
    attended=((1024, 128), F32),
    scaled=((8, 128, 128), BF),
    scaled_local=((128, 1024), BF),
    normal_b=((128, 1024), F32),
    normal_c=((128, 1024), F32),
    residual=((128, 1024), F32),
    h2_all=((8, 128, 1024), BF),
    active=((1024, 512), F32),
    slope=((1024, 512), F32),
    du2=((1024, 512), F32),
    stats=((8, 8, 128), F32),
    stats_all=((8, 8, 8, 128), F32),
    u2=((1024, 512), BF),
    dz=((1024, 512), BF),
    dh2_pair=((4, 128, 1024), BF),
    dh2_paired=((3, 128, 1024), BF),
    dh2_chips=((3, 128, 1024), BF),
    ffo_src=((8, 128, 1024), BF),
    ffo_pair=((4, 128, 1024), BF),
    ffo_paired=((3, 128, 1024), BF),
    ffo_chips=((3, 128, 1024), BF),
    dh1_src=((8, 128, 1024), BF),
    dh1_pair=((4, 128, 1024), BF),
    dh1_paired=((3, 128, 1024), BF),
    dh1_chips=((3, 128, 1024), BF),
    total=((128, 1024), F32),
    ffo_total=((128, 1024), F32),
    dr=((128, 1024), F32),
    da_all=((8, 128, 1024), BF),
    do_local=((128, 1024), BF),
    do_all=((8, 128, 128), BF),
    dq=((1024, 128), F32),
    dk=((1024, 128), F32),
    dv=((1024, 128), F32),
    dqkv=((1024, 384), BF),
    up_src=((8, 4, 32, 512), BF),
    up_terms=((4, 8, 32, 512), BF),
    down_src=((4, 128, 1024), BF),
    down_terms=((4, 128, 1024), BF),
    qkv_src=((8, 4, 32, 384), BF),
    qkv_terms=((4, 8, 32, 384), BF),
    up_passing=((8, 32, 512), BF),
    up_joined=((8, 32, 512), BF),
    down_passing=((128, 1024), BF),
    down_joined=((128, 1024), BF),
    qkv_passing=((8, 32, 384), BF),
    qkv_joined=((8, 32, 384), BF),
    out_src=((4, 32, 1024), BF),
    out_terms=((4, 32, 1024), BF),
    up_own=((8, 32, 512), BF),
    up_fin=((32, 4096), BF),
    qkv_own=((8, 32, 384), BF),
    qkv_fin=((32, 3072), BF),
    close_src=((8, 16, 128), F32),
    close_all=((32, 16, 128), F32),
    ff_src=((4, 8, 128), F32),
    ff_all=((4, 8, 128), F32),
)
COPIES = 240
INPUTS = 13
OUTPUTS = 8


def block_kernel(
    length_in,
    x_in,
    g_in,
    qkv_in,
    out_in,
    up_in,
    down_in,
    gains_in,
    biases_in,
    attn_in,
    ff_gain_in,
    ff_bias_in,
    scale_in,
    *refs,
):
    output, grad_input, grad_qkv, grad_out, grad_up, grad_down, vec_out, ff_out = refs[:OUTPUTS]
    B = type("Buffers", (), dict(zip(BUFFERS, refs[OUTPUTS : OUTPUTS + len(BUFFERS)])))
    ex = Exchange(*refs[OUTPUTS + len(BUFFERS) :])
    s, b = ex.s, ex.b
    me = s * 4 + b
    valid_rows = length_in[0, 0]

    lane = lax.broadcasted_iota(jnp.int32, (1, 128), 1)

    def spread(part):
        values = part[...].astype(F32)
        return jnp.where(lane // 32 == b, jnp.concatenate([values] * 4, axis=1), 0.0)

    B.vec_src[0:3, :] = spread(gains_in)
    B.vec_src[3:8, :] = spread(biases_in)
    B.vec_src[8:10, :] = spread(attn_in)
    B.vec_src[10:11, :] = ff_gain_in[...].astype(F32)
    B.vec_src[11:13, :] = ff_bias_in[...].astype(F32)
    B.vec_src[13:16, :] = jnp.zeros((3, 128), F32)
    held = s * 128 + lax.broadcasted_iota(jnp.int32, (128, 1), 0) < valid_rows
    B.g_all[s] = jnp.where(held, g_in[...].astype(F32), 0.0).astype(BF)
    by_head = lax.broadcasted_iota(jnp.int32, (8, 1024), 1) // HD
    head_scales = scale_in[...].astype(F32)
    scale_row = jnp.zeros((8, 1024), F32)
    for h in range(H):
        scale_row = jnp.where(by_head == h, head_scales[0:1, h : h + 1], scale_row)
    B.scale_row[...] = scale_row

    for landed in (B.up_terms, B.down_terms, B.qkv_terms):

        @pl.when(b == 3)
        def _():
            landed[0] = jnp.zeros(landed.shape[1:], BF)

        @pl.when(b == 0)
        def _():
            landed[3] = jnp.zeros(landed.shape[1:], BF)

    barrier = pltpu.get_barrier_semaphore()
    partners = [((s + j // 4) % 8, (b + j % 4) % 4) for j in range(1, 32)]
    for seq, batch in partners:
        pl.semaphore_signal(barrier, inc=1, device_id=(seq, batch), device_id_type=pl.DeviceIdType.MESH)
    pl.semaphore_wait(barrier, len(partners))

    qkv_part = lambda p, t: qkv_in.at[:, columns(t * 1024 + p * 128, 128)]
    qkv_slot = lambda t: B.qkv_w.at[s, b, :, pl.ds(t * 128, 128)]
    qkv_copies = [ex.send(qkv_part(p, t), qkv_slot(t), p, b) for p in ex.plane() for t in range(3)]
    own = [ex.local(qkv_part(s, t), qkv_slot(t)) for t in range(3)]
    own_up = ex.local(up_in.at[:, columns(s * 512, 512)], B.up_w.at[s, b])
    own_rest = [
        ex.local(out_in, B.out_w.at[s, b]),
        ex.local(x_in, B.x_all.at[s]),
        ex.local(down_in, B.down_w.at[b]),
        ex.local(B.vec_src, B.vec_all.at[me]),
    ]
    x_slot = lambda i: B.x_all.at[i]
    g_slot = lambda i: B.g_all.at[i]
    x_copies = ex.gather_start(x_in, x_slot)
    vec_copies = [ex.send(B.vec_src, B.vec_all.at[me], p, q) for p, q in partners]
    up_copies = [ex.send(up_in.at[:, columns(p * 512, 512)], B.up_w.at[s, b], p, b) for p in ex.plane()]
    ex.arrived(qkv_copies)
    for one in own:
        one.wait()
    qkv_line = ex.line_start(B.qkv_w.at[:, b], lambda i: B.qkv_w.at[:, i])
    x_passed = ex.gather_forward(x_copies, x_slot)
    ex.arrived(up_copies)
    own_up.wait()
    ex.line_relay(qkv_line)
    out_line = ex.line_start(out_in, lambda i: B.out_w.at[s, i])
    down_line = ex.line_start(down_in, lambda i: B.down_w.at[i])
    up_line = ex.line_start(B.up_w.at[:, b], lambda i: B.up_w.at[:, i])
    g_copies = ex.gather_start(B.g_all.at[s], g_slot)
    ex.arrived(vec_copies)
    for one in own_rest:
        one.wait()

    for p in range(8):
        group = B.vec_all[4 * p] + B.vec_all[4 * p + 1] + B.vec_all[4 * p + 2] + B.vec_all[4 * p + 3]
        B.rows[:, p * 128 : (p + 1) * 128] = group
    for q in range(4):
        B.ff_rows[:, q * 128 : (q + 1) * 128] = B.vec_all[s * 4 + q][8:16]
    row = lambda at: B.rows[at : at + 1, :]
    gain_a, gain_b, gain_c = row(0), row(1), row(2)
    bias_a, bias_b, bias_c, bias_out, bias_attn = row(3), row(4), row(5), row(7), row(9)
    ffn_gain, ffn_bias, ffn_shift = B.ff_rows[2:3, :], B.ff_rows[3:4, :], B.ff_rows[4:5, :]
    own_columns = columns(s * 128, 128)
    query_bias = B.rows[6:7, own_columns]
    value_bias = B.rows[8:9, own_columns]
    own_scale = B.scale_row[0:1, own_columns]

    ex.arrived(x_passed)

    @pl.loop(0, 8)
    def _(t):
        normal, _unused = centred(B.x_all[t].astype(F32))
        B.h1[pl.ds(t * 128, 128), :] = (normal * gain_a + bias_a).astype(BF)

    ex.line_arrived(qkv_line)
    offsets = jnp.concatenate([query_bias, jnp.zeros_like(query_bias), value_bias], axis=1)

    @pl.loop(0, 4)
    def _(t):
        at = pl.ds(t * 256, 256)
        B.qkv[at, :] = (matmul(B.h1[at, :], B.qkv_w[...].reshape(1024, 384)) + offsets).astype(BF)

    ex.line_relay(out_line)
    ex.line_arrived(out_line)
    out_slot = lambda i: B.out_w.at[i]
    out_copies = ex.gather_start(B.out_w.at[s], out_slot)
    g_passed = ex.gather_forward(g_copies, g_slot)

    score_scale = HD ** (-0.5)
    half_of = lax.broadcasted_iota(jnp.int32, (1, 128), 1) // HD

    def of_head(rows, h):
        return jnp.where(half_of == h, rows, jnp.zeros_like(rows))

    for size in (512, 1024):
        for h in range(2):

            @pl.loop(size // 128 - 4, size // 128)
            def _(t):
                at = pl.ds(t * 128, 128)
                scores = times_transposed(of_head(B.qkv[at, 0:128], h), B.qkv[0:size, 128:256]) * score_scale
                key_index = lax.broadcasted_iota(jnp.int32, (128, size), 1)
                query_index = t * 128 + lax.broadcasted_iota(jnp.int32, (128, size), 0)
                allowed = (key_index <= query_index) & (key_index < valid_rows)
                masked = jnp.where(allowed, scores, -1e30)
                raised = jnp.exp(masked - jnp.max(masked, axis=-1, keepdims=True))
                probs = raised * (1.0 / jnp.sum(raised, axis=-1, keepdims=True))
                kept = B.probs_low if size == 512 else B.probs_high
                kept[h, pl.ds(t * 128 - size + 512, 128), :] = probs
                found = matmul(probs.astype(BF), of_head(B.qkv[0:size, 256:384], h))
                if h == 0:
                    B.attended[at, :] = found
                else:
                    both = B.attended[at, :] + found
                    B.attended[at, :] = both
                    B.scaled[t] = (both * own_scale).astype(BF)

    local_lanes = B.scaled_local.at[:, own_columns]
    heads = [ex.send(B.scaled.at[p], local_lanes, p, b) for p in ex.plane()]
    own_heads = ex.local(B.scaled.at[s], local_lanes)
    out_passed = ex.gather_forward(out_copies, out_slot)
    ex.arrived(out_passed)
    ex.line_relay(down_line)
    ex.arrived(heads)
    own_heads.wait()

    attn_proj = matmul(B.scaled_local[...], B.out_w[...].reshape(1024, 1024)) + bias_attn
    normal_b, inverse_b = centred(attn_proj)
    B.normal_b[...] = normal_b
    residual = x_in[...].astype(F32) + normal_b * gain_b + bias_b
    B.residual[...] = residual
    normal_c, inverse_c = centred(residual)
    B.normal_c[...] = normal_c
    B.h2_all[s] = (normal_c * gain_c + bias_c).astype(BF)
    h2_slot = lambda i: B.h2_all.at[i]
    h2_copies = ex.gather_start(B.h2_all.at[s], h2_slot)

    ex.arrived(g_passed)
    ex.line_relay(up_line)
    ex.line_arrived(down_line)

    @pl.loop(0, 8)
    def _(t):
        B.du2[pl.ds(t * 128, 128), :] = times_transposed(B.g_all[t], B.down_w[...].reshape(512, 1024))

    h2_passed = ex.gather_forward(h2_copies, h2_slot)
    ex.line_arrived(up_line)
    ex.arrived(h2_passed)

    @pl.loop(0, 8)
    def _(t):
        at = pl.ds(t * 128, 128)
        hidden = matmul(B.h2_all[t], B.up_w[...].reshape(1024, 512)) + ffn_bias
        active, slope = gelu_parts(hidden)
        B.active[at, :] = active
        B.slope[at, :] = slope
        dgain = B.du2[at, :] * ffn_gain
        mean = jnp.mean(active, axis=-1, keepdims=True)
        off = active - mean
        add = lambda rows: jnp.sum(rows, axis=-1, keepdims=True)
        B.stats[t] = pack_columns([mean, add(off * off), add(dgain), add(dgain * off)])

    stats_copies = [ex.send(B.stats, B.stats_all.at[s], p, b) for p in ex.plane()]
    own_stats = ex.local(B.stats, B.stats_all.at[s])
    ex.arrived(stats_copies)
    own_stats.wait()

    for copy in x_passed[1:]:
        copy.wait_send()
        ex.sent = [one for one in ex.sent if one is not copy]

    def finish_hidden(t, sums):
        at = pl.ds(t * 128, 128)
        means = [B.stats_all[i, t, 0:1, :] for i in range(8)]
        squares = [B.stats_all[i, t, 1:2, :] for i in range(8)]
        firsts = [B.stats_all[i, t, 2:3, :] for i in range(8)]
        seconds = [B.stats_all[i, t, 3:4, :] for i in range(8)]
        mean = sum(means) * 0.125
        shifts = [one - mean for one in means]
        spread = (sum(squares) + 512.0 * sum(one * one for one in shifts)) * (1.0 / 4096.0)
        inverse = lax.rsqrt(spread + NORM_EPSILON)
        average = sum(firsts) * (1.0 / 4096.0)
        along = inverse * sum(two + one * first for two, one, first in zip(seconds, shifts, firsts)) * (1.0 / 4096.0)
        packed = jnp.concatenate([mean, inverse, average, along, jnp.zeros((124, 128), F32)], axis=0).T
        mean, inverse, average, along = (packed[:, i : i + 1] for i in range(4))
        normal = (B.active[at, :] - mean) * inverse
        B.u2[at, :] = (normal * ffn_gain + ffn_shift).astype(BF)
        du2 = B.du2[at, :]
        dz = (inverse * (du2 * ffn_gain - average - normal * along) * B.slope[at, :]).astype(BF)
        B.dz[at, :] = dz
        B.x_all[t] = times_transposed(dz, B.up_w[...].reshape(1024, 512)).astype(BF)
        return (
            sums[0] + column_sum(du2 * normal),
            sums[1] + column_sum(dz.astype(F32)),
            sums[2] + column_sum(du2),
        )

    nothing = jnp.zeros((1, 512), F32)
    ff_sums = lax.fori_loop(0, 8, finish_hidden, (nothing, nothing, nothing))
    dh2_pairs = ex.sum_pair(B.x_all, B.dh2_pair)

    @pl.loop(0, 8)
    def _(t):
        B.ffo_src[t] = matmul(B.u2[pl.ds(t * 128, 128), :], B.down_w[...].reshape(512, 1024)).astype(BF)

    dh2_over = ex.sum_chips(dh2_pairs, B.x_all, B.dh2_pair, B.dh2_paired, B.dh2_chips, B.total)
    ffo_pairs = ex.sum_pair(B.ffo_src, B.ffo_pair)

    @pl.loop(0, 4)
    def _(q):
        terms = contract_rows(B.u2[:, columns(q * 128, 128)], B.g_all[...].reshape(1024, 1024))
        B.down_src[q] = terms.astype(BF)

    down_grads = ex.terms_start(lambda q: B.down_src.at[q], B.down_terms, B.down_passing)

    @pl.loop(0, 8)
    def _(c):
        rows = B.h2_all[:, :, columns(c * 128, 128)].reshape(1024, 128)
        B.up_src[c] = contract_rows(rows, B.dz[...]).astype(BF).reshape(4, 32, 512)

    up_grads = ex.terms_start(lambda q: B.up_src.at[:, q], B.up_terms, B.up_passing)

    dh2 = ex.sum_end(dh2_over, B.dh2_chips, B.total)
    sum_gain_c = column_sum(dh2 * B.normal_c[...])
    sum_shift_c = column_sum(dh2)
    g_local = B.g_all[s].astype(F32)
    dr = g_local + norm_back(dh2, gain_c, B.normal_c[...], inverse_c)
    B.dr[...] = dr
    da = norm_back(dr, gain_b, B.normal_b[...], inverse_b).astype(BF)
    B.da_all[s] = da
    B.do_local[...] = (times_transposed(da, B.out_w[...].reshape(1024, 1024)) * B.scale_row[0:1, :]).astype(BF)
    do_copies = [ex.send(B.do_local.at[:, columns(p * 128, 128)], B.do_all.at[s], p, b) for p in ex.plane()]
    own_do = ex.local(B.do_local.at[:, own_columns], B.do_all.at[s])
    da_slot = lambda i: B.da_all.at[i]
    da_copies = ex.gather_start(B.da_all.at[s], da_slot)
    ex.terms_relay(down_grads, lambda q: B.down_src[q], B.down_joined)
    ex.terms_relay(up_grads, lambda q: B.up_src[:, q], B.up_joined)
    ffo_over = ex.sum_chips(ffo_pairs, B.ffo_src, B.ffo_pair, B.ffo_paired, B.ffo_chips, B.ffo_total)
    sum_gain_b = column_sum(dr * B.normal_b[...])
    sum_shift_b = column_sum(dr)
    sum_g = column_sum(g_local)
    sum_da = column_sum(da.astype(F32))
    B.dk[...] = jnp.zeros((1024, 128), F32)
    B.dv[...] = jnp.zeros((1024, 128), F32)
    ex.arrived(do_copies)
    own_do.wait()

    scale_sums = jnp.zeros((1, 128), F32)
    for size in (512, 1024):
        for h in range(2):

            def back(t, sums, size=size, h=h):
                at = pl.ds(t * 128, 128)
                do = of_head(B.do_all[t], h)
                along = do.astype(F32) * B.attended[at, :]
                delta = jnp.sum(along, axis=-1, keepdims=True)
                kept = B.probs_low if size == 512 else B.probs_high
                probs = kept[h, pl.ds(t * 128 - size + 512, 128), :]
                dp = times_transposed(do, B.qkv[0:size, 256:384])
                ds = (probs * (dp - delta)).astype(BF)
                found = matmul(ds, of_head(B.qkv[0:size, 128:256], h))
                if h == 0:
                    B.dq[at, :] = found
                else:
                    B.dq[at, :] += found
                B.dk[0:size, :] += contract_rows(ds, of_head(B.qkv[at, 0:128], h))
                B.dv[0:size, :] += contract_rows(probs.astype(BF), do)
                return sums + column_sum(along)

            scale_sums = lax.fori_loop(size // 128 - 4, size // 128, back, scale_sums)

    def join(t, sums):
        at = pl.ds(t * 128, 128)
        dq = (B.dq[at, :] * score_scale).astype(BF)
        dk = (B.dk[at, :] * score_scale).astype(BF)
        dv = B.dv[at, :].astype(BF)
        B.dqkv[at, 0:128] = dq
        B.dqkv[at, 128:256] = dk
        B.dqkv[at, 256:384] = dv
        B.dh1_src[t] = times_transposed(B.dqkv[at, :], B.qkv_w[...].reshape(1024, 384)).astype(BF)
        return (sums[0] + column_sum(dq.astype(F32)), sums[1] + column_sum(dv.astype(F32)))

    blank = jnp.zeros((1, 128), F32)
    sum_dq, sum_dv = lax.fori_loop(0, 8, join, (blank, blank))
    dh1_pairs = ex.sum_pair(B.dh1_src, B.dh1_pair)

    @pl.loop(0, 8)
    def _(c):
        terms = contract_rows(B.h1[:, columns(c * 128, 128)], B.dqkv[...])
        B.qkv_src[c] = terms.astype(BF).reshape(4, 32, 384)

    qkv_grads = ex.terms_start(lambda q: B.qkv_src.at[:, q], B.qkv_terms, B.qkv_passing)
    dh1_over = ex.sum_chips(dh1_pairs, B.dh1_src, B.dh1_pair, B.dh1_paired, B.dh1_chips, B.total)
    ex.terms_relay(qkv_grads, lambda q: B.qkv_src[:, q], B.qkv_joined)
    da_passed = ex.gather_forward(da_copies, da_slot)
    ffo = ex.sum_end(ffo_over, B.ffo_chips, B.ffo_total)
    output[...] = jnp.where(held, B.residual[...] + ffo + bias_out, 0.0).astype(BF)
    ex.arrived(da_passed)
    terms = contract_rows(B.scaled[...].reshape(1024, 128), B.da_all[...].reshape(1024, 1024))
    B.out_src[...] = terms.astype(BF).reshape(4, 32, 1024)
    out_grads = [ex.send(B.out_src.at[q], B.out_terms.at[b], s, q) for q in ex.line()]

    def line_sum(mine, landed):
        total = mine
        for k in (1, 2, 3):
            total = total + landed[(b + k) % 4].astype(F32)
        return total

    ex.terms_arrived(down_grads)
    grad_down[...] = line_sum(B.down_src[b].astype(F32), B.down_terms)
    ex.terms_arrived(up_grads)
    B.up_own[...] = line_sum(B.up_src[:, b].astype(F32), B.up_terms).astype(BF)
    up_lanes = B.up_fin.at[:, columns(s * 512, 512)]
    up_copies = [ex.send(B.up_own.at[p], up_lanes, p, b) for p in ex.plane()]
    own_up = ex.local(B.up_own.at[s], up_lanes)

    dh1 = ex.sum_end(dh1_over, B.dh1_chips, B.total)
    normal_a, inverse_a = centred(x_in[...].astype(F32))
    grad_input[...] = (B.dr[...] + norm_back(dh1, gain_a, normal_a, inverse_a)).astype(BF)
    wide = jnp.concatenate(
        [
            column_sum(dh1 * normal_a),
            sum_gain_b,
            sum_gain_c,
            column_sum(dh1),
            sum_shift_b,
            sum_shift_c,
            jnp.zeros((1, 1024), F32),
            sum_g,
            jnp.zeros((1, 1024), F32),
            sum_da,
            jnp.zeros((6, 1024), F32),
        ],
        axis=0,
    )
    by_head = jnp.zeros((1, 128), F32)
    for h in range(2):
        found = jnp.sum(of_head(scale_sums / own_scale, h), axis=-1, keepdims=True)
        by_head = jnp.where(lane == s * 2 + h, found, by_head)
    place = lax.broadcasted_iota(jnp.int32, (16, 128), 0)
    for p in range(8):
        mine = jnp.where(s == p, 1.0, 0.0)
        tile = wide[:, p * 128 : (p + 1) * 128]
        tile = jnp.where(place == 6, sum_dq * mine, tile)
        tile = jnp.where(place == 8, sum_dv * mine, tile)
        B.close_src[p] = jnp.where(place == 10, by_head, tile)
    for q in range(4):
        part = [one[:, q * 128 : (q + 1) * 128] for one in ff_sums]
        B.ff_src[q] = jnp.concatenate(part + [jnp.zeros((5, 128), F32)], axis=0)
    close = [ex.send(B.close_src.at[p], B.close_all.at[me], p, q) for p, q in partners]
    close_ff = [ex.send(B.ff_src.at[q], B.ff_all.at[b], s, q) for q in ex.line()]
    own_close = [ex.local(B.close_src.at[s], B.close_all.at[me]), ex.local(B.ff_src.at[b], B.ff_all.at[b])]

    ex.terms_arrived(qkv_grads)
    B.qkv_own[...] = line_sum(B.qkv_src[:, b].astype(F32), B.qkv_terms).astype(BF)
    qkv_lanes = lambda t: B.qkv_fin.at[:, columns(t * 1024 + s * 128, 128)]
    qkv_piece = lambda p, t: B.qkv_own.at[p, :, pl.ds(t * 128, 128)]
    qkv_copies = [ex.send(qkv_piece(p, t), qkv_lanes(t), p, b) for p in ex.plane() for t in range(3)]
    own_qkv = [ex.local(qkv_piece(s, t), qkv_lanes(t)) for t in range(3)]
    ex.arrived(out_grads)
    grad_out[...] = line_sum(B.out_src[b].astype(F32), B.out_terms)
    ex.arrived(up_copies)
    own_up.wait()
    grad_up[...] = B.up_fin[...].astype(F32)
    ex.arrived(close)
    ex.arrived(close_ff)
    for one in own_close:
        one.wait()
    total = B.close_all[0]
    for i in range(1, 32):
        total = total + B.close_all[i]
    vec_out[...] = total
    ff_out[...] = B.ff_all[0] + B.ff_all[1] + B.ff_all[2] + B.ff_all[3]
    ex.arrived(qkv_copies)
    for one in own_qkv:
        one.wait()
    grad_qkv[...] = B.qkv_fin[...].astype(F32)
    ex.finish()


def plane_shards(
    inputs,
    lengths,
    w_qkv,
    w_out,
    w_up,
    w_down,
    norm_gains,
    model_biases,
    attn_biases,
    ff_gain,
    ff_biases,
    head_scale,
    cotangent,
):
    b = lax.axis_index("batch")
    near = pl.BlockSpec(memory_space=pltpu.VMEM)
    outs = [
        ((128, 1024), BF),
        ((128, 1024), BF),
        ((32, 3072), F32),
        ((32, 1024), F32),
        ((32, 4096), F32),
        ((128, 1024), F32),
        ((16, 128), F32),
        ((8, 128), F32),
    ]
    found = pl.pallas_call(
        block_kernel,
        name="block",
        out_shape=[jax.ShapeDtypeStruct(shape, dtype) for shape, dtype in outs],
        in_specs=[pl.BlockSpec(memory_space=pltpu.SMEM)] + [near] * (INPUTS - 1),
        out_specs=[near] * OUTPUTS,
        scratch_shapes=[pltpu.VMEM(shape, dtype) for shape, dtype in BUFFERS.values()]
        + [
            pltpu.SemaphoreType.DMA((COPIES,)),
            pltpu.SemaphoreType.DMA((COPIES,)),
            pltpu.SemaphoreType.DMA((32,)),
        ],
        compiler_params=pltpu.CompilerParams(
            collective_id=1, has_side_effects=True, vmem_limit_bytes=67043328
        ),
    )(
        lengths.reshape(1, 1),
        inputs[0],
        cotangent[0],
        w_qkv,
        w_out,
        w_up,
        w_down,
        norm_gains,
        model_biases,
        attn_biases,
        ff_gain.reshape(1, 128),
        ff_biases,
        head_scale.reshape(1, H),
    )
    output, grad_input, grad_qkv, grad_out, grad_up, grad_down, narrow, wide = found
    narrow_own = lax.dynamic_slice_in_dim(narrow, b * 32, 32, 1)
    return (
        output[None],
        grad_input[None],
        grad_qkv,
        grad_out,
        grad_up,
        grad_down,
        narrow_own[0:3],
        narrow_own[3:8],
        narrow_own[8:10],
        wide[0],
        wide[1:3],
        narrow[10, :H],
    )


def solution(mesh):
    in_plane = mesh.shape["seq"] == 8 and mesh.shape["batch"] == 4
    return jax.shard_map(
        plane_shards if in_plane else shards,
        mesh=mesh,
        in_specs=(
            P("batch", "seq", None),
            P("batch"),
            P(("seq", "batch"), None),
            P(("seq", "batch"), None),
            P(("seq", "batch"), None),
            P(("seq", "batch"), None),
            P(None, ("seq", "batch")),
            P(None, ("seq", "batch")),
            P(None, ("seq", "batch")),
            P(("seq", "batch")),
            P(None, ("seq", "batch")),
            P(),
            P("batch", "seq", None),
        ),
        out_specs=(
            P("batch", "seq", None),
            P("batch", "seq", None),
            P(("seq", "batch"), None),
            P(("seq", "batch"), None),
            P(("seq", "batch"), None),
            P(("seq", "batch"), None),
            P(None, ("seq", "batch")),
            P(None, ("seq", "batch")),
            P(None, ("seq", "batch")),
            P(("seq", "batch")),
            P(None, ("seq", "batch")),
            P(),
        ),
        check_vma=False,
    )
```

```python
import jax
import jax.numpy as jnp
from jax import lax
from jax.experimental import pallas as pl
from jax.experimental.pallas import tpu as pltpu
from jax.sharding import PartitionSpec as P

H = 16
HD = 64


NORM_EPSILON = 1e-05


def layer_norm(vector, norm_gain, norm_bias):
    centered = vector - jnp.mean(vector, axis=-1, keepdims=True)
    spread = jnp.mean(centered * centered, axis=-1, keepdims=True)
    return centered * lax.rsqrt(spread + NORM_EPSILON) * norm_gain + norm_bias


def gelu_norm(hidden, norm_gain, norm_bias):
    return layer_norm(jax.nn.gelu(hidden, approximate=False), norm_gain, norm_bias)


def contract_rows(left, right):
    return lax.dot_general(
        left, right, (((0,), (0,)), ((), ())), preferred_element_type=jnp.float32
    )


def times_transposed(left, right):
    return lax.dot_general(
        left, right, (((1,), (1,)), ((), ())), preferred_element_type=jnp.float32
    )


def shards(
    inputs,
    lengths,
    w_qkv,
    w_out,
    w_up,
    w_down,
    norm_gains,
    model_biases,
    attn_biases,
    ff_gain,
    ff_biases,
    head_scale,
    cotangent,
):
    gathered = (
        lax.all_gather(w_qkv, ("seq", "batch"), axis=0, tiled=True),
        lax.all_gather(w_out, ("seq", "batch"), axis=0, tiled=True),
        lax.all_gather(w_up, ("seq", "batch"), axis=0, tiled=True),
        lax.all_gather(w_down, ("seq", "batch"), axis=0, tiled=True),
        lax.all_gather(norm_gains, ("seq", "batch"), axis=1, tiled=True),
        lax.all_gather(model_biases, ("seq", "batch"), axis=1, tiled=True),
        lax.all_gather(attn_biases, ("seq", "batch"), axis=1, tiled=True),
        lax.all_gather(ff_gain, ("seq", "batch"), axis=0, tiled=True),
        lax.all_gather(ff_biases, ("seq", "batch"), axis=1, tiled=True),
    )
    qkv_full, out_full, up_full, down_full = (gathered[0], gathered[1], gathered[2], gathered[3])
    gain_rows = gathered[4].astype(jnp.float32)
    bias_rows = gathered[5].astype(jnp.float32)
    attn_rows = gathered[6].astype(jnp.float32)
    ffn_gain = gathered[7].astype(jnp.float32)
    ffn_rows = gathered[8].astype(jnp.float32)
    scales = head_scale.astype(jnp.float32)
    local_rows = inputs.shape[1]
    model_width = inputs.shape[2]
    seq_length = local_rows * lax.axis_size("seq")
    tile_rows = min(512, seq_length)
    first_row = lax.axis_index("seq") * local_rows
    valid_rows = lengths[0]
    positions = first_row + jnp.arange(local_rows, dtype=jnp.int32)
    valid_mask = (positions < valid_rows)[:, None]
    score_scale = HD ** (-0.5)
    residual_in = inputs[0].astype(jnp.float32)
    normed, norm_a_pull = jax.vjp(layer_norm, residual_in, gain_rows[0], bias_rows[0])
    normed_low = normed.astype(jnp.bfloat16)
    offsets = jnp.concatenate([bias_rows[3], jnp.zeros_like(bias_rows[3]), attn_rows[0]])
    projected = (
        jnp.dot(normed_low, qkv_full, preferred_element_type=jnp.float32) + offsets
    ).astype(jnp.bfloat16)
    queries = projected[:, :model_width]
    key_local = projected[:, model_width : 2 * model_width]
    value_local = projected[:, 2 * model_width :]
    key_rows, value_rows = (
        lax.all_gather(key_local, "seq", axis=0, tiled=True),
        lax.all_gather(value_local, "seq", axis=0, tiled=True),
    )
    query_heads = queries.reshape(local_rows, H, HD)
    last_needed = jnp.minimum(first_row + local_rows - 1, valid_rows - 1)
    tile_count = last_needed // tile_rows + 1

    def tile_scores(j):
        start = j * tile_rows
        key_tile = lax.dynamic_slice_in_dim(key_rows, start, tile_rows, 0).reshape(tile_rows, H, HD)
        scores = (
            jnp.einsum("qhd,khd->hqk", query_heads, key_tile, preferred_element_type=jnp.float32)
            * score_scale
        )
        key_index = start + jnp.arange(tile_rows, dtype=jnp.int32)
        allowed = (key_index[None, :] <= positions[:, None]) & (key_index[None, :] < valid_rows)
        return (scores, allowed[None], key_tile)

    def max_and_sum(j, carry):
        running_max, running_sum = carry
        scores, allowed, unused_tile = tile_scores(j)
        masked = jnp.where(allowed, scores, -1e30)
        new_max = jnp.maximum(running_max, jnp.max(masked, axis=-1))
        kept_terms = jnp.where(allowed, jnp.exp(masked - new_max[..., None]), 0.0)
        return (
            new_max,
            running_sum * jnp.exp(running_max - new_max) + jnp.sum(kept_terms, axis=-1),
        )

    start_stats = (
        jnp.full((H, local_rows), -1e30, jnp.float32),
        jnp.zeros((H, local_rows), jnp.float32),
    )
    running_max, running_sum = lax.fori_loop(0, tile_count, max_and_sum, start_stats)
    log_total = running_max + jnp.log(running_sum)

    def tile_probs(j):
        scores, allowed, key_tile = tile_scores(j)
        attn_probs = jnp.where(allowed, jnp.exp(scores - log_total[..., None]), 0.0)
        value_tile = lax.dynamic_slice_in_dim(value_rows, j * tile_rows, tile_rows, 0).reshape(
            tile_rows, H, HD
        )
        return (attn_probs, key_tile, value_tile)

    def accumulate(j, summed):
        attn_probs, unused_tile, value_tile = tile_probs(j)
        return summed + jnp.einsum(
            "hqk,khd->qhd",
            attn_probs.astype(jnp.bfloat16),
            value_tile,
            preferred_element_type=jnp.float32,
        )

    attended = lax.fori_loop(0, tile_count, accumulate, jnp.zeros((local_rows, H, HD), jnp.float32))
    scaled_low = (
        (attended * scales[None, :, None]).reshape(local_rows, model_width).astype(jnp.bfloat16)
    )
    attn_proj = jnp.dot(scaled_low, out_full, preferred_element_type=jnp.float32) + attn_rows[1]
    attn_normed, norm_b_pull = jax.vjp(layer_norm, attn_proj, gain_rows[1], bias_rows[1])
    residual = residual_in + attn_normed
    ffn_in, norm_c_pull = jax.vjp(layer_norm, residual, gain_rows[2], bias_rows[2])
    ffn_low = ffn_in.astype(jnp.bfloat16)
    hidden = jnp.dot(ffn_low, up_full, preferred_element_type=jnp.float32) + ffn_rows[0]
    ffn_normed, ffn_pull = jax.vjp(gelu_norm, hidden, ffn_gain, ffn_rows[1])
    ffn_out_low = ffn_normed.astype(jnp.bfloat16)
    combined = jnp.where(
        valid_mask,
        residual
        + jnp.dot(ffn_out_low, down_full, preferred_element_type=jnp.float32)
        + bias_rows[4],
        0.0,
    )
    output = combined.astype(jnp.bfloat16)[None]
    barrier_out = lax.optimization_barrier(((w_qkv, w_out, w_up, w_down), combined))
    regathered = (
        lax.all_gather(barrier_out[0][0], ("seq", "batch"), axis=0, tiled=True),
        lax.all_gather(barrier_out[0][1], ("seq", "batch"), axis=0, tiled=True),
        lax.all_gather(barrier_out[0][2], ("seq", "batch"), axis=0, tiled=True),
        lax.all_gather(barrier_out[0][3], ("seq", "batch"), axis=0, tiled=True),
    )
    qkv_full, out_full, up_full, down_full = (
        regathered[0],
        regathered[1],
        regathered[2],
        regathered[3],
    )
    cotan_rows = jnp.where(valid_mask, cotangent[0], jnp.zeros_like(cotangent[0]))
    cotan_float = cotan_rows.astype(jnp.float32)
    grad_down = contract_rows(ffn_out_low, cotan_rows)
    grad_bias_out = jnp.sum(cotan_float, axis=0)
    grad_ffn_normed = times_transposed(cotan_rows, down_full)
    grad_hidden, grad_ffn_gain, grad_ffn_shift = ffn_pull(grad_ffn_normed)
    grad_hidden_low = grad_hidden.astype(jnp.bfloat16)
    grad_up = contract_rows(ffn_low, grad_hidden_low)
    grad_ffn_bias = jnp.sum(grad_hidden_low.astype(jnp.float32), axis=0)
    grad_ffn_in = times_transposed(grad_hidden_low, up_full)
    grad_from_ffn, grad_gain_c, grad_shift_c = norm_c_pull(grad_ffn_in)
    grad_residual = cotan_float + grad_from_ffn
    grad_proj, grad_gain_b, grad_shift_b = norm_b_pull(grad_residual)
    grad_proj_low = grad_proj.astype(jnp.bfloat16)
    grad_out_bias = jnp.sum(grad_proj_low.astype(jnp.float32), axis=0)
    grad_out = contract_rows(scaled_low, grad_proj_low)
    grad_scaled = times_transposed(grad_proj_low, out_full).reshape(local_rows, H, HD)
    grad_scales = jnp.sum(grad_scaled * attended, axis=(0, 2))
    grad_heads_low = (grad_scaled * scales[None, :, None]).astype(jnp.bfloat16)
    row_delta = jnp.einsum("qhd,qhd->hq", grad_heads_low.astype(jnp.float32), attended)

    def score_grads(j):
        attn_probs, key_tile, value_tile = tile_probs(j)
        grad_probs = jnp.einsum(
            "qhd,khd->hqk", grad_heads_low, value_tile, preferred_element_type=jnp.float32
        )
        grad_scores = (attn_probs * (grad_probs - row_delta[..., None])).astype(jnp.bfloat16)
        return (attn_probs, grad_scores, key_tile)

    def backward_tile(j, carry):
        grad_query, terms = carry
        attn_probs, grad_scores, key_tile = score_grads(j)
        grad_query = grad_query + jnp.einsum(
            "hqk,khd->qhd", grad_scores, key_tile, preferred_element_type=jnp.float32
        )
        grad_key = (
            jnp.einsum("hqk,qhd->khd", grad_scores, query_heads, preferred_element_type=jnp.float32)
            * score_scale
        )
        grad_value = jnp.einsum(
            "hqk,qhd->khd",
            attn_probs.astype(jnp.bfloat16),
            grad_heads_low,
            preferred_element_type=jnp.float32,
        )
        piece = jnp.concatenate(
            [grad_key.reshape(tile_rows, model_width), grad_value.reshape(tile_rows, model_width)],
            axis=1,
        )
        return (grad_query, lax.dynamic_update_slice_in_dim(terms, piece, j * tile_rows, 0))

    start_carry = (
        jnp.zeros((local_rows, H, HD), jnp.float32),
        jnp.zeros((seq_length, 2 * model_width), jnp.float32),
    )
    grad_query, terms = lax.fori_loop(0, tile_count, backward_tile, start_carry)
    grad_kv = lax.psum_scatter(terms, "seq", scatter_dimension=0, tiled=True)
    grad_query_low = (
        (grad_query * score_scale).reshape(local_rows, model_width).astype(jnp.bfloat16)
    )
    grad_kv_low = grad_kv.astype(jnp.bfloat16)
    grad_projected = jnp.concatenate([grad_query_low, grad_kv_low], axis=1)
    grad_qkv = contract_rows(normed_low, grad_projected)
    grad_query_bias = jnp.sum(grad_query_low.astype(jnp.float32), axis=0)
    grad_value_bias = jnp.sum(grad_kv_low[:, model_width:].astype(jnp.float32), axis=0)
    grad_normed = times_transposed(grad_projected, qkv_full)
    grad_from_attn, grad_gain_a, grad_shift_a = norm_a_pull(grad_normed)
    grad_input = (grad_residual + grad_from_attn).astype(jnp.bfloat16)[None]
    reduced = (
        lax.psum_scatter(grad_qkv, ("seq", "batch"), scatter_dimension=0, tiled=True),
        lax.psum_scatter(grad_out, ("seq", "batch"), scatter_dimension=0, tiled=True),
        lax.psum_scatter(grad_up, ("seq", "batch"), scatter_dimension=0, tiled=True),
        lax.psum_scatter(grad_down, ("seq", "batch"), scatter_dimension=0, tiled=True),
        lax.psum_scatter(
            jnp.stack([grad_gain_a, grad_gain_b, grad_gain_c]),
            ("seq", "batch"),
            scatter_dimension=1,
            tiled=True,
        ),
        lax.psum_scatter(
            jnp.stack([grad_shift_a, grad_shift_b, grad_shift_c, grad_query_bias, grad_bias_out]),
            ("seq", "batch"),
            scatter_dimension=1,
            tiled=True,
        ),
        lax.psum_scatter(
            jnp.stack([grad_value_bias, grad_out_bias]),
            ("seq", "batch"),
            scatter_dimension=1,
            tiled=True,
        ),
        lax.psum_scatter(grad_ffn_gain, ("seq", "batch"), scatter_dimension=0, tiled=True),
        lax.psum_scatter(
            jnp.stack([grad_ffn_bias, grad_ffn_shift]),
            ("seq", "batch"),
            scatter_dimension=1,
            tiled=True,
        ),
    )
    scale_total = lax.psum(grad_scales, ("seq", "batch"))
    return (
        output,
        grad_input,
        reduced[0],
        reduced[1],
        reduced[2],
        reduced[3],
        reduced[4],
        reduced[5],
        reduced[6],
        reduced[7],
        reduced[8],
        scale_total,
    )


BF = jnp.bfloat16
F32 = jnp.float32


class Exchange:
    def __init__(self, send_sems, recv_sems, local_sems):
        self.send_sems = send_sems
        self.recv_sems = recv_sems
        self.local_sems = local_sems
        self.count = 0
        self.locals = 0
        self.sent = []
        self.sent_if = []
        self.s = lax.axis_index("seq")
        self.b = lax.axis_index("batch")
        self.chip = self.s // 2
        self.core = self.s % 2
        self.sibling = self.chip * 2 + 1 - self.core

    def send(self, src, dst, seq, batch):
        at = self.count
        self.count += 1
        copy = pltpu.make_async_remote_copy(
            src_ref=src,
            dst_ref=dst,
            send_sem=self.send_sems.at[at],
            recv_sem=self.recv_sems.at[at],
            device_id=(seq, batch),
            device_id_type=pl.DeviceIdType.MESH,
        )
        copy.start()
        self.sent.append(copy)
        return copy

    def describe(self, src, dst, seq, batch, sent_at, recv_at):
        return pltpu.make_async_remote_copy(
            src_ref=src,
            dst_ref=dst,
            send_sem=self.send_sems.at[sent_at],
            recv_sem=self.recv_sems.at[recv_at],
            device_id=(seq, batch),
            device_id_type=pl.DeviceIdType.MESH,
        )

    def send_if(self, held, copy):
        @pl.when(held)
        def _():
            copy.start()

        self.sent_if.append((held, copy))

    def line_start(self, src, slot):
        first = self.count
        self.count += 4
        b = self.b
        copies = [
            self.describe(src, slot(b), self.s, (b + k) % 4, first + k - 1, first + k - 1) for k in (1, 2, 3)
        ]
        copies[1].start()
        self.sent.append(copies[1])
        return copies, slot, first

    def line_near(self, line):
        copies = line[0]
        self.send_if(self.b != 3, copies[0])
        self.send_if(self.b != 0, copies[2])

    def line_relay(self, line):
        copies, slot, first = line
        b = self.b

        @pl.when((b == 1) | (b == 2))
        def _():
            copies[1].wait_recv()

        came = slot((b + 2) % 4)
        self.send_if(b == 1, self.describe(came, came, self.s, 0, first + 3, first))
        self.send_if(b == 2, self.describe(came, came, self.s, 3, first + 3, first + 2))

    def line_arrived(self, line):
        copies, _slot, _first = line
        copies[0].wait_recv()
        copies[2].wait_recv()

        @pl.when((self.b == 0) | (self.b == 3))
        def _():
            copies[1].wait_recv()

    def terms_start(self, view, landed, passing):
        first = self.count
        self.count += 4
        b = self.b
        at = lambda q, k: self.describe(view(q), landed.at[b], self.s, q, first + k - 1, first + k - 1)
        up, over, down = at((b + 1) % 4, 1), at((b + 2) % 4, 2), at((b + 3) % 4, 3)
        to_one = self.describe(view(3), passing, self.s, 1, first + 3, first + 3)
        to_two = self.describe(view(0), passing, self.s, 2, first + 3, first + 3)
        self.send_if(b == 0, to_one)
        self.send_if(b == 3, to_two)
        self.send_if((b == 0) | (b == 3), over)
        self.send_if(b != 3, up)
        self.send_if(b != 0, down)
        return up, over, down, to_one, landed, passing, first

    def terms_relay(self, terms, mine, joined):
        up, over, down, to_one, landed, passing, first = terms
        b = self.b
        held = (b == 1) | (b == 2)

        @pl.when(held)
        def _():
            to_one.wait_recv()
            joined[...] = (mine((b + 2) % 4).astype(F32) + passing[...].astype(F32)).astype(BF)

        self.send_if(
            held, self.describe(joined, landed.at[b], self.s, (b + 2) % 4, first + 1, first + 1)
        )

    def terms_arrived(self, terms):
        up, over, down = terms[:3]
        over.wait_recv()

        @pl.when(self.b != 0)
        def _():
            up.wait_recv()

        @pl.when(self.b != 3)
        def _():
            down.wait_recv()

    def local(self, src, dst):
        at = self.locals
        self.locals += 1
        copy = pltpu.make_async_copy(src, dst, self.local_sems.at[at])
        copy.start()
        return copy

    def arrived(self, copies):
        for copy in copies:
            copy.wait_recv()

    def finish(self):
        for copy in self.sent:
            copy.wait_send()
        for held, copy in self.sent_if:
            pl.when(held)(copy.wait_send)

    def peer(self, k):
        return ((self.chip + k) % 4) * 2 + self.core

    def source(self, k):
        return ((self.chip + 4 - k) % 4) * 2 + self.core

    def chip_source(self, k):
        return (self.chip + 4 - k) % 4

    def tile(self, j):
        return (self.chip + j + 1) % 4 * 2 + jnp.where(j < 4, 1 - self.core, self.core)

    def plane(self):
        return [(self.s + j) % 8 for j in range(1, 8)]

    def line(self):
        return [(self.b + k) % 4 for k in range(1, 4)]

    def gather_start(self, src, slot):
        copies = [self.send(src, slot(self.s), self.peer(k), self.b) for k in (1, 2, 3)]
        copies.append(self.send(src, slot(self.s), self.sibling, self.b))
        return copies

    def gather_forward(self, copies, slot):
        passed = []
        for k in (1, 2, 3):
            copies[k - 1].wait_recv()
            came = slot(self.source(k))
            passed.append(self.send(came, came, self.sibling, self.b))
        return [copies[3]] + passed

    def sum_pair(self, src, from_pair):
        return [
            self.send(src.at[((self.chip + k) % 4) * 2 + 1 - self.core], from_pair.at[k], self.sibling, self.b)
            for k in (1, 2, 3, 0)
        ]

    def sum_chips(self, copies, src, from_pair, paired, from_chips, total):
        over = []
        for at, k in enumerate((1, 2, 3, 0)):
            copies[at].wait_recv()
            mine = src[((self.chip + k) % 4) * 2 + self.core].astype(F32)
            both = mine + from_pair[k].astype(F32)
            if k:
                paired[k - 1] = both.astype(BF)
                over.append(self.send(paired.at[k - 1], from_chips.at[k - 1], self.peer(k), self.b))
            else:
                total[...] = both
        return over

    def sum_end(self, over, from_chips, total):
        self.arrived(over)
        return total[...] + from_chips[0].astype(F32) + from_chips[1].astype(F32) + from_chips[2].astype(F32)


def columns(start, size):
    return pl.ds(pl.multiple_of(start, 128), size)


def centred(rows):
    middle = rows - jnp.mean(rows, axis=-1, keepdims=True)
    inverse = lax.rsqrt(jnp.mean(middle * middle, axis=-1, keepdims=True) + NORM_EPSILON)
    return middle * inverse, inverse


def norm_back(upstream, gain, normal, inverse):
    scaled = upstream * gain
    average = jnp.mean(scaled, axis=-1, keepdims=True)
    along = jnp.mean(scaled * normal, axis=-1, keepdims=True)
    return inverse * (scaled - average - normal * along)


def gelu_parts(z):
    phi = 0.5 * (1.0 + lax.erf(z * 0.7071067811865476))
    density = 0.3989422804014327 * jnp.exp(-0.5 * z * z)
    return z * phi, phi + z * density


def matmul(left, right):
    return jnp.dot(left, right, preferred_element_type=F32)


def column_sum(rows):
    return jnp.sum(rows, axis=0, keepdims=True)


def pack_columns(parts):
    lane = lax.broadcasted_iota(jnp.int32, (128, 128), 1)
    wide = jnp.zeros((128, 128), F32)
    for at, part in enumerate(parts):
        wide = jnp.where(lane == at, part, wide)
    return wide.T[:8]


BUFFERS = dict(
    x_all=((8, 128, 1024), BF),
    g_all=((8, 128, 1024), BF),
    qkv_w=((8, 4, 32, 384), BF),
    out_w=((8, 4, 32, 1024), BF),
    up_w=((8, 4, 32, 512), BF),
    down_w=((4, 128, 1024), BF),
    vec_src=((16, 128), F32),
    vec_all=((32, 16, 128), F32),
    scale_row=((8, 1024), F32),
    rows=((16, 1024), F32),
    ff_rows=((8, 512), F32),
    h1=((1024, 1024), BF),
    qkv=((1024, 384), BF),
    probs_low=((2, 512, 512), F32),
    probs_high=((2, 512, 1024), F32),
    attended=((1024, 128), F32),
    scaled=((8, 128, 128), BF),
    scaled_local=((128, 1024), BF),
    normal_b=((128, 1024), F32),
    normal_c=((128, 1024), F32),
    residual=((128, 1024), F32),
    h2_all=((8, 128, 1024), BF),
    active=((1024, 512), F32),
    slope=((1024, 512), F32),
    du2=((1024, 512), F32),
    stats=((8, 8, 128), F32),
    stats_all=((8, 8, 8, 128), F32),
    u2=((1024, 512), BF),
    dz=((1024, 512), BF),
    dh2_pair=((4, 128, 1024), BF),
    dh2_paired=((3, 128, 1024), BF),
    dh2_chips=((3, 128, 1024), BF),
    ffo_src=((8, 128, 1024), BF),
    ffo_pair=((4, 128, 1024), BF),
    ffo_paired=((3, 128, 1024), BF),
    ffo_chips=((3, 128, 1024), BF),
    dh1_src=((8, 128, 1024), BF),
    dh1_pair=((4, 128, 1024), BF),
    dh1_paired=((3, 128, 1024), BF),
    dh1_chips=((3, 128, 1024), BF),
    total=((128, 1024), F32),
    ffo_total=((128, 1024), F32),
    dr=((128, 1024), F32),
    da_all=((8, 128, 1024), BF),
    do_local=((128, 1024), BF),
    do_all=((8, 128, 128), BF),
    dq=((1024, 128), F32),
    dk=((1024, 128), F32),
    dv=((1024, 128), F32),
    dqkv=((1024, 384), BF),
    up_src=((8, 4, 32, 512), BF),
    up_terms=((4, 8, 32, 512), BF),
    down_src=((4, 128, 1024), BF),
    down_terms=((4, 128, 1024), BF),
    qkv_src=((8, 4, 32, 384), BF),
    qkv_terms=((4, 8, 32, 384), BF),
    up_passing=((8, 32, 512), BF),
    up_joined=((8, 32, 512), BF),
    down_passing=((128, 1024), BF),
    down_joined=((128, 1024), BF),
    qkv_passing=((8, 32, 384), BF),
    qkv_joined=((8, 32, 384), BF),
    out_src=((4, 32, 1024), BF),
    out_terms=((4, 32, 1024), BF),
    up_own=((8, 32, 512), BF),
    qkv_own=((8, 32, 384), BF),
    close_src=((8, 16, 128), F32),
    close_all=((32, 16, 128), F32),
    ff_src=((4, 8, 128), F32),
    ff_all=((4, 8, 128), F32),
)
COPIES = 240
INPUTS = 13
OUTPUTS = 8


def block_kernel(
    length_in,
    x_in,
    g_in,
    qkv_in,
    out_in,
    up_in,
    down_in,
    gains_in,
    biases_in,
    attn_in,
    ff_gain_in,
    ff_bias_in,
    scale_in,
    *refs,
):
    output, grad_input, qkv_fin, grad_out, up_fin, grad_down, vec_out, ff_out = refs[:OUTPUTS]
    B = type("Buffers", (), dict(zip(BUFFERS, refs[OUTPUTS : OUTPUTS + len(BUFFERS)])))
    ex = Exchange(*refs[OUTPUTS + len(BUFFERS) :])
    s, b = ex.s, ex.b
    me = s * 4 + b
    valid_rows = length_in[0, 0]

    lane = lax.broadcasted_iota(jnp.int32, (1, 128), 1)

    def spread(part):
        values = part[...].astype(F32)
        return jnp.where(lane // 32 == b, jnp.concatenate([values] * 4, axis=1), 0.0)

    B.vec_src[0:3, :] = spread(gains_in)
    B.vec_src[3:8, :] = spread(biases_in)
    B.vec_src[8:10, :] = spread(attn_in)
    B.vec_src[10:11, :] = ff_gain_in[...].astype(F32)
    B.vec_src[11:13, :] = ff_bias_in[...].astype(F32)
    B.vec_src[13:16, :] = jnp.zeros((3, 128), F32)
    held = s * 128 + lax.broadcasted_iota(jnp.int32, (128, 1), 0) < valid_rows
    B.g_all[s] = jnp.where(held, g_in[...].astype(F32), 0.0).astype(BF)
    by_head = lax.broadcasted_iota(jnp.int32, (8, 1024), 1) // HD
    head_scales = scale_in[...].astype(F32)
    scale_row = jnp.zeros((8, 1024), F32)
    for h in range(H):
        scale_row = jnp.where(by_head == h, head_scales[0:1, h : h + 1], scale_row)
    B.scale_row[...] = scale_row

    for landed in (B.up_terms, B.down_terms, B.qkv_terms):

        @pl.when(b == 3)
        def _():
            landed[0] = jnp.zeros(landed.shape[1:], BF)

        @pl.when(b == 0)
        def _():
            landed[3] = jnp.zeros(landed.shape[1:], BF)

    barrier = pltpu.get_barrier_semaphore()
    partners = [((s + j // 4) % 8, (b + j % 4) % 4) for j in range(1, 32)]
    for seq, batch in partners:
        pl.semaphore_signal(barrier, inc=1, device_id=(seq, batch), device_id_type=pl.DeviceIdType.MESH)
    pl.semaphore_wait(barrier, len(partners))

    qkv_part = lambda p, t: qkv_in.at[:, columns(t * 1024 + p * 128, 128)]
    qkv_slot = lambda t: B.qkv_w.at[s, b, :, pl.ds(t * 128, 128)]
    qkv_copies = [ex.send(qkv_part(p, t), qkv_slot(t), p, b) for p in ex.plane() for t in range(3)]
    out_line = ex.line_start(out_in, lambda i: B.out_w.at[s, i])
    ex.line_near(out_line)
    own = [ex.local(qkv_part(s, t), qkv_slot(t)) for t in range(3)]
    own_up = ex.local(up_in.at[:, columns(s * 512, 512)], B.up_w.at[s, b])
    own_rest = [
        ex.local(out_in, B.out_w.at[s, b]),
        ex.local(x_in, B.x_all.at[s]),
        ex.local(down_in, B.down_w.at[b]),
        ex.local(B.vec_src, B.vec_all.at[me]),
    ]
    x_slot = lambda i: B.x_all.at[i]
    g_slot = lambda i: B.g_all.at[i]
    x_copies = ex.gather_start(x_in, x_slot)
    vec_copies = [ex.send(B.vec_src, B.vec_all.at[me], p, q) for p, q in partners]
    up_copies = [ex.send(up_in.at[:, columns(p * 512, 512)], B.up_w.at[s, b], p, b) for p in ex.plane()]
    ex.arrived(qkv_copies)
    for one in own:
        one.wait()
    qkv_line = ex.line_start(B.qkv_w.at[:, b], lambda i: B.qkv_w.at[:, i])
    ex.line_near(qkv_line)
    ex.line_relay(out_line)
    x_passed = ex.gather_forward(x_copies, x_slot)
    ex.arrived(up_copies)
    own_up.wait()
    ex.line_relay(qkv_line)
    down_line = ex.line_start(down_in, lambda i: B.down_w.at[i])
    up_line = ex.line_start(B.up_w.at[:, b], lambda i: B.up_w.at[:, i])
    ex.line_near(down_line)
    ex.line_near(up_line)
    g_copies = ex.gather_start(B.g_all.at[s], g_slot)
    ex.arrived(vec_copies)
    for one in own_rest:
        one.wait()

    for p in range(8):
        group = B.vec_all[4 * p] + B.vec_all[4 * p + 1] + B.vec_all[4 * p + 2] + B.vec_all[4 * p + 3]
        B.rows[:, p * 128 : (p + 1) * 128] = group
    for q in range(4):
        B.ff_rows[:, q * 128 : (q + 1) * 128] = B.vec_all[s * 4 + q][8:16]
    row = lambda at: B.rows[at : at + 1, :]
    gain_a, gain_b, gain_c = row(0), row(1), row(2)
    bias_a, bias_b, bias_c, bias_out, bias_attn = row(3), row(4), row(5), row(7), row(9)
    ffn_gain, ffn_bias, ffn_shift = B.ff_rows[2:3, :], B.ff_rows[3:4, :], B.ff_rows[4:5, :]
    own_columns = columns(s * 128, 128)
    query_bias = B.rows[6:7, own_columns]
    value_bias = B.rows[8:9, own_columns]
    own_scale = B.scale_row[0:1, own_columns]

    ex.arrived(x_passed)

    @pl.loop(0, 8)
    def _(t):
        normal, _unused = centred(B.x_all[t].astype(F32))
        B.h1[pl.ds(t * 128, 128), :] = (normal * gain_a + bias_a).astype(BF)

    ex.line_arrived(qkv_line)
    offsets = jnp.concatenate([query_bias, jnp.zeros_like(query_bias), value_bias], axis=1)

    @pl.loop(0, 4)
    def _(t):
        at = pl.ds(t * 256, 256)
        B.qkv[at, :] = (matmul(B.h1[at, :], B.qkv_w[...].reshape(1024, 384)) + offsets).astype(BF)

    ex.line_arrived(out_line)
    out_slot = lambda i: B.out_w.at[i]
    out_copies = ex.gather_start(B.out_w.at[s], out_slot)
    g_passed = ex.gather_forward(g_copies, g_slot)

    score_scale = HD ** (-0.5)
    half_of = lax.broadcasted_iota(jnp.int32, (1, 128), 1) // HD

    def of_head(rows, h):
        return jnp.where(half_of == h, rows, jnp.zeros_like(rows))

    for size in (512, 1024):
        if size == 1024:
            ex.line_relay(down_line)
            ex.line_relay(up_line)
        for h in range(2):

            @pl.loop(size // 128 - 4, size // 128)
            def _(t):
                at = pl.ds(t * 128, 128)
                scores = times_transposed(of_head(B.qkv[at, 0:128], h), B.qkv[0:size, 128:256]) * score_scale
                key_index = lax.broadcasted_iota(jnp.int32, (128, size), 1)
                query_index = t * 128 + lax.broadcasted_iota(jnp.int32, (128, size), 0)
                allowed = (key_index <= query_index) & (key_index < valid_rows)
                masked = jnp.where(allowed, scores, -1e30)
                raised = jnp.exp(masked - jnp.max(masked, axis=-1, keepdims=True))
                probs = raised * (1.0 / jnp.sum(raised, axis=-1, keepdims=True))
                kept = B.probs_low if size == 512 else B.probs_high
                kept[h, pl.ds(t * 128 - size + 512, 128), :] = probs
                found = matmul(probs.astype(BF), of_head(B.qkv[0:size, 256:384], h))
                if h == 0:
                    B.attended[at, :] = found
                else:
                    both = B.attended[at, :] + found
                    B.attended[at, :] = both
                    B.scaled[t] = (both * own_scale).astype(BF)

    local_lanes = B.scaled_local.at[:, own_columns]
    heads = [ex.send(B.scaled.at[p], local_lanes, p, b) for p in ex.plane()]
    own_heads = ex.local(B.scaled.at[s], local_lanes)
    out_passed = ex.gather_forward(out_copies, out_slot)
    ex.arrived(out_passed)
    ex.arrived(heads)
    own_heads.wait()

    attn_proj = matmul(B.scaled_local[...], B.out_w[...].reshape(1024, 1024)) + bias_attn
    normal_b, inverse_b = centred(attn_proj)
    B.normal_b[...] = normal_b
    residual = x_in[...].astype(F32) + normal_b * gain_b + bias_b
    B.residual[...] = residual
    normal_c, inverse_c = centred(residual)
    B.normal_c[...] = normal_c
    B.h2_all[s] = (normal_c * gain_c + bias_c).astype(BF)
    h2_slot = lambda i: B.h2_all.at[i]
    h2_copies = ex.gather_start(B.h2_all.at[s], h2_slot)

    ex.arrived(g_passed)
    ex.line_arrived(down_line)
    ex.line_arrived(up_line)

    def upstream(t):
        B.du2[pl.ds(t * 128, 128), :] = times_transposed(B.g_all[t], B.down_w[...].reshape(512, 1024))

    def hidden_tile(t):
        at = pl.ds(t * 128, 128)
        active, slope = gelu_parts(matmul(B.h2_all[t], B.up_w[...].reshape(1024, 512)) + ffn_bias)
        B.active[at, :] = active
        B.slope[at, :] = slope
        dgain = B.du2[at, :] * ffn_gain
        mean = jnp.mean(active, axis=-1, keepdims=True)
        off = active - mean
        add = lambda rows: jnp.sum(rows, axis=-1, keepdims=True)
        B.stats[t] = pack_columns([mean, add(off * off), add(dgain), add(dgain * off)])

    pl.loop(0, 8)(upstream)
    hidden_tile(s)
    h2_copies[3].wait_recv()
    hidden_tile(ex.sibling)
    h2_passed = []
    for k in (1, 3, 2):
        h2_copies[k - 1].wait_recv()
        came = h2_slot(ex.source(k))
        h2_passed.append(ex.send(came, came, ex.sibling, b))
        hidden_tile(ex.source(k))
    for at, k in enumerate((1, 3, 2)):
        h2_passed[at].wait_recv()
        hidden_tile(ex.chip_source(k) * 2 + 1 - ex.core)

    stats_copies = [ex.send(B.stats, B.stats_all.at[s], p, b) for p in ex.plane()]
    own_stats = ex.local(B.stats, B.stats_all.at[s])
    ex.arrived(stats_copies)
    own_stats.wait()

    for copy in x_passed[1:]:
        copy.wait_send()
        ex.sent = [one for one in ex.sent if one is not copy]

    def finish_hidden(j, sums):
        t = ex.tile(j)
        at = pl.ds(t * 128, 128)
        means = [B.stats_all[i, t, 0:1, :] for i in range(8)]
        squares = [B.stats_all[i, t, 1:2, :] for i in range(8)]
        firsts = [B.stats_all[i, t, 2:3, :] for i in range(8)]
        seconds = [B.stats_all[i, t, 3:4, :] for i in range(8)]
        mean = sum(means) * 0.125
        shifts = [one - mean for one in means]
        spread = (sum(squares) + 512.0 * sum(one * one for one in shifts)) * (1.0 / 4096.0)
        inverse = lax.rsqrt(spread + NORM_EPSILON)
        average = sum(firsts) * (1.0 / 4096.0)
        along = inverse * sum(two + one * first for two, one, first in zip(seconds, shifts, firsts)) * (1.0 / 4096.0)
        packed = jnp.concatenate([mean, inverse, average, along, jnp.zeros((124, 128), F32)], axis=0).T
        mean, inverse, average, along = (packed[:, i : i + 1] for i in range(4))
        normal = (B.active[at, :] - mean) * inverse
        B.u2[at, :] = (normal * ffn_gain + ffn_shift).astype(BF)
        du2 = B.du2[at, :]
        dz = (inverse * (du2 * ffn_gain - average - normal * along) * B.slope[at, :]).astype(BF)
        B.dz[at, :] = dz
        B.x_all[t] = times_transposed(dz, B.up_w[...].reshape(1024, 512)).astype(BF)
        return (
            sums[0] + column_sum(du2 * normal),
            sums[1] + column_sum(dz.astype(F32)),
            sums[2] + column_sum(du2),
        )

    nothing = jnp.zeros((1, 512), F32)
    ff_sums = lax.fori_loop(0, 4, finish_hidden, (nothing, nothing, nothing))
    dh2_pairs = ex.sum_pair(B.x_all, B.dh2_pair)
    ff_sums = lax.fori_loop(4, 8, finish_hidden, ff_sums)
    dh2_over = ex.sum_chips(dh2_pairs, B.x_all, B.dh2_pair, B.dh2_paired, B.dh2_chips, B.total)

    @pl.loop(0, 4)
    def _(q):
        terms = contract_rows(B.u2[:, columns(q * 128, 128)], B.g_all[...].reshape(1024, 1024))
        B.down_src[q] = terms.astype(BF)

    down_grads = ex.terms_start(lambda q: B.down_src.at[q], B.down_terms, B.down_passing)

    @pl.loop(0, 8)
    def _(c):
        rows = B.h2_all[:, :, columns(c * 128, 128)].reshape(1024, 128)
        B.up_src[c] = contract_rows(rows, B.dz[...]).astype(BF).reshape(4, 32, 512)

    up_grads = ex.terms_start(lambda q: B.up_src.at[:, q], B.up_terms, B.up_passing)

    @pl.loop(0, 8)
    def _(t):
        B.ffo_src[t] = matmul(B.u2[pl.ds(t * 128, 128), :], B.down_w[...].reshape(512, 1024)).astype(BF)

    ffo_pairs = ex.sum_pair(B.ffo_src, B.ffo_pair)

    dh2 = ex.sum_end(dh2_over, B.dh2_chips, B.total)
    sum_gain_c = column_sum(dh2 * B.normal_c[...])
    sum_shift_c = column_sum(dh2)
    g_local = B.g_all[s].astype(F32)
    dr = g_local + norm_back(dh2, gain_c, B.normal_c[...], inverse_c)
    B.dr[...] = dr
    da = norm_back(dr, gain_b, B.normal_b[...], inverse_b).astype(BF)
    B.da_all[s] = da
    B.do_local[...] = (times_transposed(da, B.out_w[...].reshape(1024, 1024)) * B.scale_row[0:1, :]).astype(BF)
    do_copies = [ex.send(B.do_local.at[:, columns(p * 128, 128)], B.do_all.at[s], p, b) for p in ex.plane()]
    own_do = ex.local(B.do_local.at[:, own_columns], B.do_all.at[s])
    da_slot = lambda i: B.da_all.at[i]
    da_copies = ex.gather_start(B.da_all.at[s], da_slot)
    ex.terms_relay(down_grads, lambda q: B.down_src[q], B.down_joined)
    ex.terms_relay(up_grads, lambda q: B.up_src[:, q], B.up_joined)
    ffo_over = ex.sum_chips(ffo_pairs, B.ffo_src, B.ffo_pair, B.ffo_paired, B.ffo_chips, B.ffo_total)
    sum_gain_b = column_sum(dr * B.normal_b[...])
    sum_shift_b = column_sum(dr)
    sum_g = column_sum(g_local)
    sum_da = column_sum(da.astype(F32))
    B.dk[...] = jnp.zeros((1024, 128), F32)
    B.dv[...] = jnp.zeros((1024, 128), F32)
    ex.arrived(do_copies)
    own_do.wait()

    scale_sums = jnp.zeros((1, 128), F32)
    for size in (512, 1024):
        for h in range(2):

            def back(t, sums, size=size, h=h):
                at = pl.ds(t * 128, 128)
                do = of_head(B.do_all[t], h)
                along = do.astype(F32) * B.attended[at, :]
                delta = jnp.sum(along, axis=-1, keepdims=True)
                kept = B.probs_low if size == 512 else B.probs_high
                probs = kept[h, pl.ds(t * 128 - size + 512, 128), :]
                dp = times_transposed(do, B.qkv[0:size, 256:384])
                ds = (probs * (dp - delta)).astype(BF)
                found = matmul(ds, of_head(B.qkv[0:size, 128:256], h))
                if h == 0:
                    B.dq[at, :] = found
                else:
                    B.dq[at, :] += found
                B.dk[0:size, :] += contract_rows(ds, of_head(B.qkv[at, 0:128], h))
                B.dv[0:size, :] += contract_rows(probs.astype(BF), do)
                return sums + column_sum(along)

            scale_sums = lax.fori_loop(size // 128 - 4, size // 128, back, scale_sums)

    def join(t, sums):
        at = pl.ds(t * 128, 128)
        dq = (B.dq[at, :] * score_scale).astype(BF)
        dk = (B.dk[at, :] * score_scale).astype(BF)
        dv = B.dv[at, :].astype(BF)
        B.dqkv[at, 0:128] = dq
        B.dqkv[at, 128:256] = dk
        B.dqkv[at, 256:384] = dv
        return (sums[0] + column_sum(dq.astype(F32)), sums[1] + column_sum(dv.astype(F32)))

    def dh1_tile(j):
        t = ex.tile(j)
        rows = B.dqkv[pl.ds(t * 128, 128), :]
        B.dh1_src[t] = times_transposed(rows, B.qkv_w[...].reshape(1024, 384)).astype(BF)

    blank = jnp.zeros((1, 128), F32)
    sum_dq, sum_dv = lax.fori_loop(0, 8, join, (blank, blank))
    pl.loop(0, 4)(dh1_tile)
    dh1_pairs = ex.sum_pair(B.dh1_src, B.dh1_pair)

    @pl.loop(0, 8)
    def _(c):
        terms = contract_rows(B.h1[:, columns(c * 128, 128)], B.dqkv[...])
        B.qkv_src[c] = terms.astype(BF).reshape(4, 32, 384)

    qkv_grads = ex.terms_start(lambda q: B.qkv_src.at[:, q], B.qkv_terms, B.qkv_passing)
    pl.loop(4, 8)(dh1_tile)
    dh1_over = ex.sum_chips(dh1_pairs, B.dh1_src, B.dh1_pair, B.dh1_paired, B.dh1_chips, B.total)
    ex.terms_relay(qkv_grads, lambda q: B.qkv_src[:, q], B.qkv_joined)
    da_passed = ex.gather_forward(da_copies, da_slot)
    ffo = ex.sum_end(ffo_over, B.ffo_chips, B.ffo_total)
    output[...] = jnp.where(held, B.residual[...] + ffo + bias_out, 0.0).astype(BF)
    ex.arrived(da_passed)
    terms = contract_rows(B.scaled[...].reshape(1024, 128), B.da_all[...].reshape(1024, 1024))
    B.out_src[...] = terms.astype(BF).reshape(4, 32, 1024)
    out_grads = [ex.send(B.out_src.at[q], B.out_terms.at[b], s, q) for q in ex.line()]

    def line_sum(mine, landed):
        total = mine
        for k in (1, 2, 3):
            total = total + landed[(b + k) % 4].astype(F32)
        return total

    ex.terms_arrived(down_grads)
    grad_down[...] = line_sum(B.down_src[b].astype(F32), B.down_terms)
    ex.terms_arrived(up_grads)
    B.up_own[...] = line_sum(B.up_src[:, b].astype(F32), B.up_terms).astype(BF)
    up_lanes = up_fin.at[:, columns(s * 512, 512)]
    up_copies = [ex.send(B.up_own.at[p], up_lanes, p, b) for p in ex.plane()]
    own_up = ex.local(B.up_own.at[s], up_lanes)

    dh1 = ex.sum_end(dh1_over, B.dh1_chips, B.total)
    normal_a, inverse_a = centred(x_in[...].astype(F32))
    grad_input[...] = (B.dr[...] + norm_back(dh1, gain_a, normal_a, inverse_a)).astype(BF)
    wide = jnp.concatenate(
        [
            column_sum(dh1 * normal_a),
            sum_gain_b,
            sum_gain_c,
            column_sum(dh1),
            sum_shift_b,
            sum_shift_c,
            jnp.zeros((1, 1024), F32),
            sum_g,
            jnp.zeros((1, 1024), F32),
            sum_da,
            jnp.zeros((6, 1024), F32),
        ],
        axis=0,
    )
    by_head = jnp.zeros((1, 128), F32)
    for h in range(2):
        found = jnp.sum(of_head(scale_sums / own_scale, h), axis=-1, keepdims=True)
        by_head = jnp.where(lane == s * 2 + h, found, by_head)
    place = lax.broadcasted_iota(jnp.int32, (16, 128), 0)
    for p in range(8):
        mine = jnp.where(s == p, 1.0, 0.0)
        tile = wide[:, p * 128 : (p + 1) * 128]
        tile = jnp.where(place == 6, sum_dq * mine, tile)
        tile = jnp.where(place == 8, sum_dv * mine, tile)
        B.close_src[p] = jnp.where(place == 10, by_head, tile)
    for q in range(4):
        part = [one[:, q * 128 : (q + 1) * 128] for one in ff_sums]
        B.ff_src[q] = jnp.concatenate(part + [jnp.zeros((5, 128), F32)], axis=0)
    close = [ex.send(B.close_src.at[p], B.close_all.at[me], p, q) for p, q in partners]
    close_ff = [ex.send(B.ff_src.at[q], B.ff_all.at[b], s, q) for q in ex.line()]
    own_close = [ex.local(B.close_src.at[s], B.close_all.at[me]), ex.local(B.ff_src.at[b], B.ff_all.at[b])]

    ex.terms_arrived(qkv_grads)
    B.qkv_own[...] = line_sum(B.qkv_src[:, b].astype(F32), B.qkv_terms).astype(BF)
    qkv_lanes = lambda t: qkv_fin.at[:, columns(t * 1024 + s * 128, 128)]
    qkv_piece = lambda p, t: B.qkv_own.at[p, :, pl.ds(t * 128, 128)]
    qkv_copies = [ex.send(qkv_piece(p, t), qkv_lanes(t), p, b) for p in ex.plane() for t in range(3)]
    own_qkv = [ex.local(qkv_piece(s, t), qkv_lanes(t)) for t in range(3)]
    ex.arrived(out_grads)
    grad_out[...] = line_sum(B.out_src[b].astype(F32), B.out_terms)
    ex.arrived(up_copies)
    own_up.wait()
    ex.arrived(close)
    ex.arrived(close_ff)
    for one in own_close:
        one.wait()
    total = B.close_all[0]
    for i in range(1, 32):
        total = total + B.close_all[i]
    vec_out[...] = total
    ff_out[...] = B.ff_all[0] + B.ff_all[1] + B.ff_all[2] + B.ff_all[3]
    ex.arrived(qkv_copies)
    for one in own_qkv:
        one.wait()
    ex.finish()


def finish_kernel(output, grad_input, qkv, out, up, down, narrow, wide, *outs):
    b = lax.axis_index("batch")
    outs[0][0] = output[...]
    outs[1][0] = grad_input[...]
    outs[2][...] = qkv[...].astype(F32)
    outs[3][...] = out[...]
    outs[4][...] = up[...].astype(F32)
    outs[5][...] = down[...]
    rows = narrow[...]
    own = rows[:, 0:32]
    for q in range(1, 4):
        own = jnp.where(b == q, rows[:, q * 32 : (q + 1) * 32], own)
    outs[6][...] = own[0:3]
    outs[7][...] = own[3:8]
    outs[8][...] = own[8:10]
    outs[9][...] = wide[0:1, :]
    outs[10][...] = wide[1:3, :]
    outs[11][...] = rows[10:11, :H]


def plane_shards(
    inputs,
    lengths,
    w_qkv,
    w_out,
    w_up,
    w_down,
    norm_gains,
    model_biases,
    attn_biases,
    ff_gain,
    ff_biases,
    head_scale,
    cotangent,
):
    b = lax.axis_index("batch")
    near = pl.BlockSpec(memory_space=pltpu.VMEM)
    outs = [
        ((128, 1024), BF),
        ((128, 1024), BF),
        ((32, 3072), BF),
        ((32, 1024), F32),
        ((32, 4096), BF),
        ((128, 1024), F32),
        ((16, 128), F32),
        ((8, 128), F32),
    ]
    found = pl.pallas_call(
        block_kernel,
        name="block",
        out_shape=[jax.ShapeDtypeStruct(shape, dtype) for shape, dtype in outs],
        in_specs=[pl.BlockSpec(memory_space=pltpu.SMEM)] + [near] * (INPUTS - 1),
        out_specs=[near] * OUTPUTS,
        scratch_shapes=[pltpu.VMEM(shape, dtype) for shape, dtype in BUFFERS.values()]
        + [
            pltpu.SemaphoreType.DMA((COPIES,)),
            pltpu.SemaphoreType.DMA((COPIES,)),
            pltpu.SemaphoreType.DMA((32,)),
        ],
        compiler_params=pltpu.CompilerParams(
            collective_id=1, has_side_effects=True, vmem_limit_bytes=67043328
        ),
    )(
        lengths.reshape(1, 1),
        inputs[0],
        cotangent[0],
        w_qkv,
        w_out,
        w_up,
        w_down,
        norm_gains,
        model_biases,
        attn_biases,
        ff_gain.reshape(1, 128),
        ff_biases,
        head_scale.reshape(1, H),
    )
    finals = [
        ((1, 128, 1024), BF),
        ((1, 128, 1024), BF),
        ((32, 3072), F32),
        ((32, 1024), F32),
        ((32, 4096), F32),
        ((128, 1024), F32),
        ((3, 32), F32),
        ((5, 32), F32),
        ((2, 32), F32),
        ((1, 128), F32),
        ((2, 128), F32),
        ((1, H), F32),
    ]
    last = pl.pallas_call(
        finish_kernel,
        name="finish",
        out_shape=[jax.ShapeDtypeStruct(shape, dtype) for shape, dtype in finals],
        in_specs=[near] * OUTPUTS,
        out_specs=[near] * len(finals),
        compiler_params=pltpu.CompilerParams(vmem_limit_bytes=67043328),
    )(*found)
    return tuple(last[:9]) + (last[9].reshape(128), last[10], last[11].reshape(H))


def solution(mesh):
    in_plane = mesh.shape["seq"] == 8 and mesh.shape["batch"] == 4
    return jax.shard_map(
        plane_shards if in_plane else shards,
        mesh=mesh,
        in_specs=(
            P("batch", "seq", None),
            P("batch"),
            P(("seq", "batch"), None),
            P(("seq", "batch"), None),
            P(("seq", "batch"), None),
            P(("seq", "batch"), None),
            P(None, ("seq", "batch")),
            P(None, ("seq", "batch")),
            P(None, ("seq", "batch")),
            P(("seq", "batch")),
            P(None, ("seq", "batch")),
            P(),
            P("batch", "seq", None),
        ),
        out_specs=(
            P("batch", "seq", None),
            P("batch", "seq", None),
            P(("seq", "batch"), None),
            P(("seq", "batch"), None),
            P(("seq", "batch"), None),
            P(("seq", "batch"), None),
            P(None, ("seq", "batch")),
            P(None, ("seq", "batch")),
            P(None, ("seq", "batch")),
            P(("seq", "batch")),
            P(None, ("seq", "batch")),
            P(),
        ),
        check_vma=False,
    )
```

```python
import jax
import jax.numpy as jnp
from jax import lax
from jax.experimental import pallas as pl
from jax.experimental.pallas import tpu as pltpu
from jax.sharding import PartitionSpec as P

H = 16
HD = 64


NORM_EPSILON = 1e-05


def layer_norm(vector, norm_gain, norm_bias):
    centered = vector - jnp.mean(vector, axis=-1, keepdims=True)
    spread = jnp.mean(centered * centered, axis=-1, keepdims=True)
    return centered * lax.rsqrt(spread + NORM_EPSILON) * norm_gain + norm_bias


def gelu_norm(hidden, norm_gain, norm_bias):
    return layer_norm(jax.nn.gelu(hidden, approximate=False), norm_gain, norm_bias)


def contract_rows(left, right):
    return lax.dot_general(
        left, right, (((0,), (0,)), ((), ())), preferred_element_type=jnp.float32
    )


def times_transposed(left, right):
    return lax.dot_general(
        left, right, (((1,), (1,)), ((), ())), preferred_element_type=jnp.float32
    )


def shards(
    inputs,
    lengths,
    w_qkv,
    w_out,
    w_up,
    w_down,
    norm_gains,
    model_biases,
    attn_biases,
    ff_gain,
    ff_biases,
    head_scale,
    cotangent,
):
    gathered = (
        lax.all_gather(w_qkv, ("seq", "batch"), axis=0, tiled=True),
        lax.all_gather(w_out, ("seq", "batch"), axis=0, tiled=True),
        lax.all_gather(w_up, ("seq", "batch"), axis=0, tiled=True),
        lax.all_gather(w_down, ("seq", "batch"), axis=0, tiled=True),
        lax.all_gather(norm_gains, ("seq", "batch"), axis=1, tiled=True),
        lax.all_gather(model_biases, ("seq", "batch"), axis=1, tiled=True),
        lax.all_gather(attn_biases, ("seq", "batch"), axis=1, tiled=True),
        lax.all_gather(ff_gain, ("seq", "batch"), axis=0, tiled=True),
        lax.all_gather(ff_biases, ("seq", "batch"), axis=1, tiled=True),
    )
    qkv_full, out_full, up_full, down_full = (gathered[0], gathered[1], gathered[2], gathered[3])
    gain_rows = gathered[4].astype(jnp.float32)
    bias_rows = gathered[5].astype(jnp.float32)
    attn_rows = gathered[6].astype(jnp.float32)
    ffn_gain = gathered[7].astype(jnp.float32)
    ffn_rows = gathered[8].astype(jnp.float32)
    scales = head_scale.astype(jnp.float32)
    local_rows = inputs.shape[1]
    model_width = inputs.shape[2]
    seq_length = local_rows * lax.axis_size("seq")
    tile_rows = min(512, seq_length)
    first_row = lax.axis_index("seq") * local_rows
    valid_rows = lengths[0]
    positions = first_row + jnp.arange(local_rows, dtype=jnp.int32)
    valid_mask = (positions < valid_rows)[:, None]
    score_scale = HD ** (-0.5)
    residual_in = inputs[0].astype(jnp.float32)
    normed, norm_a_pull = jax.vjp(layer_norm, residual_in, gain_rows[0], bias_rows[0])
    normed_low = normed.astype(jnp.bfloat16)
    offsets = jnp.concatenate([bias_rows[3], jnp.zeros_like(bias_rows[3]), attn_rows[0]])
    projected = (
        jnp.dot(normed_low, qkv_full, preferred_element_type=jnp.float32) + offsets
    ).astype(jnp.bfloat16)
    queries = projected[:, :model_width]
    key_local = projected[:, model_width : 2 * model_width]
    value_local = projected[:, 2 * model_width :]
    key_rows, value_rows = (
        lax.all_gather(key_local, "seq", axis=0, tiled=True),
        lax.all_gather(value_local, "seq", axis=0, tiled=True),
    )
    query_heads = queries.reshape(local_rows, H, HD)
    last_needed = jnp.minimum(first_row + local_rows - 1, valid_rows - 1)
    tile_count = last_needed // tile_rows + 1

    def tile_scores(j):
        start = j * tile_rows
        key_tile = lax.dynamic_slice_in_dim(key_rows, start, tile_rows, 0).reshape(tile_rows, H, HD)
        scores = (
            jnp.einsum("qhd,khd->hqk", query_heads, key_tile, preferred_element_type=jnp.float32)
            * score_scale
        )
        key_index = start + jnp.arange(tile_rows, dtype=jnp.int32)
        allowed = (key_index[None, :] <= positions[:, None]) & (key_index[None, :] < valid_rows)
        return (scores, allowed[None], key_tile)

    def max_and_sum(j, carry):
        running_max, running_sum = carry
        scores, allowed, unused_tile = tile_scores(j)
        masked = jnp.where(allowed, scores, -1e30)
        new_max = jnp.maximum(running_max, jnp.max(masked, axis=-1))
        kept_terms = jnp.where(allowed, jnp.exp(masked - new_max[..., None]), 0.0)
        return (
            new_max,
            running_sum * jnp.exp(running_max - new_max) + jnp.sum(kept_terms, axis=-1),
        )

    start_stats = (
        jnp.full((H, local_rows), -1e30, jnp.float32),
        jnp.zeros((H, local_rows), jnp.float32),
    )
    running_max, running_sum = lax.fori_loop(0, tile_count, max_and_sum, start_stats)
    log_total = running_max + jnp.log(running_sum)

    def tile_probs(j):
        scores, allowed, key_tile = tile_scores(j)
        attn_probs = jnp.where(allowed, jnp.exp(scores - log_total[..., None]), 0.0)
        value_tile = lax.dynamic_slice_in_dim(value_rows, j * tile_rows, tile_rows, 0).reshape(
            tile_rows, H, HD
        )
        return (attn_probs, key_tile, value_tile)

    def accumulate(j, summed):
        attn_probs, unused_tile, value_tile = tile_probs(j)
        return summed + jnp.einsum(
            "hqk,khd->qhd",
            attn_probs.astype(jnp.bfloat16),
            value_tile,
            preferred_element_type=jnp.float32,
        )

    attended = lax.fori_loop(0, tile_count, accumulate, jnp.zeros((local_rows, H, HD), jnp.float32))
    scaled_low = (
        (attended * scales[None, :, None]).reshape(local_rows, model_width).astype(jnp.bfloat16)
    )
    attn_proj = jnp.dot(scaled_low, out_full, preferred_element_type=jnp.float32) + attn_rows[1]
    attn_normed, norm_b_pull = jax.vjp(layer_norm, attn_proj, gain_rows[1], bias_rows[1])
    residual = residual_in + attn_normed
    ffn_in, norm_c_pull = jax.vjp(layer_norm, residual, gain_rows[2], bias_rows[2])
    ffn_low = ffn_in.astype(jnp.bfloat16)
    hidden = jnp.dot(ffn_low, up_full, preferred_element_type=jnp.float32) + ffn_rows[0]
    ffn_normed, ffn_pull = jax.vjp(gelu_norm, hidden, ffn_gain, ffn_rows[1])
    ffn_out_low = ffn_normed.astype(jnp.bfloat16)
    combined = jnp.where(
        valid_mask,
        residual
        + jnp.dot(ffn_out_low, down_full, preferred_element_type=jnp.float32)
        + bias_rows[4],
        0.0,
    )
    output = combined.astype(jnp.bfloat16)[None]
    barrier_out = lax.optimization_barrier(((w_qkv, w_out, w_up, w_down), combined))
    regathered = (
        lax.all_gather(barrier_out[0][0], ("seq", "batch"), axis=0, tiled=True),
        lax.all_gather(barrier_out[0][1], ("seq", "batch"), axis=0, tiled=True),
        lax.all_gather(barrier_out[0][2], ("seq", "batch"), axis=0, tiled=True),
        lax.all_gather(barrier_out[0][3], ("seq", "batch"), axis=0, tiled=True),
    )
    qkv_full, out_full, up_full, down_full = (
        regathered[0],
        regathered[1],
        regathered[2],
        regathered[3],
    )
    cotan_rows = jnp.where(valid_mask, cotangent[0], jnp.zeros_like(cotangent[0]))
    cotan_float = cotan_rows.astype(jnp.float32)
    grad_down = contract_rows(ffn_out_low, cotan_rows)
    grad_bias_out = jnp.sum(cotan_float, axis=0)
    grad_ffn_normed = times_transposed(cotan_rows, down_full)
    grad_hidden, grad_ffn_gain, grad_ffn_shift = ffn_pull(grad_ffn_normed)
    grad_hidden_low = grad_hidden.astype(jnp.bfloat16)
    grad_up = contract_rows(ffn_low, grad_hidden_low)
    grad_ffn_bias = jnp.sum(grad_hidden_low.astype(jnp.float32), axis=0)
    grad_ffn_in = times_transposed(grad_hidden_low, up_full)
    grad_from_ffn, grad_gain_c, grad_shift_c = norm_c_pull(grad_ffn_in)
    grad_residual = cotan_float + grad_from_ffn
    grad_proj, grad_gain_b, grad_shift_b = norm_b_pull(grad_residual)
    grad_proj_low = grad_proj.astype(jnp.bfloat16)
    grad_out_bias = jnp.sum(grad_proj_low.astype(jnp.float32), axis=0)
    grad_out = contract_rows(scaled_low, grad_proj_low)
    grad_scaled = times_transposed(grad_proj_low, out_full).reshape(local_rows, H, HD)
    grad_scales = jnp.sum(grad_scaled * attended, axis=(0, 2))
    grad_heads_low = (grad_scaled * scales[None, :, None]).astype(jnp.bfloat16)
    row_delta = jnp.einsum("qhd,qhd->hq", grad_heads_low.astype(jnp.float32), attended)

    def score_grads(j):
        attn_probs, key_tile, value_tile = tile_probs(j)
        grad_probs = jnp.einsum(
            "qhd,khd->hqk", grad_heads_low, value_tile, preferred_element_type=jnp.float32
        )
        grad_scores = (attn_probs * (grad_probs - row_delta[..., None])).astype(jnp.bfloat16)
        return (attn_probs, grad_scores, key_tile)

    def backward_tile(j, carry):
        grad_query, terms = carry
        attn_probs, grad_scores, key_tile = score_grads(j)
        grad_query = grad_query + jnp.einsum(
            "hqk,khd->qhd", grad_scores, key_tile, preferred_element_type=jnp.float32
        )
        grad_key = (
            jnp.einsum("hqk,qhd->khd", grad_scores, query_heads, preferred_element_type=jnp.float32)
            * score_scale
        )
        grad_value = jnp.einsum(
            "hqk,qhd->khd",
            attn_probs.astype(jnp.bfloat16),
            grad_heads_low,
            preferred_element_type=jnp.float32,
        )
        piece = jnp.concatenate(
            [grad_key.reshape(tile_rows, model_width), grad_value.reshape(tile_rows, model_width)],
            axis=1,
        )
        return (grad_query, lax.dynamic_update_slice_in_dim(terms, piece, j * tile_rows, 0))

    start_carry = (
        jnp.zeros((local_rows, H, HD), jnp.float32),
        jnp.zeros((seq_length, 2 * model_width), jnp.float32),
    )
    grad_query, terms = lax.fori_loop(0, tile_count, backward_tile, start_carry)
    grad_kv = lax.psum_scatter(terms, "seq", scatter_dimension=0, tiled=True)
    grad_query_low = (
        (grad_query * score_scale).reshape(local_rows, model_width).astype(jnp.bfloat16)
    )
    grad_kv_low = grad_kv.astype(jnp.bfloat16)
    grad_projected = jnp.concatenate([grad_query_low, grad_kv_low], axis=1)
    grad_qkv = contract_rows(normed_low, grad_projected)
    grad_query_bias = jnp.sum(grad_query_low.astype(jnp.float32), axis=0)
    grad_value_bias = jnp.sum(grad_kv_low[:, model_width:].astype(jnp.float32), axis=0)
    grad_normed = times_transposed(grad_projected, qkv_full)
    grad_from_attn, grad_gain_a, grad_shift_a = norm_a_pull(grad_normed)
    grad_input = (grad_residual + grad_from_attn).astype(jnp.bfloat16)[None]
    reduced = (
        lax.psum_scatter(grad_qkv, ("seq", "batch"), scatter_dimension=0, tiled=True),
        lax.psum_scatter(grad_out, ("seq", "batch"), scatter_dimension=0, tiled=True),
        lax.psum_scatter(grad_up, ("seq", "batch"), scatter_dimension=0, tiled=True),
        lax.psum_scatter(grad_down, ("seq", "batch"), scatter_dimension=0, tiled=True),
        lax.psum_scatter(
            jnp.stack([grad_gain_a, grad_gain_b, grad_gain_c]),
            ("seq", "batch"),
            scatter_dimension=1,
            tiled=True,
        ),
        lax.psum_scatter(
            jnp.stack([grad_shift_a, grad_shift_b, grad_shift_c, grad_query_bias, grad_bias_out]),
            ("seq", "batch"),
            scatter_dimension=1,
            tiled=True,
        ),
        lax.psum_scatter(
            jnp.stack([grad_value_bias, grad_out_bias]),
            ("seq", "batch"),
            scatter_dimension=1,
            tiled=True,
        ),
        lax.psum_scatter(grad_ffn_gain, ("seq", "batch"), scatter_dimension=0, tiled=True),
        lax.psum_scatter(
            jnp.stack([grad_ffn_bias, grad_ffn_shift]),
            ("seq", "batch"),
            scatter_dimension=1,
            tiled=True,
        ),
    )
    scale_total = lax.psum(grad_scales, ("seq", "batch"))
    return (
        output,
        grad_input,
        reduced[0],
        reduced[1],
        reduced[2],
        reduced[3],
        reduced[4],
        reduced[5],
        reduced[6],
        reduced[7],
        reduced[8],
        scale_total,
    )


BF = jnp.bfloat16
F32 = jnp.float32


class Exchange:
    def __init__(self, send_sems, recv_sems, local_sems):
        self.send_sems = send_sems
        self.recv_sems = recv_sems
        self.local_sems = local_sems
        self.count = 0
        self.locals = 0
        self.sent = []
        self.sent_if = []
        self.s = lax.axis_index("seq")
        self.b = lax.axis_index("batch")
        self.chip = self.s // 2
        self.core = self.s % 2
        self.sibling = self.chip * 2 + 1 - self.core
        self.plane_peers = [(self.s + j) % 8 for j in range(1, 8)]
        self.line_peers = [(self.b + k) % 4 for k in range(1, 4)]

    def send(self, src, dst, seq, batch):
        at = self.count
        self.count += 1
        copy = pltpu.make_async_remote_copy(
            src_ref=src,
            dst_ref=dst,
            send_sem=self.send_sems.at[at],
            recv_sem=self.recv_sems.at[at],
            device_id=(seq, batch),
            device_id_type=pl.DeviceIdType.MESH,
        )
        copy.start()
        self.sent.append(copy)
        return copy

    def describe(self, src, dst, seq, batch, sent_at, recv_at):
        return pltpu.make_async_remote_copy(
            src_ref=src,
            dst_ref=dst,
            send_sem=self.send_sems.at[sent_at],
            recv_sem=self.recv_sems.at[recv_at],
            device_id=(seq, batch),
            device_id_type=pl.DeviceIdType.MESH,
        )

    def send_if(self, held, copy):
        @pl.when(held)
        def _():
            copy.start()

        self.sent_if.append((held, copy))

    def line_start(self, src, slot):
        first = self.count
        self.count += 4
        b = self.b
        copies = [
            self.describe(src, slot(b), self.s, (b + k) % 4, first + k - 1, first + k - 1) for k in (1, 2, 3)
        ]
        copies[1].start()
        self.sent.append(copies[1])
        return copies, slot, first

    def line_near(self, line):
        copies = line[0]
        self.send_if(self.b != 3, copies[0])
        self.send_if(self.b != 0, copies[2])

    def line_relay(self, line):
        copies, slot, first = line
        b = self.b

        @pl.when((b == 1) | (b == 2))
        def _():
            copies[1].wait_recv()

        came = slot((b + 2) % 4)
        self.send_if(b == 1, self.describe(came, came, self.s, 0, first + 3, first))
        self.send_if(b == 2, self.describe(came, came, self.s, 3, first + 3, first + 2))

    def line_arrived(self, line):
        copies, _slot, _first = line
        copies[0].wait_recv()
        copies[2].wait_recv()

        @pl.when((self.b == 0) | (self.b == 3))
        def _():
            copies[1].wait_recv()

    def terms_start(self, view, landed, passing):
        first = self.count
        self.count += 4
        b = self.b
        at = lambda q, k: self.describe(view(q), landed.at[b], self.s, q, first + k - 1, first + k - 1)
        up, over, down = at((b + 1) % 4, 1), at((b + 2) % 4, 2), at((b + 3) % 4, 3)
        to_one = self.describe(view(3), passing, self.s, 1, first + 3, first + 3)
        to_two = self.describe(view(0), passing, self.s, 2, first + 3, first + 3)
        self.send_if(b == 0, to_one)
        self.send_if(b == 3, to_two)
        self.send_if((b == 0) | (b == 3), over)
        self.send_if(b != 3, up)
        self.send_if(b != 0, down)
        return up, over, down, to_one, landed, passing, first

    def terms_relay(self, terms, mine, joined):
        up, over, down, to_one, landed, passing, first = terms
        b = self.b
        held = (b == 1) | (b == 2)

        @pl.when(held)
        def _():
            to_one.wait_recv()
            joined[...] = (mine((b + 2) % 4).astype(F32) + passing[...].astype(F32)).astype(BF)

        self.send_if(
            held, self.describe(joined, landed.at[b], self.s, (b + 2) % 4, first + 1, first + 1)
        )

    def terms_arrived(self, terms):
        up, over, down = terms[:3]
        over.wait_recv()

        @pl.when(self.b != 0)
        def _():
            up.wait_recv()

        @pl.when(self.b != 3)
        def _():
            down.wait_recv()

    def local(self, src, dst):
        at = self.locals
        self.locals += 1
        copy = pltpu.make_async_copy(src, dst, self.local_sems.at[at])
        copy.start()
        return copy

    def arrived(self, copies):
        for copy in copies:
            copy.wait_recv()

    def finish(self):
        for copy in self.sent:
            copy.wait_send()
        for held, copy in self.sent_if:
            pl.when(held)(copy.wait_send)

    def peer(self, k):
        return ((self.chip + k) % 4) * 2 + self.core

    def source(self, k):
        return ((self.chip + 4 - k) % 4) * 2 + self.core

    def chip_source(self, k):
        return (self.chip + 4 - k) % 4

    def tile(self, j):
        return (self.chip + j + 1) % 4 * 2 + jnp.where(j < 4, 1 - self.core, self.core)

    def plane(self):
        return self.plane_peers

    def line(self):
        return self.line_peers

    def gather_start(self, src, slot):
        copies = [self.send(src, slot(self.s), self.peer(k), self.b) for k in (1, 2, 3)]
        copies.append(self.send(src, slot(self.s), self.sibling, self.b))
        return copies

    def gather_forward(self, copies, slot):
        passed = []
        for k in (1, 2, 3):
            copies[k - 1].wait_recv()
            came = slot(self.source(k))
            passed.append(self.send(came, came, self.sibling, self.b))
        return [copies[3]] + passed

    def sum_pair(self, src, from_pair):
        return [
            self.send(src.at[((self.chip + k) % 4) * 2 + 1 - self.core], from_pair.at[k], self.sibling, self.b)
            for k in (1, 2, 3, 0)
        ]

    def sum_chips(self, copies, src, from_pair, paired, from_chips, total):
        over = []
        for at, k in enumerate((1, 2, 3, 0)):
            copies[at].wait_recv()
            mine = src[((self.chip + k) % 4) * 2 + self.core].astype(F32)
            both = mine + from_pair[k].astype(F32)
            if k:
                paired[k - 1] = both.astype(BF)
                over.append(self.send(paired.at[k - 1], from_chips.at[k - 1], self.peer(k), self.b))
            else:
                total[...] = both
        return over

    def sum_end(self, over, from_chips, total):
        self.arrived(over)
        return total[...] + from_chips[0].astype(F32) + from_chips[1].astype(F32) + from_chips[2].astype(F32)


def columns(start, size):
    return pl.ds(pl.multiple_of(start, 128), size)


def centred(rows):
    middle = rows - jnp.mean(rows, axis=-1, keepdims=True)
    inverse = lax.rsqrt(jnp.mean(middle * middle, axis=-1, keepdims=True) + NORM_EPSILON)
    return middle * inverse, inverse


def norm_back(upstream, gain, normal, inverse):
    scaled = upstream * gain
    average = jnp.mean(scaled, axis=-1, keepdims=True)
    along = jnp.mean(scaled * normal, axis=-1, keepdims=True)
    return inverse * (scaled - average - normal * along)


def gelu_parts(z):
    phi = 0.5 * (1.0 + lax.erf(z * 0.7071067811865476))
    density = 0.3989422804014327 * jnp.exp(-0.5 * z * z)
    return z * phi, phi + z * density


def matmul(left, right):
    return jnp.dot(left, right, preferred_element_type=F32)


def column_sum(rows):
    return jnp.sum(rows, axis=0, keepdims=True)


def pack_columns(parts):
    lane = lax.broadcasted_iota(jnp.int32, (128, 128), 1)
    wide = jnp.zeros((128, 128), F32)
    for at, part in enumerate(parts):
        wide = jnp.where(lane == at, part, wide)
    return wide.T[:8]


BUFFERS = dict(
    x_all=((8, 128, 1024), BF),
    g_all=((8, 128, 1024), BF),
    qkv_w=((8, 4, 32, 384), BF),
    out_w=((8, 4, 32, 1024), BF),
    up_w=((8, 4, 32, 512), BF),
    down_w=((4, 128, 1024), BF),
    vec_src=((16, 128), F32),
    vec_all=((8, 4, 16, 128), F32),
    qkv_send=((8, 32, 384), BF),
    scale_row=((8, 1024), F32),
    rows=((16, 1024), F32),
    ff_rows=((8, 512), F32),
    h1=((1024, 1024), BF),
    qkv=((1024, 384), BF),
    probs_low=((2, 512, 512), F32),
    probs_high=((2, 512, 1024), F32),
    attended=((1024, 128), F32),
    scaled=((8, 128, 128), BF),
    scaled_local=((128, 1024), BF),
    normal_b=((128, 1024), F32),
    normal_c=((128, 1024), F32),
    residual=((128, 1024), F32),
    h2_all=((8, 128, 1024), BF),
    active=((1024, 512), F32),
    slope=((1024, 512), F32),
    du2=((1024, 512), F32),
    stats=((8, 8, 128), F32),
    stats_all=((8, 8, 8, 128), F32),
    u2=((1024, 512), BF),
    dz=((1024, 512), BF),
    dh2_pair=((4, 128, 1024), BF),
    dh2_paired=((3, 128, 1024), BF),
    dh2_chips=((3, 128, 1024), BF),
    ffo_src=((8, 128, 1024), BF),
    ffo_pair=((4, 128, 1024), BF),
    ffo_paired=((3, 128, 1024), BF),
    ffo_chips=((3, 128, 1024), BF),
    dh1_src=((8, 128, 1024), BF),
    dh1_pair=((4, 128, 1024), BF),
    dh1_paired=((3, 128, 1024), BF),
    dh1_chips=((3, 128, 1024), BF),
    total=((128, 1024), F32),
    ffo_total=((128, 1024), F32),
    dr=((128, 1024), F32),
    da_all=((8, 128, 1024), BF),
    do_local=((128, 1024), BF),
    do_all=((8, 128, 128), BF),
    dq=((1024, 128), F32),
    dk=((1024, 128), F32),
    dv=((1024, 128), F32),
    dqkv=((1024, 384), BF),
    up_src=((8, 4, 32, 512), BF),
    up_terms=((4, 8, 32, 512), BF),
    down_src=((4, 128, 1024), BF),
    down_terms=((4, 128, 1024), BF),
    qkv_src=((8, 4, 32, 384), BF),
    qkv_terms=((4, 8, 32, 384), BF),
    up_passing=((8, 32, 512), BF),
    up_joined=((8, 32, 512), BF),
    down_passing=((128, 1024), BF),
    down_joined=((128, 1024), BF),
    qkv_passing=((8, 32, 384), BF),
    qkv_joined=((8, 32, 384), BF),
    out_src=((4, 32, 1024), BF),
    out_terms=((4, 32, 1024), BF),
    up_own=((8, 32, 512), BF),
    qkv_own=((8, 32, 384), BF),
    close_src=((8, 16, 128), F32),
    close_plane=((8, 16, 128), F32),
    close_line=((4, 24, 128), F32),
    close_all=((4, 24, 128), F32),
)
COPIES = 240
INPUTS = 13
OUTPUTS = 7


def block_kernel(
    length_in,
    x_in,
    g_in,
    qkv_in,
    out_in,
    up_in,
    down_in,
    gains_in,
    biases_in,
    attn_in,
    ff_gain_in,
    ff_bias_in,
    scale_in,
    *refs,
):
    output, grad_input, qkv_fin, grad_out, up_fin, grad_down, vec_out = refs[:OUTPUTS]
    B = type("Buffers", (), dict(zip(BUFFERS, refs[OUTPUTS : OUTPUTS + len(BUFFERS)])))
    ex = Exchange(*refs[OUTPUTS + len(BUFFERS) :])
    s, b = ex.s, ex.b
    valid_rows = length_in[0, 0]

    lane = lax.broadcasted_iota(jnp.int32, (1, 128), 1)

    def spread(part):
        values = part[...].astype(F32)
        return jnp.where(lane // 32 == b, jnp.concatenate([values] * 4, axis=1), 0.0)

    B.vec_src[0:3, :] = spread(gains_in)
    B.vec_src[3:8, :] = spread(biases_in)
    B.vec_src[8:10, :] = spread(attn_in)
    B.vec_src[10:11, :] = ff_gain_in[...].astype(F32)
    B.vec_src[11:13, :] = ff_bias_in[...].astype(F32)
    B.vec_src[13:16, :] = jnp.zeros((3, 128), F32)
    held = s * 128 + lax.broadcasted_iota(jnp.int32, (128, 1), 0) < valid_rows
    B.g_all[s] = jnp.where(held, g_in[...].astype(F32), 0.0).astype(BF)
    by_head = lax.broadcasted_iota(jnp.int32, (8, 1024), 1) // HD
    head_scales = scale_in[...].astype(F32)
    scale_row = jnp.zeros((8, 1024), F32)
    for h in range(H):
        scale_row = jnp.where(by_head == h, head_scales[0:1, h : h + 1], scale_row)
    B.scale_row[...] = scale_row

    for p in range(8):
        for t in range(3):
            B.qkv_send[p, :, t * 128 : (t + 1) * 128] = qkv_in[:, t * 1024 + p * 128 : t * 1024 + (p + 1) * 128]

    for landed in (B.up_terms, B.down_terms, B.qkv_terms):

        @pl.when(b == 3)
        def _():
            landed[0] = jnp.zeros(landed.shape[1:], BF)

        @pl.when(b == 0)
        def _():
            landed[3] = jnp.zeros(landed.shape[1:], BF)

    barrier = pltpu.get_barrier_semaphore()
    partners = [(p, b) for p in ex.plane()] + [(s, q) for q in ex.line()]
    for seq, batch in partners:
        pl.semaphore_signal(barrier, inc=1, device_id=(seq, batch), device_id_type=pl.DeviceIdType.MESH)
    pl.semaphore_wait(barrier, len(partners))

    qkv_copies = [ex.send(B.qkv_send.at[p], B.qkv_w.at[s, b], p, b) for p in ex.plane()]
    out_line = ex.line_start(out_in, lambda i: B.out_w.at[s, i])
    ex.line_near(out_line)
    own = [ex.local(B.qkv_send.at[s], B.qkv_w.at[s, b])]
    own_up = ex.local(up_in.at[:, columns(s * 512, 512)], B.up_w.at[s, b])
    own_rest = [
        ex.local(out_in, B.out_w.at[s, b]),
        ex.local(x_in, B.x_all.at[s]),
        ex.local(down_in, B.down_w.at[b]),
        ex.local(B.vec_src, B.vec_all.at[s, b]),
    ]
    x_slot = lambda i: B.x_all.at[i]
    g_slot = lambda i: B.g_all.at[i]
    x_copies = ex.gather_start(x_in, x_slot)
    vec_line = [ex.send(B.vec_src, B.vec_all.at[s, b], s, q) for q in ex.line()]
    up_copies = [ex.send(up_in.at[:, columns(p * 512, 512)], B.up_w.at[s, b], p, b) for p in ex.plane()]
    ex.arrived(qkv_copies)
    for one in own:
        one.wait()
    qkv_line = ex.line_start(B.qkv_w.at[:, b], lambda i: B.qkv_w.at[:, i])
    ex.line_near(qkv_line)
    for one in own_rest:
        one.wait()
    ex.arrived(vec_line)
    vec_slot = lambda i: B.vec_all.at[i]
    vec_copies = ex.gather_start(B.vec_all.at[s], vec_slot)
    ex.line_relay(out_line)
    x_passed = ex.gather_forward(x_copies, x_slot)
    ex.arrived(up_copies)
    own_up.wait()
    ex.line_relay(qkv_line)
    down_line = ex.line_start(down_in, lambda i: B.down_w.at[i])
    up_line = ex.line_start(B.up_w.at[:, b], lambda i: B.up_w.at[:, i])
    ex.line_near(down_line)
    ex.line_near(up_line)
    g_copies = ex.gather_start(B.g_all.at[s], g_slot)
    ex.arrived(ex.gather_forward(vec_copies, vec_slot))

    for p in range(8):
        group = B.vec_all[p, 0] + B.vec_all[p, 1] + B.vec_all[p, 2] + B.vec_all[p, 3]
        B.rows[:, p * 128 : (p + 1) * 128] = group
    for q in range(4):
        B.ff_rows[:, q * 128 : (q + 1) * 128] = B.vec_all[s, q][8:16]
    row = lambda at: B.rows[at : at + 1, :]
    gain_a, gain_b, gain_c = row(0), row(1), row(2)
    bias_a, bias_b, bias_c, bias_out, bias_attn = row(3), row(4), row(5), row(7), row(9)
    ffn_gain, ffn_bias, ffn_shift = B.ff_rows[2:3, :], B.ff_rows[3:4, :], B.ff_rows[4:5, :]
    own_columns = columns(s * 128, 128)
    query_bias = B.rows[6:7, own_columns]
    value_bias = B.rows[8:9, own_columns]
    own_scale = B.scale_row[0:1, own_columns]

    ex.arrived(x_passed)

    @pl.loop(0, 8)
    def _(t):
        normal, _unused = centred(B.x_all[t].astype(F32))
        B.h1[pl.ds(t * 128, 128), :] = (normal * gain_a + bias_a).astype(BF)

    ex.line_arrived(qkv_line)
    offsets = jnp.concatenate([query_bias, jnp.zeros_like(query_bias), value_bias], axis=1)

    @pl.loop(0, 4)
    def _(t):
        at = pl.ds(t * 256, 256)
        B.qkv[at, :] = (matmul(B.h1[at, :], B.qkv_w[...].reshape(1024, 384)) + offsets).astype(BF)

    ex.line_arrived(out_line)
    out_slot = lambda i: B.out_w.at[i]
    out_copies = ex.gather_start(B.out_w.at[s], out_slot)
    g_passed = ex.gather_forward(g_copies, g_slot)

    score_scale = HD ** (-0.5)
    half_of = lax.broadcasted_iota(jnp.int32, (1, 128), 1) // HD

    def of_head(rows, h):
        return jnp.where(half_of == h, rows, jnp.zeros_like(rows))

    for size in (512, 1024):
        if size == 1024:
            ex.line_relay(down_line)
            ex.line_relay(up_line)
        for h in range(2):

            @pl.loop(size // 128 - 4, size // 128)
            def _(t):
                at = pl.ds(t * 128, 128)
                query = of_head(B.qkv[at, 0:128], h).astype(F32) * score_scale
                scores = times_transposed(query.astype(BF), B.qkv[0:size, 128:256])
                key_index = lax.broadcasted_iota(jnp.int32, (128, size), 1)
                query_index = t * 128 + lax.broadcasted_iota(jnp.int32, (128, 1), 0)
                masked = jnp.where(key_index <= jnp.minimum(query_index, valid_rows - 1), scores, -1e30)
                raised = jnp.exp(masked - jnp.max(masked, axis=-1, keepdims=True))
                probs = raised * (1.0 / jnp.sum(raised, axis=-1, keepdims=True))
                kept = B.probs_low if size == 512 else B.probs_high
                kept[h, pl.ds(t * 128 - size + 512, 128), :] = probs
                found = matmul(probs.astype(BF), of_head(B.qkv[0:size, 256:384], h))
                if h == 0:
                    B.attended[at, :] = found
                else:
                    both = B.attended[at, :] + found
                    B.attended[at, :] = both
                    B.scaled[t] = (both * own_scale).astype(BF)

    local_lanes = B.scaled_local.at[:, own_columns]
    heads = [ex.send(B.scaled.at[p], local_lanes, p, b) for p in ex.plane()]
    own_heads = ex.local(B.scaled.at[s], local_lanes)
    out_passed = ex.gather_forward(out_copies, out_slot)
    ex.arrived(out_passed)
    ex.arrived(heads)
    own_heads.wait()

    attn_proj = matmul(B.scaled_local[...], B.out_w[...].reshape(1024, 1024)) + bias_attn
    normal_b, inverse_b = centred(attn_proj)
    B.normal_b[...] = normal_b
    residual = x_in[...].astype(F32) + normal_b * gain_b + bias_b
    B.residual[...] = residual
    normal_c, inverse_c = centred(residual)
    B.normal_c[...] = normal_c
    B.h2_all[s] = (normal_c * gain_c + bias_c).astype(BF)
    h2_slot = lambda i: B.h2_all.at[i]
    h2_copies = ex.gather_start(B.h2_all.at[s], h2_slot)

    ex.arrived(g_passed)
    ex.line_arrived(down_line)
    ex.line_arrived(up_line)

    def upstream(t):
        B.du2[pl.ds(t * 128, 128), :] = times_transposed(B.g_all[t], B.down_w[...].reshape(512, 1024))

    def hidden_tile(t):
        at = pl.ds(t * 128, 128)
        active, slope = gelu_parts(matmul(B.h2_all[t], B.up_w[...].reshape(1024, 512)) + ffn_bias)
        B.active[at, :] = active
        B.slope[at, :] = slope
        dgain = B.du2[at, :] * ffn_gain
        mean = jnp.mean(active, axis=-1, keepdims=True)
        off = active - mean
        add = lambda rows: jnp.sum(rows, axis=-1, keepdims=True)
        B.stats[t] = pack_columns([mean, add(off * off), add(dgain), add(dgain * off)])

    pl.loop(0, 8)(upstream)
    hidden_tile(s)
    h2_copies[3].wait_recv()
    hidden_tile(ex.sibling)
    h2_passed = []
    for k in (1, 3, 2):
        h2_copies[k - 1].wait_recv()
        came = h2_slot(ex.source(k))
        h2_passed.append(ex.send(came, came, ex.sibling, b))
        hidden_tile(ex.source(k))
    for at, k in enumerate((1, 3, 2)):
        h2_passed[at].wait_recv()
        hidden_tile(ex.chip_source(k) * 2 + 1 - ex.core)

    stats_copies = [ex.send(B.stats, B.stats_all.at[s], p, b) for p in ex.plane()]
    own_stats = ex.local(B.stats, B.stats_all.at[s])
    ex.arrived(stats_copies)
    own_stats.wait()

    for copy in x_passed[1:]:
        copy.wait_send()
        ex.sent = [one for one in ex.sent if one is not copy]

    def finish_hidden(j, sums):
        t = ex.tile(j)
        at = pl.ds(t * 128, 128)
        means = [B.stats_all[i, t, 0:1, :] for i in range(8)]
        squares = [B.stats_all[i, t, 1:2, :] for i in range(8)]
        firsts = [B.stats_all[i, t, 2:3, :] for i in range(8)]
        seconds = [B.stats_all[i, t, 3:4, :] for i in range(8)]
        mean = sum(means) * 0.125
        shifts = [one - mean for one in means]
        spread = (sum(squares) + 512.0 * sum(one * one for one in shifts)) * (1.0 / 4096.0)
        inverse = lax.rsqrt(spread + NORM_EPSILON)
        average = sum(firsts) * (1.0 / 4096.0)
        along = inverse * sum(two + one * first for two, one, first in zip(seconds, shifts, firsts)) * (1.0 / 4096.0)
        packed = jnp.concatenate([mean, inverse, average, along, jnp.zeros((124, 128), F32)], axis=0).T
        mean, inverse, average, along = (packed[:, i : i + 1] for i in range(4))
        normal = (B.active[at, :] - mean) * inverse
        B.u2[at, :] = (normal * ffn_gain + ffn_shift).astype(BF)
        du2 = B.du2[at, :]
        dz = (inverse * (du2 * ffn_gain - average - normal * along) * B.slope[at, :]).astype(BF)
        B.dz[at, :] = dz
        B.x_all[t] = times_transposed(dz, B.up_w[...].reshape(1024, 512)).astype(BF)
        return (
            sums[0] + column_sum(du2 * normal),
            sums[1] + column_sum(dz.astype(F32)),
            sums[2] + column_sum(du2),
        )

    nothing = jnp.zeros((1, 512), F32)
    ff_sums = lax.fori_loop(0, 4, finish_hidden, (nothing, nothing, nothing))
    dh2_pairs = ex.sum_pair(B.x_all, B.dh2_pair)
    ff_sums = lax.fori_loop(4, 8, finish_hidden, ff_sums)
    dh2_over = ex.sum_chips(dh2_pairs, B.x_all, B.dh2_pair, B.dh2_paired, B.dh2_chips, B.total)

    @pl.loop(0, 4)
    def _(q):
        terms = contract_rows(B.u2[:, columns(q * 128, 128)], B.g_all[...].reshape(1024, 1024))
        B.down_src[q] = terms.astype(BF)

    down_grads = ex.terms_start(lambda q: B.down_src.at[q], B.down_terms, B.down_passing)

    @pl.loop(0, 8)
    def _(c):
        rows = B.h2_all[:, :, columns(c * 128, 128)].reshape(1024, 128)
        B.up_src[c] = contract_rows(rows, B.dz[...]).astype(BF).reshape(4, 32, 512)

    up_grads = ex.terms_start(lambda q: B.up_src.at[:, q], B.up_terms, B.up_passing)

    @pl.loop(0, 8)
    def _(t):
        B.ffo_src[t] = matmul(B.u2[pl.ds(t * 128, 128), :], B.down_w[...].reshape(512, 1024)).astype(BF)

    ffo_pairs = ex.sum_pair(B.ffo_src, B.ffo_pair)

    dh2 = ex.sum_end(dh2_over, B.dh2_chips, B.total)
    sum_gain_c = column_sum(dh2 * B.normal_c[...])
    sum_shift_c = column_sum(dh2)
    g_local = B.g_all[s].astype(F32)
    dr = g_local + norm_back(dh2, gain_c, B.normal_c[...], inverse_c)
    B.dr[...] = dr
    da = norm_back(dr, gain_b, B.normal_b[...], inverse_b).astype(BF)
    B.da_all[s] = da
    B.do_local[...] = (times_transposed(da, B.out_w[...].reshape(1024, 1024)) * B.scale_row[0:1, :]).astype(BF)
    do_copies = [ex.send(B.do_local.at[:, columns(p * 128, 128)], B.do_all.at[s], p, b) for p in ex.plane()]
    own_do = ex.local(B.do_local.at[:, own_columns], B.do_all.at[s])
    da_slot = lambda i: B.da_all.at[i]
    da_copies = ex.gather_start(B.da_all.at[s], da_slot)
    ex.terms_relay(down_grads, lambda q: B.down_src[q], B.down_joined)
    ex.terms_relay(up_grads, lambda q: B.up_src[:, q], B.up_joined)
    ffo_over = ex.sum_chips(ffo_pairs, B.ffo_src, B.ffo_pair, B.ffo_paired, B.ffo_chips, B.ffo_total)
    sum_gain_b = column_sum(dr * B.normal_b[...])
    sum_shift_b = column_sum(dr)
    sum_g = column_sum(g_local)
    sum_da = column_sum(da.astype(F32))
    B.dk[...] = jnp.zeros((1024, 128), F32)
    B.dv[...] = jnp.zeros((1024, 128), F32)
    ex.arrived(do_copies)
    own_do.wait()

    scale_sums = jnp.zeros((1, 128), F32)
    for size in (512, 1024):
        for h in range(2):

            def back(t, sums, size=size, h=h):
                at = pl.ds(t * 128, 128)
                do = of_head(B.do_all[t], h)
                along = do.astype(F32) * B.attended[at, :]
                delta = jnp.sum(along, axis=-1, keepdims=True)
                kept = B.probs_low if size == 512 else B.probs_high
                probs = kept[h, pl.ds(t * 128 - size + 512, 128), :]
                dp = times_transposed(do, B.qkv[0:size, 256:384])
                ds = (probs * (dp - delta)).astype(BF)
                found = matmul(ds, of_head(B.qkv[0:size, 128:256], h))
                if h == 0:
                    B.dq[at, :] = found
                else:
                    B.dq[at, :] += found
                B.dk[0:size, :] += contract_rows(ds, of_head(B.qkv[at, 0:128], h))
                B.dv[0:size, :] += contract_rows(probs.astype(BF), do)
                return sums + column_sum(along)

            scale_sums = lax.fori_loop(size // 128 - 4, size // 128, back, scale_sums)

    def join(t, sums):
        at = pl.ds(t * 128, 128)
        dq = (B.dq[at, :] * score_scale).astype(BF)
        dk = (B.dk[at, :] * score_scale).astype(BF)
        dv = B.dv[at, :].astype(BF)
        B.dqkv[at, 0:128] = dq
        B.dqkv[at, 128:256] = dk
        B.dqkv[at, 256:384] = dv
        return (sums[0] + column_sum(dq.astype(F32)), sums[1] + column_sum(dv.astype(F32)))

    def dh1_tile(j):
        t = ex.tile(j)
        rows = B.dqkv[pl.ds(t * 128, 128), :]
        B.dh1_src[t] = times_transposed(rows, B.qkv_w[...].reshape(1024, 384)).astype(BF)

    blank = jnp.zeros((1, 128), F32)
    sum_dq, sum_dv = lax.fori_loop(0, 8, join, (blank, blank))
    pl.loop(0, 4)(dh1_tile)
    dh1_pairs = ex.sum_pair(B.dh1_src, B.dh1_pair)

    @pl.loop(0, 8)
    def _(c):
        terms = contract_rows(B.h1[:, columns(c * 128, 128)], B.dqkv[...])
        B.qkv_src[c] = terms.astype(BF).reshape(4, 32, 384)

    qkv_grads = ex.terms_start(lambda q: B.qkv_src.at[:, q], B.qkv_terms, B.qkv_passing)
    pl.loop(4, 8)(dh1_tile)
    dh1_over = ex.sum_chips(dh1_pairs, B.dh1_src, B.dh1_pair, B.dh1_paired, B.dh1_chips, B.total)
    ex.terms_relay(qkv_grads, lambda q: B.qkv_src[:, q], B.qkv_joined)
    da_passed = ex.gather_forward(da_copies, da_slot)
    ffo = ex.sum_end(ffo_over, B.ffo_chips, B.ffo_total)
    output[...] = jnp.where(held, B.residual[...] + ffo + bias_out, 0.0).astype(BF)
    ex.arrived(da_passed)
    terms = contract_rows(B.scaled[...].reshape(1024, 128), B.da_all[...].reshape(1024, 1024))
    B.out_src[...] = terms.astype(BF).reshape(4, 32, 1024)
    out_grads = [ex.send(B.out_src.at[q], B.out_terms.at[b], s, q) for q in ex.line()]

    def line_sum(mine, landed):
        total = mine
        for k in (1, 2, 3):
            total = total + landed[(b + k) % 4].astype(F32)
        return total

    ex.terms_arrived(down_grads)
    grad_down[...] = line_sum(B.down_src[b].astype(F32), B.down_terms)
    ex.terms_arrived(up_grads)
    B.up_own[...] = line_sum(B.up_src[:, b].astype(F32), B.up_terms).astype(BF)
    up_lanes = up_fin.at[s]
    up_copies = [ex.send(B.up_own.at[p], up_lanes, p, b) for p in ex.plane()]
    own_up = ex.local(B.up_own.at[s], up_lanes)

    dh1 = ex.sum_end(dh1_over, B.dh1_chips, B.total)
    normal_a, inverse_a = centred(x_in[...].astype(F32))
    grad_input[...] = (B.dr[...] + norm_back(dh1, gain_a, normal_a, inverse_a)).astype(BF)
    wide = jnp.concatenate(
        [
            column_sum(dh1 * normal_a),
            sum_gain_b,
            sum_gain_c,
            column_sum(dh1),
            sum_shift_b,
            sum_shift_c,
            jnp.zeros((1, 1024), F32),
            sum_g,
            jnp.zeros((1, 1024), F32),
            sum_da,
            jnp.zeros((6, 1024), F32),
        ],
        axis=0,
    )
    by_head = jnp.zeros((1, 128), F32)
    for h in range(2):
        found = jnp.sum(of_head(scale_sums / own_scale, h), axis=-1, keepdims=True)
        by_head = jnp.where(lane == s * 2 + h, found, by_head)
    place = lax.broadcasted_iota(jnp.int32, (16, 128), 0)
    for p in range(8):
        mine = jnp.where(s == p, 1.0, 0.0)
        tile = wide[:, p * 128 : (p + 1) * 128]
        tile = jnp.where(place == 6, sum_dq * mine, tile)
        tile = jnp.where(place == 8, sum_dv * mine, tile)
        B.close_src[p] = jnp.where(place == 10, by_head, tile)
    close = [ex.send(B.close_src.at[p], B.close_plane.at[s], p, b) for p in ex.plane()]
    own_close = ex.local(B.close_src.at[s], B.close_plane.at[s])
    for q in range(4):
        part = [one[:, q * 128 : (q + 1) * 128] for one in ff_sums]
        B.close_line[q, 16:24, :] = jnp.concatenate(part + [jnp.zeros((5, 128), F32)], axis=0)

    ex.terms_arrived(qkv_grads)
    B.qkv_own[...] = line_sum(B.qkv_src[:, b].astype(F32), B.qkv_terms).astype(BF)
    qkv_copies = [ex.send(B.qkv_own.at[p], qkv_fin.at[s], p, b) for p in ex.plane()]
    own_qkv = [ex.local(B.qkv_own.at[s], qkv_fin.at[s])]
    ex.arrived(close)
    own_close.wait()
    total = B.close_plane[0]
    for i in range(1, 8):
        total = total + B.close_plane[i]
    for q in range(4):
        B.close_line[q, 0:16, :] = total
    close = [ex.send(B.close_line.at[q], B.close_all.at[b], s, q) for q in ex.line()]
    own_close = ex.local(B.close_line.at[b], B.close_all.at[b])
    ex.arrived(out_grads)
    grad_out[...] = line_sum(B.out_src[b].astype(F32), B.out_terms)
    ex.arrived(up_copies)
    own_up.wait()
    ex.arrived(close)
    own_close.wait()
    vec_out[...] = B.close_all[0] + B.close_all[1] + B.close_all[2] + B.close_all[3]
    ex.arrived(qkv_copies)
    for one in own_qkv:
        one.wait()
    ex.finish()


def finish_kernel(output, grad_input, qkv, out, up, down, vectors, *outs):
    b = lax.axis_index("batch")
    outs[0][0] = output[...]
    outs[1][0] = grad_input[...]
    for p in range(8):
        for t in range(3):
            at = t * 1024 + p * 128
            outs[2][:, at : at + 128] = qkv[p, :, t * 128 : (t + 1) * 128].astype(F32)
        outs[4][:, p * 512 : (p + 1) * 512] = up[p].astype(F32)
    outs[3][...] = out[...]
    outs[5][...] = down[...]
    rows = vectors[...]
    own = rows[:, 0:32]
    for q in range(1, 4):
        own = jnp.where(b == q, rows[:, q * 32 : (q + 1) * 32], own)
    outs[6][...] = own[0:3]
    outs[7][...] = own[3:8]
    outs[8][...] = own[8:10]
    outs[9][...] = rows[16:17]
    outs[10][...] = rows[17:19]
    outs[11][...] = rows[10:11, :H]


def plane_shards(
    inputs,
    lengths,
    w_qkv,
    w_out,
    w_up,
    w_down,
    norm_gains,
    model_biases,
    attn_biases,
    ff_gain,
    ff_biases,
    head_scale,
    cotangent,
):
    b = lax.axis_index("batch")
    near = pl.BlockSpec(memory_space=pltpu.VMEM)
    outs = [
        ((128, 1024), BF),
        ((128, 1024), BF),
        ((8, 32, 384), BF),
        ((32, 1024), F32),
        ((8, 32, 512), BF),
        ((128, 1024), F32),
        ((24, 128), F32),
    ]
    found = pl.pallas_call(
        block_kernel,
        name="block",
        out_shape=[jax.ShapeDtypeStruct(shape, dtype) for shape, dtype in outs],
        in_specs=[pl.BlockSpec(memory_space=pltpu.SMEM)] + [near] * (INPUTS - 1),
        out_specs=[near] * OUTPUTS,
        scratch_shapes=[pltpu.VMEM(shape, dtype) for shape, dtype in BUFFERS.values()]
        + [
            pltpu.SemaphoreType.DMA((COPIES,)),
            pltpu.SemaphoreType.DMA((COPIES,)),
            pltpu.SemaphoreType.DMA((32,)),
        ],
        compiler_params=pltpu.CompilerParams(
            collective_id=1, has_side_effects=True, vmem_limit_bytes=67043328
        ),
    )(
        lengths.reshape(1, 1),
        inputs[0],
        cotangent[0],
        w_qkv,
        w_out,
        w_up,
        w_down,
        norm_gains,
        model_biases,
        attn_biases,
        ff_gain.reshape(1, 128),
        ff_biases,
        head_scale.reshape(1, H),
    )
    finals = [
        ((1, 128, 1024), BF),
        ((1, 128, 1024), BF),
        ((32, 3072), F32),
        ((32, 1024), F32),
        ((32, 4096), F32),
        ((128, 1024), F32),
        ((3, 32), F32),
        ((5, 32), F32),
        ((2, 32), F32),
        ((1, 128), F32),
        ((2, 128), F32),
        ((1, H), F32),
    ]
    last = pl.pallas_call(
        finish_kernel,
        name="finish",
        out_shape=[jax.ShapeDtypeStruct(shape, dtype) for shape, dtype in finals],
        in_specs=[near] * OUTPUTS,
        out_specs=[near] * len(finals),
        compiler_params=pltpu.CompilerParams(vmem_limit_bytes=67043328),
    )(*found)
    return tuple(last[:9]) + (last[9].reshape(128), last[10], last[11].reshape(H))


def solution(mesh):
    in_plane = mesh.shape["seq"] == 8 and mesh.shape["batch"] == 4
    return jax.shard_map(
        plane_shards if in_plane else shards,
        mesh=mesh,
        in_specs=(
            P("batch", "seq", None),
            P("batch"),
            P(("seq", "batch"), None),
            P(("seq", "batch"), None),
            P(("seq", "batch"), None),
            P(("seq", "batch"), None),
            P(None, ("seq", "batch")),
            P(None, ("seq", "batch")),
            P(None, ("seq", "batch")),
            P(("seq", "batch")),
            P(None, ("seq", "batch")),
            P(),
            P("batch", "seq", None),
        ),
        out_specs=(
            P("batch", "seq", None),
            P("batch", "seq", None),
            P(("seq", "batch"), None),
            P(("seq", "batch"), None),
            P(("seq", "batch"), None),
            P(("seq", "batch"), None),
            P(None, ("seq", "batch")),
            P(None, ("seq", "batch")),
            P(None, ("seq", "batch")),
            P(("seq", "batch")),
            P(None, ("seq", "batch")),
            P(),
        ),
        check_vma=False,
    )
```

```python
import jax
import jax.numpy as jnp
from jax import lax
from jax.experimental import pallas as pl
from jax.experimental.pallas import tpu as pltpu
from jax.sharding import PartitionSpec as P

H = 16
HD = 64


NORM_EPSILON = 1e-05


def layer_norm(vector, norm_gain, norm_bias):
    centered = vector - jnp.mean(vector, axis=-1, keepdims=True)
    spread = jnp.mean(centered * centered, axis=-1, keepdims=True)
    return centered * lax.rsqrt(spread + NORM_EPSILON) * norm_gain + norm_bias


def gelu_norm(hidden, norm_gain, norm_bias):
    return layer_norm(jax.nn.gelu(hidden, approximate=False), norm_gain, norm_bias)


def contract_rows(left, right):
    return lax.dot_general(
        left, right, (((0,), (0,)), ((), ())), preferred_element_type=jnp.float32
    )


def times_transposed(left, right):
    return lax.dot_general(
        left, right, (((1,), (1,)), ((), ())), preferred_element_type=jnp.float32
    )


def shards(
    inputs,
    lengths,
    w_qkv,
    w_out,
    w_up,
    w_down,
    norm_gains,
    model_biases,
    attn_biases,
    ff_gain,
    ff_biases,
    head_scale,
    cotangent,
):
    gathered = (
        lax.all_gather(w_qkv, ("seq", "batch"), axis=0, tiled=True),
        lax.all_gather(w_out, ("seq", "batch"), axis=0, tiled=True),
        lax.all_gather(w_up, ("seq", "batch"), axis=0, tiled=True),
        lax.all_gather(w_down, ("seq", "batch"), axis=0, tiled=True),
        lax.all_gather(norm_gains, ("seq", "batch"), axis=1, tiled=True),
        lax.all_gather(model_biases, ("seq", "batch"), axis=1, tiled=True),
        lax.all_gather(attn_biases, ("seq", "batch"), axis=1, tiled=True),
        lax.all_gather(ff_gain, ("seq", "batch"), axis=0, tiled=True),
        lax.all_gather(ff_biases, ("seq", "batch"), axis=1, tiled=True),
    )
    qkv_full, out_full, up_full, down_full = (gathered[0], gathered[1], gathered[2], gathered[3])
    gain_rows = gathered[4].astype(jnp.float32)
    bias_rows = gathered[5].astype(jnp.float32)
    attn_rows = gathered[6].astype(jnp.float32)
    ffn_gain = gathered[7].astype(jnp.float32)
    ffn_rows = gathered[8].astype(jnp.float32)
    scales = head_scale.astype(jnp.float32)
    local_rows = inputs.shape[1]
    model_width = inputs.shape[2]
    seq_length = local_rows * lax.axis_size("seq")
    tile_rows = min(512, seq_length)
    first_row = lax.axis_index("seq") * local_rows
    valid_rows = lengths[0]
    positions = first_row + jnp.arange(local_rows, dtype=jnp.int32)
    valid_mask = (positions < valid_rows)[:, None]
    score_scale = HD ** (-0.5)
    residual_in = inputs[0].astype(jnp.float32)
    normed, norm_a_pull = jax.vjp(layer_norm, residual_in, gain_rows[0], bias_rows[0])
    normed_low = normed.astype(jnp.bfloat16)
    offsets = jnp.concatenate([bias_rows[3], jnp.zeros_like(bias_rows[3]), attn_rows[0]])
    projected = (
        jnp.dot(normed_low, qkv_full, preferred_element_type=jnp.float32) + offsets
    ).astype(jnp.bfloat16)
    queries = projected[:, :model_width]
    key_local = projected[:, model_width : 2 * model_width]
    value_local = projected[:, 2 * model_width :]
    key_rows, value_rows = (
        lax.all_gather(key_local, "seq", axis=0, tiled=True),
        lax.all_gather(value_local, "seq", axis=0, tiled=True),
    )
    query_heads = queries.reshape(local_rows, H, HD)
    last_needed = jnp.minimum(first_row + local_rows - 1, valid_rows - 1)
    tile_count = last_needed // tile_rows + 1

    def tile_scores(j):
        start = j * tile_rows
        key_tile = lax.dynamic_slice_in_dim(key_rows, start, tile_rows, 0).reshape(tile_rows, H, HD)
        scores = (
            jnp.einsum("qhd,khd->hqk", query_heads, key_tile, preferred_element_type=jnp.float32)
            * score_scale
        )
        key_index = start + jnp.arange(tile_rows, dtype=jnp.int32)
        allowed = (key_index[None, :] <= positions[:, None]) & (key_index[None, :] < valid_rows)
        return (scores, allowed[None], key_tile)

    def max_and_sum(j, carry):
        running_max, running_sum = carry
        scores, allowed, unused_tile = tile_scores(j)
        masked = jnp.where(allowed, scores, -1e30)
        new_max = jnp.maximum(running_max, jnp.max(masked, axis=-1))
        kept_terms = jnp.where(allowed, jnp.exp(masked - new_max[..., None]), 0.0)
        return (
            new_max,
            running_sum * jnp.exp(running_max - new_max) + jnp.sum(kept_terms, axis=-1),
        )

    start_stats = (
        jnp.full((H, local_rows), -1e30, jnp.float32),
        jnp.zeros((H, local_rows), jnp.float32),
    )
    running_max, running_sum = lax.fori_loop(0, tile_count, max_and_sum, start_stats)
    log_total = running_max + jnp.log(running_sum)

    def tile_probs(j):
        scores, allowed, key_tile = tile_scores(j)
        attn_probs = jnp.where(allowed, jnp.exp(scores - log_total[..., None]), 0.0)
        value_tile = lax.dynamic_slice_in_dim(value_rows, j * tile_rows, tile_rows, 0).reshape(
            tile_rows, H, HD
        )
        return (attn_probs, key_tile, value_tile)

    def accumulate(j, summed):
        attn_probs, unused_tile, value_tile = tile_probs(j)
        return summed + jnp.einsum(
            "hqk,khd->qhd",
            attn_probs.astype(jnp.bfloat16),
            value_tile,
            preferred_element_type=jnp.float32,
        )

    attended = lax.fori_loop(0, tile_count, accumulate, jnp.zeros((local_rows, H, HD), jnp.float32))
    scaled_low = (
        (attended * scales[None, :, None]).reshape(local_rows, model_width).astype(jnp.bfloat16)
    )
    attn_proj = jnp.dot(scaled_low, out_full, preferred_element_type=jnp.float32) + attn_rows[1]
    attn_normed, norm_b_pull = jax.vjp(layer_norm, attn_proj, gain_rows[1], bias_rows[1])
    residual = residual_in + attn_normed
    ffn_in, norm_c_pull = jax.vjp(layer_norm, residual, gain_rows[2], bias_rows[2])
    ffn_low = ffn_in.astype(jnp.bfloat16)
    hidden = jnp.dot(ffn_low, up_full, preferred_element_type=jnp.float32) + ffn_rows[0]
    ffn_normed, ffn_pull = jax.vjp(gelu_norm, hidden, ffn_gain, ffn_rows[1])
    ffn_out_low = ffn_normed.astype(jnp.bfloat16)
    combined = jnp.where(
        valid_mask,
        residual
        + jnp.dot(ffn_out_low, down_full, preferred_element_type=jnp.float32)
        + bias_rows[4],
        0.0,
    )
    output = combined.astype(jnp.bfloat16)[None]
    barrier_out = lax.optimization_barrier(((w_qkv, w_out, w_up, w_down), combined))
    regathered = (
        lax.all_gather(barrier_out[0][0], ("seq", "batch"), axis=0, tiled=True),
        lax.all_gather(barrier_out[0][1], ("seq", "batch"), axis=0, tiled=True),
        lax.all_gather(barrier_out[0][2], ("seq", "batch"), axis=0, tiled=True),
        lax.all_gather(barrier_out[0][3], ("seq", "batch"), axis=0, tiled=True),
    )
    qkv_full, out_full, up_full, down_full = (
        regathered[0],
        regathered[1],
        regathered[2],
        regathered[3],
    )
    cotan_rows = jnp.where(valid_mask, cotangent[0], jnp.zeros_like(cotangent[0]))
    cotan_float = cotan_rows.astype(jnp.float32)
    grad_down = contract_rows(ffn_out_low, cotan_rows)
    grad_bias_out = jnp.sum(cotan_float, axis=0)
    grad_ffn_normed = times_transposed(cotan_rows, down_full)
    grad_hidden, grad_ffn_gain, grad_ffn_shift = ffn_pull(grad_ffn_normed)
    grad_hidden_low = grad_hidden.astype(jnp.bfloat16)
    grad_up = contract_rows(ffn_low, grad_hidden_low)
    grad_ffn_bias = jnp.sum(grad_hidden_low.astype(jnp.float32), axis=0)
    grad_ffn_in = times_transposed(grad_hidden_low, up_full)
    grad_from_ffn, grad_gain_c, grad_shift_c = norm_c_pull(grad_ffn_in)
    grad_residual = cotan_float + grad_from_ffn
    grad_proj, grad_gain_b, grad_shift_b = norm_b_pull(grad_residual)
    grad_proj_low = grad_proj.astype(jnp.bfloat16)
    grad_out_bias = jnp.sum(grad_proj_low.astype(jnp.float32), axis=0)
    grad_out = contract_rows(scaled_low, grad_proj_low)
    grad_scaled = times_transposed(grad_proj_low, out_full).reshape(local_rows, H, HD)
    grad_scales = jnp.sum(grad_scaled * attended, axis=(0, 2))
    grad_heads_low = (grad_scaled * scales[None, :, None]).astype(jnp.bfloat16)
    row_delta = jnp.einsum("qhd,qhd->hq", grad_heads_low.astype(jnp.float32), attended)

    def score_grads(j):
        attn_probs, key_tile, value_tile = tile_probs(j)
        grad_probs = jnp.einsum(
            "qhd,khd->hqk", grad_heads_low, value_tile, preferred_element_type=jnp.float32
        )
        grad_scores = (attn_probs * (grad_probs - row_delta[..., None])).astype(jnp.bfloat16)
        return (attn_probs, grad_scores, key_tile)

    def backward_tile(j, carry):
        grad_query, terms = carry
        attn_probs, grad_scores, key_tile = score_grads(j)
        grad_query = grad_query + jnp.einsum(
            "hqk,khd->qhd", grad_scores, key_tile, preferred_element_type=jnp.float32
        )
        grad_key = (
            jnp.einsum("hqk,qhd->khd", grad_scores, query_heads, preferred_element_type=jnp.float32)
            * score_scale
        )
        grad_value = jnp.einsum(
            "hqk,qhd->khd",
            attn_probs.astype(jnp.bfloat16),
            grad_heads_low,
            preferred_element_type=jnp.float32,
        )
        piece = jnp.concatenate(
            [grad_key.reshape(tile_rows, model_width), grad_value.reshape(tile_rows, model_width)],
            axis=1,
        )
        return (grad_query, lax.dynamic_update_slice_in_dim(terms, piece, j * tile_rows, 0))

    start_carry = (
        jnp.zeros((local_rows, H, HD), jnp.float32),
        jnp.zeros((seq_length, 2 * model_width), jnp.float32),
    )
    grad_query, terms = lax.fori_loop(0, tile_count, backward_tile, start_carry)
    grad_kv = lax.psum_scatter(terms, "seq", scatter_dimension=0, tiled=True)
    grad_query_low = (
        (grad_query * score_scale).reshape(local_rows, model_width).astype(jnp.bfloat16)
    )
    grad_kv_low = grad_kv.astype(jnp.bfloat16)
    grad_projected = jnp.concatenate([grad_query_low, grad_kv_low], axis=1)
    grad_qkv = contract_rows(normed_low, grad_projected)
    grad_query_bias = jnp.sum(grad_query_low.astype(jnp.float32), axis=0)
    grad_value_bias = jnp.sum(grad_kv_low[:, model_width:].astype(jnp.float32), axis=0)
    grad_normed = times_transposed(grad_projected, qkv_full)
    grad_from_attn, grad_gain_a, grad_shift_a = norm_a_pull(grad_normed)
    grad_input = (grad_residual + grad_from_attn).astype(jnp.bfloat16)[None]
    reduced = (
        lax.psum_scatter(grad_qkv, ("seq", "batch"), scatter_dimension=0, tiled=True),
        lax.psum_scatter(grad_out, ("seq", "batch"), scatter_dimension=0, tiled=True),
        lax.psum_scatter(grad_up, ("seq", "batch"), scatter_dimension=0, tiled=True),
        lax.psum_scatter(grad_down, ("seq", "batch"), scatter_dimension=0, tiled=True),
        lax.psum_scatter(
            jnp.stack([grad_gain_a, grad_gain_b, grad_gain_c]),
            ("seq", "batch"),
            scatter_dimension=1,
            tiled=True,
        ),
        lax.psum_scatter(
            jnp.stack([grad_shift_a, grad_shift_b, grad_shift_c, grad_query_bias, grad_bias_out]),
            ("seq", "batch"),
            scatter_dimension=1,
            tiled=True,
        ),
        lax.psum_scatter(
            jnp.stack([grad_value_bias, grad_out_bias]),
            ("seq", "batch"),
            scatter_dimension=1,
            tiled=True,
        ),
        lax.psum_scatter(grad_ffn_gain, ("seq", "batch"), scatter_dimension=0, tiled=True),
        lax.psum_scatter(
            jnp.stack([grad_ffn_bias, grad_ffn_shift]),
            ("seq", "batch"),
            scatter_dimension=1,
            tiled=True,
        ),
    )
    scale_total = lax.psum(grad_scales, ("seq", "batch"))
    return (
        output,
        grad_input,
        reduced[0],
        reduced[1],
        reduced[2],
        reduced[3],
        reduced[4],
        reduced[5],
        reduced[6],
        reduced[7],
        reduced[8],
        scale_total,
    )


BF = jnp.bfloat16
F32 = jnp.float32


class Exchange:
    def __init__(self, send_sems, recv_sems, local_sems):
        self.send_sems = send_sems
        self.recv_sems = recv_sems
        self.local_sems = local_sems
        self.count = 0
        self.locals = 0
        self.sent = []
        self.sent_if = []
        self.s = lax.axis_index("seq")
        self.b = lax.axis_index("batch")
        self.chip = self.s // 2
        self.core = self.s % 2
        self.sibling = self.chip * 2 + 1 - self.core
        self.plane_peers = [(self.s + j) % 8 for j in range(1, 8)]
        self.line_peers = [(self.b + k) % 4 for k in range(1, 4)]

    def send(self, src, dst, seq, batch):
        at = self.count
        self.count += 1
        copy = pltpu.make_async_remote_copy(
            src_ref=src,
            dst_ref=dst,
            send_sem=self.send_sems.at[at],
            recv_sem=self.recv_sems.at[at],
            device_id=(seq, batch),
            device_id_type=pl.DeviceIdType.MESH,
        )
        copy.start()
        self.sent.append(copy)
        return copy

    def describe(self, src, dst, seq, batch, sent_at, recv_at):
        return pltpu.make_async_remote_copy(
            src_ref=src,
            dst_ref=dst,
            send_sem=self.send_sems.at[sent_at],
            recv_sem=self.recv_sems.at[recv_at],
            device_id=(seq, batch),
            device_id_type=pl.DeviceIdType.MESH,
        )

    def send_if(self, held, copy):
        @pl.when(held)
        def _():
            copy.start()

        self.sent_if.append((held, copy))

    def line_start(self, src, slot):
        first = self.count
        self.count += 4
        b = self.b
        copies = [
            self.describe(src, slot(b), self.s, (b + k) % 4, first + k - 1, first + k - 1) for k in (1, 2, 3)
        ]
        copies[1].start()
        self.sent.append(copies[1])
        return copies, slot, first

    def line_near(self, line):
        copies = line[0]
        self.send_if(self.b != 3, copies[0])
        self.send_if(self.b != 0, copies[2])

    def line_relay(self, line):
        copies, slot, first = line
        b = self.b

        @pl.when((b == 1) | (b == 2))
        def _():
            copies[1].wait_recv()

        came = slot((b + 2) % 4)
        self.send_if(b == 1, self.describe(came, came, self.s, 0, first + 3, first))
        self.send_if(b == 2, self.describe(came, came, self.s, 3, first + 3, first + 2))

    def line_arrived(self, line):
        copies, _slot, _first = line
        copies[0].wait_recv()
        copies[2].wait_recv()

        @pl.when((self.b == 0) | (self.b == 3))
        def _():
            copies[1].wait_recv()

    def terms_start(self, view, landed, passing):
        first = self.count
        self.count += 4
        b = self.b
        at = lambda q, k: self.describe(view(q), landed.at[b], self.s, q, first + k - 1, first + k - 1)
        up, over, down = at((b + 1) % 4, 1), at((b + 2) % 4, 2), at((b + 3) % 4, 3)
        to_one = self.describe(view(3), passing, self.s, 1, first + 3, first + 3)
        to_two = self.describe(view(0), passing, self.s, 2, first + 3, first + 3)
        self.send_if(b == 0, to_one)
        self.send_if(b == 3, to_two)
        self.send_if((b == 0) | (b == 3), over)
        self.send_if(b != 3, up)
        self.send_if(b != 0, down)
        return up, over, down, to_one, landed, passing, first

    def terms_relay(self, terms, mine, joined):
        up, over, down, to_one, landed, passing, first = terms
        b = self.b
        held = (b == 1) | (b == 2)

        @pl.when(held)
        def _():
            to_one.wait_recv()
            joined[...] = (mine((b + 2) % 4).astype(F32) + passing[...].astype(F32)).astype(BF)

        self.send_if(
            held, self.describe(joined, landed.at[b], self.s, (b + 2) % 4, first + 1, first + 1)
        )

    def terms_arrived(self, terms):
        up, over, down = terms[:3]
        over.wait_recv()

        @pl.when(self.b != 0)
        def _():
            up.wait_recv()

        @pl.when(self.b != 3)
        def _():
            down.wait_recv()

    def local(self, src, dst):
        at = self.locals
        self.locals += 1
        copy = pltpu.make_async_copy(src, dst, self.local_sems.at[at])
        copy.start()
        return copy

    def arrived(self, copies):
        for copy in copies:
            copy.wait_recv()

    def finish(self):
        for copy in self.sent:
            copy.wait_send()
        for held, copy in self.sent_if:
            pl.when(held)(copy.wait_send)

    def peer(self, k):
        return ((self.chip + k) % 4) * 2 + self.core

    def source(self, k):
        return ((self.chip + 4 - k) % 4) * 2 + self.core

    def chip_source(self, k):
        return (self.chip + 4 - k) % 4

    def tile(self, j):
        return (self.chip + j + 1) % 4 * 2 + jnp.where(j < 4, 1 - self.core, self.core)

    def plane(self):
        return self.plane_peers

    def line(self):
        return self.line_peers

    def gather_start(self, src, slot):
        copies = [self.send(src, slot(self.s), self.peer(k), self.b) for k in (1, 2, 3)]
        copies.append(self.send(src, slot(self.s), self.sibling, self.b))
        return copies

    def gather_forward(self, copies, slot):
        passed = []
        for k in (1, 2, 3):
            copies[k - 1].wait_recv()
            came = slot(self.source(k))
            passed.append(self.send(came, came, self.sibling, self.b))
        return [copies[3]] + passed

    def sum_pair(self, src, from_pair):
        return [
            self.send(src.at[((self.chip + k) % 4) * 2 + 1 - self.core], from_pair.at[k], self.sibling, self.b)
            for k in (1, 2, 3, 0)
        ]

    def sum_chips(self, copies, src, from_pair, paired, from_chips, total):
        over = []
        for at, k in enumerate((1, 2, 3, 0)):
            copies[at].wait_recv()
            mine = src[((self.chip + k) % 4) * 2 + self.core].astype(F32)
            both = mine + from_pair[k].astype(F32)
            if k:
                paired[k - 1] = both.astype(BF)
                over.append(self.send(paired.at[k - 1], from_chips.at[k - 1], self.peer(k), self.b))
            else:
                total[...] = both
        return over

    def sum_end(self, over, from_chips, total):
        self.arrived(over)
        return total[...] + from_chips[0].astype(F32) + from_chips[1].astype(F32) + from_chips[2].astype(F32)


def columns(start, size):
    return pl.ds(pl.multiple_of(start, 128), size)


def centred(rows):
    middle = rows - jnp.mean(rows, axis=-1, keepdims=True)
    inverse = lax.rsqrt(jnp.mean(middle * middle, axis=-1, keepdims=True) + NORM_EPSILON)
    return middle * inverse, inverse


def norm_back(upstream, gain, normal, inverse):
    scaled = upstream * gain
    average = jnp.mean(scaled, axis=-1, keepdims=True)
    along = jnp.mean(scaled * normal, axis=-1, keepdims=True)
    return inverse * (scaled - average - normal * along)


def gelu_parts(z):
    phi = 0.5 * (1.0 + lax.erf(z * 0.7071067811865476))
    density = 0.3989422804014327 * jnp.exp(-0.5 * z * z)
    return z * phi, phi + z * density


def matmul(left, right):
    return jnp.dot(left, right, preferred_element_type=F32)


def column_sum(rows):
    return jnp.sum(rows, axis=0, keepdims=True)


def pack_columns(parts):
    lane = lax.broadcasted_iota(jnp.int32, (128, 128), 1)
    wide = jnp.zeros((128, 128), F32)
    for at, part in enumerate(parts):
        wide = jnp.where(lane == at, part, wide)
    return wide.T[:8]


BUFFERS = dict(
    x_all=((8, 128, 1024), BF),
    g_all=((8, 128, 1024), BF),
    qkv_w=((8, 4, 32, 384), BF),
    out_w=((8, 4, 32, 1024), BF),
    up_w=((8, 4, 32, 512), BF),
    down_w=((4, 128, 1024), BF),
    vec_src=((16, 128), F32),
    vec_all=((8, 4, 16, 128), F32),
    qkv_send=((8, 32, 384), BF),
    scale_row=((8, 1024), F32),
    rows=((16, 1024), F32),
    ff_rows=((8, 512), F32),
    h1=((1024, 1024), BF),
    qkv=((1024, 384), BF),
    probs_low=((2, 512, 512), F32),
    probs_high=((2, 512, 1024), F32),
    attended=((1024, 128), F32),
    scaled=((8, 128, 128), BF),
    scaled_local=((128, 1024), BF),
    normal_b=((128, 1024), F32),
    normal_c=((128, 1024), F32),
    residual=((128, 1024), F32),
    h2_all=((8, 128, 1024), BF),
    active=((1024, 512), F32),
    slope=((1024, 512), F32),
    du2=((1024, 512), F32),
    stats=((8, 8, 128), F32),
    stats_all=((8, 8, 8, 128), F32),
    u2=((1024, 512), BF),
    dz=((1024, 512), BF),
    dh2_pair=((4, 128, 1024), BF),
    dh2_paired=((3, 128, 1024), BF),
    dh2_chips=((3, 128, 1024), BF),
    ffo_src=((8, 128, 1024), BF),
    ffo_pair=((4, 128, 1024), BF),
    ffo_paired=((3, 128, 1024), BF),
    ffo_chips=((3, 128, 1024), BF),
    dh1_src=((8, 128, 1024), BF),
    dh1_pair=((4, 128, 1024), BF),
    dh1_paired=((3, 128, 1024), BF),
    dh1_chips=((3, 128, 1024), BF),
    total=((128, 1024), F32),
    ffo_total=((128, 1024), F32),
    dr=((128, 1024), F32),
    da_all=((8, 128, 1024), BF),
    do_local=((128, 1024), BF),
    do_all=((8, 128, 128), BF),
    dq=((1024, 128), F32),
    dk=((1024, 128), F32),
    dv=((1024, 128), F32),
    dqkv=((1024, 384), BF),
    up_src=((8, 4, 32, 512), BF),
    up_terms=((4, 8, 32, 512), BF),
    down_src=((4, 128, 1024), BF),
    down_terms=((4, 128, 1024), BF),
    qkv_src=((8, 4, 32, 384), BF),
    qkv_terms=((4, 8, 32, 384), BF),
    up_passing=((8, 32, 512), BF),
    up_joined=((8, 32, 512), BF),
    down_passing=((128, 1024), BF),
    down_joined=((128, 1024), BF),
    qkv_passing=((8, 32, 384), BF),
    qkv_joined=((8, 32, 384), BF),
    out_src=((4, 32, 1024), BF),
    out_terms=((4, 32, 1024), BF),
    up_own=((8, 32, 512), BF),
    qkv_own=((8, 32, 384), BF),
    close_src=((8, 16, 128), F32),
    close_plane=((8, 16, 128), F32),
    close_line=((4, 24, 128), F32),
    close_all=((4, 24, 128), F32),
)
COPIES = 240
INPUTS = 13
OUTPUTS = 7


def block_kernel(
    length_in,
    x_in,
    g_in,
    qkv_in,
    out_in,
    up_in,
    down_in,
    gains_in,
    biases_in,
    attn_in,
    ff_gain_in,
    ff_bias_in,
    scale_in,
    *refs,
):
    output, grad_input, qkv_fin, grad_out, up_fin, grad_down, vec_out = refs[:OUTPUTS]
    B = type("Buffers", (), dict(zip(BUFFERS, refs[OUTPUTS : OUTPUTS + len(BUFFERS)])))
    ex = Exchange(*refs[OUTPUTS + len(BUFFERS) :])
    s, b = ex.s, ex.b
    valid_rows = length_in[0, 0]

    lane = lax.broadcasted_iota(jnp.int32, (1, 128), 1)

    def spread(part):
        values = part[...].astype(F32)
        return jnp.where(lane // 32 == b, jnp.concatenate([values] * 4, axis=1), 0.0)

    B.vec_src[0:3, :] = spread(gains_in)
    B.vec_src[3:8, :] = spread(biases_in)
    B.vec_src[8:10, :] = spread(attn_in)
    B.vec_src[10:11, :] = ff_gain_in[...].astype(F32)
    B.vec_src[11:13, :] = ff_bias_in[...].astype(F32)
    B.vec_src[13:16, :] = jnp.zeros((3, 128), F32)
    held = s * 128 + lax.broadcasted_iota(jnp.int32, (128, 1), 0) < valid_rows
    B.g_all[s] = jnp.where(held, g_in[...].astype(F32), 0.0).astype(BF)
    by_head = lax.broadcasted_iota(jnp.int32, (8, 1024), 1) // HD
    head_scales = scale_in[...].astype(F32)
    scale_row = jnp.zeros((8, 1024), F32)
    for h in range(H):
        scale_row = jnp.where(by_head == h, head_scales[0:1, h : h + 1], scale_row)
    B.scale_row[...] = scale_row

    for p in range(8):
        for t in range(3):
            B.qkv_send[p, :, t * 128 : (t + 1) * 128] = qkv_in[:, t * 1024 + p * 128 : t * 1024 + (p + 1) * 128]

    for landed in (B.up_terms, B.down_terms, B.qkv_terms):

        @pl.when(b == 3)
        def _():
            landed[0] = jnp.zeros(landed.shape[1:], BF)

        @pl.when(b == 0)
        def _():
            landed[3] = jnp.zeros(landed.shape[1:], BF)

    barrier = pltpu.get_barrier_semaphore()
    partners = [(p, b) for p in ex.plane()] + [(s, q) for q in ex.line()]
    for seq, batch in partners:
        pl.semaphore_signal(barrier, inc=1, device_id=(seq, batch), device_id_type=pl.DeviceIdType.MESH)
    pl.semaphore_wait(barrier, len(partners))

    qkv_copies = [ex.send(B.qkv_send.at[p], B.qkv_w.at[s, b], p, b) for p in ex.plane()]
    out_line = ex.line_start(out_in, lambda i: B.out_w.at[s, i])
    ex.line_near(out_line)
    own = [ex.local(B.qkv_send.at[s], B.qkv_w.at[s, b])]
    own_up = ex.local(up_in.at[:, columns(s * 512, 512)], B.up_w.at[s, b])
    own_rest = [
        ex.local(out_in, B.out_w.at[s, b]),
        ex.local(x_in, B.x_all.at[s]),
        ex.local(down_in, B.down_w.at[b]),
        ex.local(B.vec_src, B.vec_all.at[s, b]),
    ]
    x_slot = lambda i: B.x_all.at[i]
    g_slot = lambda i: B.g_all.at[i]
    x_copies = ex.gather_start(x_in, x_slot)
    vec_line = [ex.send(B.vec_src, B.vec_all.at[s, b], s, q) for q in ex.line()]
    up_copies = [ex.send(up_in.at[:, columns(p * 512, 512)], B.up_w.at[s, b], p, b) for p in ex.plane()]
    ex.arrived(qkv_copies)
    for one in own:
        one.wait()
    qkv_line = ex.line_start(B.qkv_w.at[:, b], lambda i: B.qkv_w.at[:, i])
    ex.line_near(qkv_line)
    for one in own_rest:
        one.wait()
    ex.arrived(vec_line)
    vec_slot = lambda i: B.vec_all.at[i]
    vec_copies = ex.gather_start(B.vec_all.at[s], vec_slot)
    ex.line_relay(out_line)
    ex.line_relay(qkv_line)
    down_line = ex.line_start(down_in, lambda i: B.down_w.at[i])
    ex.line_near(down_line)
    x_passed = ex.gather_forward(x_copies, x_slot)
    ex.arrived(up_copies)
    own_up.wait()
    up_line = ex.line_start(B.up_w.at[:, b], lambda i: B.up_w.at[:, i])
    ex.line_near(up_line)
    ex.line_arrived(out_line)
    out_slot = lambda i: B.out_w.at[i]
    out_copies = ex.gather_start(B.out_w.at[s], out_slot)
    g_copies = ex.gather_start(B.g_all.at[s], g_slot)
    ex.arrived(ex.gather_forward(vec_copies, vec_slot))

    for p in range(8):
        group = B.vec_all[p, 0] + B.vec_all[p, 1] + B.vec_all[p, 2] + B.vec_all[p, 3]
        B.rows[:, p * 128 : (p + 1) * 128] = group
    for q in range(4):
        B.ff_rows[:, q * 128 : (q + 1) * 128] = B.vec_all[s, q][8:16]
    row = lambda at: B.rows[at : at + 1, :]
    gain_a, gain_b, gain_c = row(0), row(1), row(2)
    bias_a, bias_b, bias_c, bias_out, bias_attn = row(3), row(4), row(5), row(7), row(9)
    ffn_gain, ffn_bias, ffn_shift = B.ff_rows[2:3, :], B.ff_rows[3:4, :], B.ff_rows[4:5, :]
    own_columns = columns(s * 128, 128)
    query_bias = B.rows[6:7, own_columns]
    value_bias = B.rows[8:9, own_columns]
    own_scale = B.scale_row[0:1, own_columns]

    ex.arrived(x_passed)

    @pl.loop(0, 8)
    def _(t):
        normal, _unused = centred(B.x_all[t].astype(F32))
        B.h1[pl.ds(t * 128, 128), :] = (normal * gain_a + bias_a).astype(BF)

    ex.line_arrived(qkv_line)
    offsets = jnp.concatenate([query_bias, jnp.zeros_like(query_bias), value_bias], axis=1)

    @pl.loop(0, 4)
    def _(t):
        at = pl.ds(t * 256, 256)
        B.qkv[at, :] = (matmul(B.h1[at, :], B.qkv_w[...].reshape(1024, 384)) + offsets).astype(BF)

    ex.line_relay(down_line)
    out_passed = ex.gather_forward(out_copies, out_slot)

    score_scale = HD ** (-0.5)
    half_of = lax.broadcasted_iota(jnp.int32, (1, 128), 1) // HD

    def of_head(rows, h):
        return jnp.where(half_of == h, rows, jnp.zeros_like(rows))

    for size in (256, 512, 768, 1024):
        if size == 768:
            ex.line_relay(up_line)
        for h in range(2):

            @pl.loop(size // 128 - 2, size // 128)
            def _(t):
                at = pl.ds(t * 128, 128)
                query = of_head(B.qkv[at, 0:128], h).astype(F32) * score_scale
                scores = times_transposed(query.astype(BF), B.qkv[0:size, 128:256])
                key_index = lax.broadcasted_iota(jnp.int32, (128, size), 1)
                query_index = t * 128 + lax.broadcasted_iota(jnp.int32, (128, 1), 0)
                masked = jnp.where(key_index <= jnp.minimum(query_index, valid_rows - 1), scores, -1e30)
                raised = jnp.exp(masked - jnp.max(masked, axis=-1, keepdims=True))
                probs = raised * (1.0 / jnp.sum(raised, axis=-1, keepdims=True))
                kept, first = (B.probs_low, 0) if size <= 512 else (B.probs_high, 512)
                kept[h, pl.ds(t * 128 - first, 128), 0:size] = probs
                found = matmul(probs.astype(BF), of_head(B.qkv[0:size, 256:384], h))
                if h == 0:
                    B.attended[at, :] = found
                else:
                    both = B.attended[at, :] + found
                    B.attended[at, :] = both
                    B.scaled[t] = (both * own_scale).astype(BF)

    local_lanes = B.scaled_local.at[:, own_columns]
    heads = [ex.send(B.scaled.at[p], local_lanes, p, b) for p in ex.plane()]
    own_heads = ex.local(B.scaled.at[s], local_lanes)
    g_passed = ex.gather_forward(g_copies, g_slot)
    ex.arrived(out_passed)
    ex.arrived(heads)
    own_heads.wait()

    attn_proj = matmul(B.scaled_local[...], B.out_w[...].reshape(1024, 1024)) + bias_attn
    normal_b, inverse_b = centred(attn_proj)
    B.normal_b[...] = normal_b
    residual = x_in[...].astype(F32) + normal_b * gain_b + bias_b
    B.residual[...] = residual
    normal_c, inverse_c = centred(residual)
    B.normal_c[...] = normal_c
    B.h2_all[s] = (normal_c * gain_c + bias_c).astype(BF)
    h2_slot = lambda i: B.h2_all.at[i]
    h2_copies = ex.gather_start(B.h2_all.at[s], h2_slot)

    ex.arrived(g_passed)
    ex.line_arrived(down_line)
    ex.line_arrived(up_line)

    def upstream(t):
        B.du2[pl.ds(t * 128, 128), :] = times_transposed(B.g_all[t], B.down_w[...].reshape(512, 1024))

    def hidden_tile(t):
        at = pl.ds(t * 128, 128)
        active, slope = gelu_parts(matmul(B.h2_all[t], B.up_w[...].reshape(1024, 512)) + ffn_bias)
        B.active[at, :] = active
        B.slope[at, :] = slope
        dgain = B.du2[at, :] * ffn_gain
        mean = jnp.mean(active, axis=-1, keepdims=True)
        off = active - mean
        add = lambda rows: jnp.sum(rows, axis=-1, keepdims=True)
        B.stats[t] = pack_columns([mean, add(off * off), add(dgain), add(dgain * off)])

    pl.loop(0, 8)(upstream)
    hidden_tile(s)
    h2_copies[3].wait_recv()
    hidden_tile(ex.sibling)
    h2_passed = []
    for k in (1, 3, 2):
        h2_copies[k - 1].wait_recv()
        came = h2_slot(ex.source(k))
        h2_passed.append(ex.send(came, came, ex.sibling, b))
        hidden_tile(ex.source(k))
    for at, k in enumerate((1, 3, 2)):
        h2_passed[at].wait_recv()
        hidden_tile(ex.chip_source(k) * 2 + 1 - ex.core)

    stats_copies = [ex.send(B.stats, B.stats_all.at[s], p, b) for p in ex.plane()]
    own_stats = ex.local(B.stats, B.stats_all.at[s])
    ex.arrived(stats_copies)
    own_stats.wait()

    for copy in x_passed[1:]:
        copy.wait_send()
        ex.sent = [one for one in ex.sent if one is not copy]

    def finish_hidden(j, sums):
        t = ex.tile(j)
        at = pl.ds(t * 128, 128)
        means = [B.stats_all[i, t, 0:1, :] for i in range(8)]
        squares = [B.stats_all[i, t, 1:2, :] for i in range(8)]
        firsts = [B.stats_all[i, t, 2:3, :] for i in range(8)]
        seconds = [B.stats_all[i, t, 3:4, :] for i in range(8)]
        mean = sum(means) * 0.125
        shifts = [one - mean for one in means]
        spread = (sum(squares) + 512.0 * sum(one * one for one in shifts)) * (1.0 / 4096.0)
        inverse = lax.rsqrt(spread + NORM_EPSILON)
        average = sum(firsts) * (1.0 / 4096.0)
        along = inverse * sum(two + one * first for two, one, first in zip(seconds, shifts, firsts)) * (1.0 / 4096.0)
        packed = jnp.concatenate([mean, inverse, average, along, jnp.zeros((124, 128), F32)], axis=0).T
        mean, inverse, average, along = (packed[:, i : i + 1] for i in range(4))
        normal = (B.active[at, :] - mean) * inverse
        B.u2[at, :] = (normal * ffn_gain + ffn_shift).astype(BF)
        du2 = B.du2[at, :]
        dz = (inverse * (du2 * ffn_gain - average - normal * along) * B.slope[at, :]).astype(BF)
        B.dz[at, :] = dz
        B.x_all[t] = times_transposed(dz, B.up_w[...].reshape(1024, 512)).astype(BF)
        return (
            sums[0] + column_sum(du2 * normal),
            sums[1] + column_sum(dz.astype(F32)),
            sums[2] + column_sum(du2),
        )

    nothing = jnp.zeros((1, 512), F32)
    ff_sums = lax.fori_loop(0, 4, finish_hidden, (nothing, nothing, nothing))
    dh2_pairs = ex.sum_pair(B.x_all, B.dh2_pair)
    ff_sums = lax.fori_loop(4, 8, finish_hidden, ff_sums)
    dh2_over = ex.sum_chips(dh2_pairs, B.x_all, B.dh2_pair, B.dh2_paired, B.dh2_chips, B.total)

    @pl.loop(0, 4)
    def _(q):
        terms = contract_rows(B.u2[:, columns(q * 128, 128)], B.g_all[...].reshape(1024, 1024))
        B.down_src[q] = terms.astype(BF)

    down_grads = ex.terms_start(lambda q: B.down_src.at[q], B.down_terms, B.down_passing)

    @pl.loop(0, 8)
    def _(c):
        rows = B.h2_all[:, :, columns(c * 128, 128)].reshape(1024, 128)
        B.up_src[c] = contract_rows(rows, B.dz[...]).astype(BF).reshape(4, 32, 512)

    up_grads = ex.terms_start(lambda q: B.up_src.at[:, q], B.up_terms, B.up_passing)

    @pl.loop(0, 8)
    def _(t):
        B.ffo_src[t] = matmul(B.u2[pl.ds(t * 128, 128), :], B.down_w[...].reshape(512, 1024)).astype(BF)

    ffo_pairs = ex.sum_pair(B.ffo_src, B.ffo_pair)

    dh2 = ex.sum_end(dh2_over, B.dh2_chips, B.total)
    sum_gain_c = column_sum(dh2 * B.normal_c[...])
    sum_shift_c = column_sum(dh2)
    g_local = B.g_all[s].astype(F32)
    dr = g_local + norm_back(dh2, gain_c, B.normal_c[...], inverse_c)
    B.dr[...] = dr
    da = norm_back(dr, gain_b, B.normal_b[...], inverse_b).astype(BF)
    B.da_all[s] = da
    B.do_local[...] = (times_transposed(da, B.out_w[...].reshape(1024, 1024)) * B.scale_row[0:1, :]).astype(BF)
    do_copies = [ex.send(B.do_local.at[:, columns(p * 128, 128)], B.do_all.at[s], p, b) for p in ex.plane()]
    own_do = ex.local(B.do_local.at[:, own_columns], B.do_all.at[s])
    da_slot = lambda i: B.da_all.at[i]
    da_copies = ex.gather_start(B.da_all.at[s], da_slot)
    ex.terms_relay(down_grads, lambda q: B.down_src[q], B.down_joined)
    ex.terms_relay(up_grads, lambda q: B.up_src[:, q], B.up_joined)
    ffo_over = ex.sum_chips(ffo_pairs, B.ffo_src, B.ffo_pair, B.ffo_paired, B.ffo_chips, B.ffo_total)
    sum_gain_b = column_sum(dr * B.normal_b[...])
    sum_shift_b = column_sum(dr)
    sum_g = column_sum(g_local)
    sum_da = column_sum(da.astype(F32))
    B.dk[...] = jnp.zeros((1024, 128), F32)
    B.dv[...] = jnp.zeros((1024, 128), F32)
    ex.arrived(do_copies)
    own_do.wait()

    scale_sums = jnp.zeros((1, 128), F32)
    for size in (256, 512, 768, 1024):
        for h in range(2):

            def back(t, sums, size=size, h=h):
                at = pl.ds(t * 128, 128)
                do = of_head(B.do_all[t], h)
                along = do.astype(F32) * B.attended[at, :]
                delta = jnp.sum(along, axis=-1, keepdims=True)
                kept, first = (B.probs_low, 0) if size <= 512 else (B.probs_high, 512)
                probs = kept[h, pl.ds(t * 128 - first, 128), 0:size]
                dp = times_transposed(do, B.qkv[0:size, 256:384])
                ds = (probs * (dp - delta)).astype(BF)
                found = matmul(ds, of_head(B.qkv[0:size, 128:256], h))
                if h == 0:
                    B.dq[at, :] = found
                else:
                    B.dq[at, :] += found
                B.dk[0:size, :] += contract_rows(ds, of_head(B.qkv[at, 0:128], h))
                B.dv[0:size, :] += contract_rows(probs.astype(BF), do)
                return sums + column_sum(along)

            scale_sums = lax.fori_loop(size // 128 - 2, size // 128, back, scale_sums)

    def join(t, sums):
        at = pl.ds(t * 128, 128)
        dq = (B.dq[at, :] * score_scale).astype(BF)
        dk = (B.dk[at, :] * score_scale).astype(BF)
        dv = B.dv[at, :].astype(BF)
        B.dqkv[at, 0:128] = dq
        B.dqkv[at, 128:256] = dk
        B.dqkv[at, 256:384] = dv
        return (sums[0] + column_sum(dq.astype(F32)), sums[1] + column_sum(dv.astype(F32)))

    def dh1_tile(j):
        t = ex.tile(j)
        rows = B.dqkv[pl.ds(t * 128, 128), :]
        B.dh1_src[t] = times_transposed(rows, B.qkv_w[...].reshape(1024, 384)).astype(BF)

    blank = jnp.zeros((1, 128), F32)
    sum_dq, sum_dv = lax.fori_loop(0, 8, join, (blank, blank))
    pl.loop(0, 4)(dh1_tile)
    dh1_pairs = ex.sum_pair(B.dh1_src, B.dh1_pair)

    @pl.loop(0, 8)
    def _(c):
        terms = contract_rows(B.h1[:, columns(c * 128, 128)], B.dqkv[...])
        B.qkv_src[c] = terms.astype(BF).reshape(4, 32, 384)

    qkv_grads = ex.terms_start(lambda q: B.qkv_src.at[:, q], B.qkv_terms, B.qkv_passing)
    pl.loop(4, 8)(dh1_tile)
    dh1_over = ex.sum_chips(dh1_pairs, B.dh1_src, B.dh1_pair, B.dh1_paired, B.dh1_chips, B.total)
    ex.terms_relay(qkv_grads, lambda q: B.qkv_src[:, q], B.qkv_joined)
    da_passed = ex.gather_forward(da_copies, da_slot)
    ffo = ex.sum_end(ffo_over, B.ffo_chips, B.ffo_total)
    output[...] = jnp.where(held, B.residual[...] + ffo + bias_out, 0.0).astype(BF)
    ex.arrived(da_passed)
    terms = contract_rows(B.scaled[...].reshape(1024, 128), B.da_all[...].reshape(1024, 1024))
    B.out_src[...] = terms.astype(BF).reshape(4, 32, 1024)
    out_grads = [ex.send(B.out_src.at[q], B.out_terms.at[b], s, q) for q in ex.line()]

    def line_sum(mine, landed):
        total = mine
        for k in (1, 2, 3):
            total = total + landed[(b + k) % 4].astype(F32)
        return total

    ex.terms_arrived(down_grads)
    grad_down[...] = line_sum(B.down_src[b].astype(F32), B.down_terms)
    ex.terms_arrived(up_grads)
    B.up_own[...] = line_sum(B.up_src[:, b].astype(F32), B.up_terms).astype(BF)
    up_lanes = up_fin.at[s]
    up_copies = [ex.send(B.up_own.at[p], up_lanes, p, b) for p in ex.plane()]
    own_up = ex.local(B.up_own.at[s], up_lanes)

    dh1 = ex.sum_end(dh1_over, B.dh1_chips, B.total)
    normal_a, inverse_a = centred(x_in[...].astype(F32))
    grad_input[...] = (B.dr[...] + norm_back(dh1, gain_a, normal_a, inverse_a)).astype(BF)
    wide = jnp.concatenate(
        [
            column_sum(dh1 * normal_a),
            sum_gain_b,
            sum_gain_c,
            column_sum(dh1),
            sum_shift_b,
            sum_shift_c,
            jnp.zeros((1, 1024), F32),
            sum_g,
            jnp.zeros((1, 1024), F32),
            sum_da,
            jnp.zeros((6, 1024), F32),
        ],
        axis=0,
    )
    by_head = jnp.zeros((1, 128), F32)
    for h in range(2):
        found = jnp.sum(of_head(scale_sums / own_scale, h), axis=-1, keepdims=True)
        by_head = jnp.where(lane == s * 2 + h, found, by_head)
    place = lax.broadcasted_iota(jnp.int32, (16, 128), 0)
    for p in range(8):
        mine = jnp.where(s == p, 1.0, 0.0)
        tile = wide[:, p * 128 : (p + 1) * 128]
        tile = jnp.where(place == 6, sum_dq * mine, tile)
        tile = jnp.where(place == 8, sum_dv * mine, tile)
        B.close_src[p] = jnp.where(place == 10, by_head, tile)
    close = [ex.send(B.close_src.at[p], B.close_plane.at[s], p, b) for p in ex.plane()]
    own_close = ex.local(B.close_src.at[s], B.close_plane.at[s])
    for q in range(4):
        part = [one[:, q * 128 : (q + 1) * 128] for one in ff_sums]
        B.close_line[q, 16:24, :] = jnp.concatenate(part + [jnp.zeros((5, 128), F32)], axis=0)

    ex.terms_arrived(qkv_grads)
    B.qkv_own[...] = line_sum(B.qkv_src[:, b].astype(F32), B.qkv_terms).astype(BF)
    qkv_copies = [ex.send(B.qkv_own.at[p], qkv_fin.at[s], p, b) for p in ex.plane()]
    own_qkv = [ex.local(B.qkv_own.at[s], qkv_fin.at[s])]
    ex.arrived(close)
    own_close.wait()
    total = B.close_plane[0]
    for i in range(1, 8):
        total = total + B.close_plane[i]
    for q in range(4):
        B.close_line[q, 0:16, :] = total
    close = [ex.send(B.close_line.at[q], B.close_all.at[b], s, q) for q in ex.line()]
    own_close = ex.local(B.close_line.at[b], B.close_all.at[b])
    ex.arrived(out_grads)
    grad_out[...] = line_sum(B.out_src[b].astype(F32), B.out_terms)
    ex.arrived(up_copies)
    own_up.wait()
    ex.arrived(close)
    own_close.wait()
    vec_out[...] = B.close_all[0] + B.close_all[1] + B.close_all[2] + B.close_all[3]
    ex.arrived(qkv_copies)
    for one in own_qkv:
        one.wait()
    ex.finish()


def finish_kernel(output, grad_input, qkv, out, up, down, vectors, *outs):
    b = lax.axis_index("batch")
    outs[0][0] = output[...]
    outs[1][0] = grad_input[...]
    for p in range(8):
        for t in range(3):
            at = t * 1024 + p * 128
            outs[2][:, at : at + 128] = qkv[p, :, t * 128 : (t + 1) * 128].astype(F32)
        outs[4][:, p * 512 : (p + 1) * 512] = up[p].astype(F32)
    outs[3][...] = out[...]
    outs[5][...] = down[...]
    rows = vectors[...]
    own = rows[:, 0:32]
    for q in range(1, 4):
        own = jnp.where(b == q, rows[:, q * 32 : (q + 1) * 32], own)
    outs[6][...] = own[0:3]
    outs[7][...] = own[3:8]
    outs[8][...] = own[8:10]
    outs[9][...] = rows[16:17]
    outs[10][...] = rows[17:19]
    outs[11][...] = rows[10:11, :H]


def plane_shards(
    inputs,
    lengths,
    w_qkv,
    w_out,
    w_up,
    w_down,
    norm_gains,
    model_biases,
    attn_biases,
    ff_gain,
    ff_biases,
    head_scale,
    cotangent,
):
    b = lax.axis_index("batch")
    near = pl.BlockSpec(memory_space=pltpu.VMEM)
    outs = [
        ((128, 1024), BF),
        ((128, 1024), BF),
        ((8, 32, 384), BF),
        ((32, 1024), F32),
        ((8, 32, 512), BF),
        ((128, 1024), F32),
        ((24, 128), F32),
    ]
    found = pl.pallas_call(
        block_kernel,
        name="block",
        out_shape=[jax.ShapeDtypeStruct(shape, dtype) for shape, dtype in outs],
        in_specs=[pl.BlockSpec(memory_space=pltpu.SMEM)] + [near] * (INPUTS - 1),
        out_specs=[near] * OUTPUTS,
        scratch_shapes=[pltpu.VMEM(shape, dtype) for shape, dtype in BUFFERS.values()]
        + [
            pltpu.SemaphoreType.DMA((COPIES,)),
            pltpu.SemaphoreType.DMA((COPIES,)),
            pltpu.SemaphoreType.DMA((32,)),
        ],
        compiler_params=pltpu.CompilerParams(
            collective_id=1, has_side_effects=True, vmem_limit_bytes=67043328
        ),
    )(
        lengths.reshape(1, 1),
        inputs[0],
        cotangent[0],
        w_qkv,
        w_out,
        w_up,
        w_down,
        norm_gains,
        model_biases,
        attn_biases,
        ff_gain.reshape(1, 128),
        ff_biases,
        head_scale.reshape(1, H),
    )
    finals = [
        ((1, 128, 1024), BF),
        ((1, 128, 1024), BF),
        ((32, 3072), F32),
        ((32, 1024), F32),
        ((32, 4096), F32),
        ((128, 1024), F32),
        ((3, 32), F32),
        ((5, 32), F32),
        ((2, 32), F32),
        ((1, 128), F32),
        ((2, 128), F32),
        ((1, H), F32),
    ]
    last = pl.pallas_call(
        finish_kernel,
        name="finish",
        out_shape=[jax.ShapeDtypeStruct(shape, dtype) for shape, dtype in finals],
        in_specs=[near] * OUTPUTS,
        out_specs=[near] * len(finals),
        compiler_params=pltpu.CompilerParams(vmem_limit_bytes=67043328),
    )(*found)
    return tuple(last[:9]) + (last[9].reshape(128), last[10], last[11].reshape(H))


def solution(mesh):
    in_plane = mesh.shape["seq"] == 8 and mesh.shape["batch"] == 4
    return jax.shard_map(
        plane_shards if in_plane else shards,
        mesh=mesh,
        in_specs=(
            P("batch", "seq", None),
            P("batch"),
            P(("seq", "batch"), None),
            P(("seq", "batch"), None),
            P(("seq", "batch"), None),
            P(("seq", "batch"), None),
            P(None, ("seq", "batch")),
            P(None, ("seq", "batch")),
            P(None, ("seq", "batch")),
            P(("seq", "batch")),
            P(None, ("seq", "batch")),
            P(),
            P("batch", "seq", None),
        ),
        out_specs=(
            P("batch", "seq", None),
            P("batch", "seq", None),
            P(("seq", "batch"), None),
            P(("seq", "batch"), None),
            P(("seq", "batch"), None),
            P(("seq", "batch"), None),
            P(None, ("seq", "batch")),
            P(None, ("seq", "batch")),
            P(None, ("seq", "batch")),
            P(("seq", "batch")),
            P(None, ("seq", "batch")),
            P(),
        ),
        check_vma=False,
    )
```
